32 devices in a mesh: dp: 8 (over y, x, core), tensor: 4 (over z).
Axes of the slice: x: 2, y: 2, z: 4, core: 2. Of those that a mesh axis runs over, the one named last changes fastest.
Arguments:
- hidden_in: bfloat16 [4096, 2048], P('dp', 'tensor'), may hold values from -6 to 6
- segment_ids: int32 [8, 512], P('dp'), may hold values from 0 to 3, never falling along the last dimension, each value on 1 to 256 neighbouring positions
- norm1_gain: bfloat16 [2048], P('tensor'), may hold values from 0.099609375 to 1.8984375
- norm1_bias: bfloat16 [2048], P('tensor'), may hold values from -3 to 3
- norm2_gain: bfloat16 [2048], P('tensor'), may hold values from 0.099609375 to 1.8984375
- norm2_bias: bfloat16 [2048], P('tensor'), may hold values from -3 to 3
- qkv_weight: bfloat16 [2048, 6144], P(None, 'tensor'), may hold values from -0.125 to 0.125
- qkv_bias: bfloat16 [6144], P('tensor'), may hold values from -3 to 3
- proj_weight: bfloat16 [2048, 2048], P('tensor'), may hold values from -1 to 1
- up_weight: bfloat16 [2048, 8192], P(None, 'tensor'), may hold values from -0.125 to 0.125
- up_bias: bfloat16 [8192], P('tensor'), may hold values from -3 to 3
- down_weight: bfloat16 [8192, 2048], P('tensor'), may hold values from -0.0625 to 0.0625
- out_bias: bfloat16 [2048], P('tensor'), may hold values from -3 to 3
- cotangent: bfloat16 [4096, 2048], P('dp', 'tensor'), may hold values from -6 to 6
Outputs:
- hidden_out: float32 [4096, 2048], P('dp', 'tensor')
- hidden_grad: float32 [4096, 2048], P('dp', 'tensor')
- norm1_gain_grad: float32 [2048], P('tensor')
- norm1_bias_grad: float32 [2048], P('tensor')
- norm2_gain_grad: float32 [2048], P('tensor')
- norm2_bias_grad: float32 [2048], P('tensor')
- qkv_weight_grad: float32 [2048, 6144], P(None, 'tensor')
- qkv_bias_grad: float32 [6144], P('tensor')
- proj_weight_grad: float32 [2048, 2048], P('tensor')
- up_weight_grad: float32 [2048, 8192], P(None, 'tensor')
- up_bias_grad: float32 [8192], P('tensor')
- down_weight_grad: float32 [8192, 2048], P('tensor')
- out_bias_grad: float32 [2048], P('tensor')
The draws below stay inside these ranges and needn't reach their ends.
Inputs may be any that keep to these rules, and one draw needn't show every extreme that they name: `segment_ids`: row s gives the sequence numbers of data shard s's tokens in order; along a row they never fall, every row holds 4 sequences of 1 to 256 tokens, and some sequence holds exactly 256 tokens.
All inputs are finite; a program needn't handle non-finite values.
Results may differ from the reference program's by a relative error of at most 0.012.
The reference program's roundings to bfloat16 on the way count: a program that leaves them out, or rounds other values in their place, can miss the bound.
Values may be sent and summed in bfloat16 or wider, within the bound.
A program may use at most 320 MiB of HBM per device.

```python
import math
import jax
import jax.numpy as jnp
import numpy as np
from jax import lax

D = 2048
H = 8
HD = 256
ROT = 64
FF = 8192
TOK_DEV = 512
SEQS = 4
MAXLEN = 256
SHARDS = 8
TOKENS = 4096


def steps_of(own_key, dims, cuts, least, high):
    factor_of, own = 1.0, jax.random.fold_in(own_key, 6)
    for dim, blocks in cuts:
        steps = jnp.exp(jax.random.uniform(jax.random.fold_in(own, dim), (blocks,), jnp.float32, least / len(cuts), high / len(cuts)))
        factor_of = factor_of * jnp.repeat(steps, dims[dim] // blocks).reshape([-1 if axis == dim else 1 for axis in range(len(dims))])
    return factor_of


def split_up(number_of, total, bound, lean):
    weights = [(1 << 20) // math.isqrt(rank ** lean) + 1 for rank in range(2, number_of + 1)]
    rest, holding = total - bound - (number_of - 1), [1] * (number_of - 1)
    while rest > 0:
        movable = [i for i in range(number_of - 1) if holding[i] < bound]
        pool, left = sum([weights[i] for i in movable]), rest
        for i in movable:
            extra = min(bound - holding[i], max(1, left * weights[i] // pool), rest)
            holding[i] = holding[i] + extra
            rest = rest - extra
    return np.array([bound] + holding)


def uneven(key, count, total, bound, lean):
    if count == 2:
        one = jax.random.randint(key, (), max(1, total - bound), min(bound, total - 1) + 1)
        return jnp.stack([one, total - one])
    sizes = jnp.asarray(split_up(count, total, bound, lean), jnp.int32)
    pairs = (count - 1) // 2
    donor, sink = sizes[1:1 + 2 * pairs:2], sizes[2:2 + 2 * pairs:2]
    room = jnp.minimum(donor - 1, bound - sink)
    shifted = jax.random.randint(jax.random.fold_in(key, 1), (pairs,), 0, 1 << 20) % (room + 1)
    sizes = sizes.at[1:1 + 2 * pairs:2].set(donor - shifted).at[2:2 + 2 * pairs:2].set(sink + shifted)
    return sizes[jax.random.permutation(jax.random.fold_in(key, 2), count)]


def gaussian(key, extent, spread, bound, cuts=(), kind=jnp.bfloat16):
    loudness = steps_of(key, extent, cuts, -0.22, 0.18) if cuts else 1.0
    drawn = jax.random.normal(key, extent, jnp.float32) * spread * loudness
    return jnp.minimum(jnp.maximum(drawn, -bound), bound).astype(kind)


def setup_inputs(seed: int = 0) -> dict:
    keys = jax.random.split(jax.random.key(seed), 15)
    hidden_in = gaussian(keys[0], (TOKENS, D), 1.0, 6.0, ((0, 8), (1, 4)))
    segment_ids = jax.vmap(lambda own: jnp.searchsorted(jnp.cumsum(uneven(own, SEQS, TOK_DEV, MAXLEN, 2)), jnp.arange(TOK_DEV), side="right"))(jax.random.split(keys[1], SHARDS)).reshape((SHARDS, TOK_DEV)).astype(jnp.int32)
    norm1_gain = jnp.clip(1.0 + 0.18 * jax.random.normal(keys[2], (D,), jnp.float32), 0.099609375, 1.8984375).astype(jnp.bfloat16)
    norm1_bias = gaussian(keys[3], (D,), 0.5, 3.0, ((0, 4),))
    norm2_gain = jnp.clip(1.0 + 0.18 * jax.random.normal(keys[4], (D,), jnp.float32), 0.099609375, 1.8984375).astype(jnp.bfloat16)
    norm2_bias = gaussian(keys[5], (D,), 0.5, 3.0, ((0, 4),))
    qkv_weight = gaussian(keys[6], (D, H * 3 * HD), D ** -0.5, 0.125, ((1, 4),))
    qkv_bias = gaussian(keys[7], (H * 3 * HD,), 0.5, 3.0, ((0, 4),))
    proj_weight = gaussian(keys[8], (H * HD, D), (max(H * HD // 64, 1)) ** -0.5, 1.0, ((0, 4),))
    up_weight = gaussian(keys[9], (D, FF), D ** -0.5, 0.125, ((1, 4),))
    up_bias = gaussian(keys[10], (FF,), 0.5, 3.0, ((0, 4),))
    down_weight = gaussian(keys[11], (FF, D), FF ** -0.5, 0.0625, ((0, 4),))
    out_bias = gaussian(keys[12], (D,), 0.5, 3.0, ((0, 4),))
    cotangent = gaussian(keys[13], (TOKENS, D), 1.0, 6.0, ((0, 8), (1, 4)))
    return {"hidden_in": hidden_in, "segment_ids": segment_ids, "norm1_gain": norm1_gain, "norm1_bias": norm1_bias, "norm2_gain": norm2_gain, "norm2_bias": norm2_bias, "qkv_weight": qkv_weight, "qkv_bias": qkv_bias, "proj_weight": proj_weight, "up_weight": up_weight, "up_bias": up_bias, "down_weight": down_weight, "out_bias": out_bias, "cotangent": cotangent}


root_half = 0.7071067811865476
inv_root_tau = 0.3989422804014327

def norm_stats(values):
    average = lax.optimization_barrier(jnp.mean(values, axis=1, keepdims=True))
    centred = values - average
    spread_sq = lax.optimization_barrier(jnp.mean(centred * centred, axis=1, keepdims=True))
    inverse = lax.rsqrt(spread_sq + 1e-05)
    return (centred * inverse, inverse)

def norm_backward(grad_out, gain, normed, inverse):
    scaled = grad_out * gain[None, :]
    first_mean = lax.optimization_barrier(jnp.mean(scaled, axis=1, keepdims=True))
    second_mean = lax.optimization_barrier(jnp.mean(scaled * normed, axis=1, keepdims=True))
    grad_in = inverse * (scaled - first_mean - normed * second_mean)
    return (grad_in, lax.optimization_barrier(jnp.sum(grad_out * normed, axis=0)), lax.optimization_barrier(jnp.sum(grad_out, axis=0)))

def seq_positions(segment_row):
    indices = jnp.arange(segment_row.shape[0], dtype=jnp.int32)
    earlier = jnp.concatenate([segment_row[:1] - 1, segment_row[:-1]])
    starts = lax.cummax(jnp.where(segment_row != earlier, indices, 0), axis=0)
    return (indices - starts).astype(jnp.float32)

def rotary_tables(positions, rot_dims):
    half_dims = rot_dims // 2
    exponent = jnp.arange(half_dims, dtype=jnp.float32) * (2.0 / rot_dims)
    inv_freq = jnp.exp(-exponent * math.log(10000.0))
    angles = positions[:, None] * inv_freq[None, :]
    return (jnp.cos(angles), jnp.sin(angles))

def rotate_rows(values, cosine, sine, rot_dims, direction):
    half_dims = rot_dims // 2
    first_half = values[:, :half_dims]
    second_half = values[:, half_dims:rot_dims]
    turned_first = first_half * cosine - direction * second_half * sine
    turned_second = second_half * cosine + direction * first_half * sine
    return jnp.concatenate([turned_first, turned_second, values[:, rot_dims:]], axis=1)

def gelu_exact(values):
    return 0.5 * values * (1.0 + lax.erf(values * root_half))

def gelu_slope(values):
    return 0.5 * (1.0 + lax.erf(values * root_half)) + values * jnp.exp(-0.5 * values * values) * inv_root_tau

def masked_scores(query_block, key_cols, segment_block, segment_row, block_start, block_rows, score_scale):
    row_count = segment_row.shape[0]
    key_index = jnp.arange(row_count, dtype=jnp.int32)
    row_index = block_start + jnp.arange(block_rows, dtype=jnp.int32)
    scores = jnp.dot(query_block, key_cols, preferred_element_type=jnp.float32) * score_scale
    allowed = (segment_block[:, None] == segment_row[None, :]) & (key_index[None, :] <= row_index[:, None])
    return jnp.where(allowed, scores, -1e+30)

def head_forward(query_rows, key_rows, value_rows, segment_row, block_rows):
    row_count = query_rows.shape[0]
    score_scale = 1.0 / math.sqrt(query_rows.shape[1])
    key_cols = key_rows.T

    def one_block(block_start):
        query_block = lax.dynamic_slice_in_dim(query_rows, block_start, block_rows, 0)
        segment_block = lax.dynamic_slice_in_dim(segment_row, block_start, block_rows, 0)
        scores = masked_scores(query_block, key_cols, segment_block, segment_row, block_start, block_rows, score_scale)
        row_max = lax.optimization_barrier(jnp.max(scores, axis=1, keepdims=True))
        log_total = row_max + jnp.log(lax.optimization_barrier(jnp.sum(jnp.exp(scores - row_max), axis=1, keepdims=True)))
        attn_probs = jnp.exp(scores - log_total).astype(jnp.bfloat16)
        context = jnp.dot(attn_probs, value_rows, preferred_element_type=jnp.float32).astype(jnp.bfloat16)
        return (context, log_total[:, 0])
    block_starts = jnp.arange(row_count // block_rows, dtype=jnp.int32) * block_rows
    context, log_totals = lax.map(one_block, block_starts)
    return (context.reshape(row_count, -1), log_totals.reshape(row_count))

def head_backward(query_rows, key_rows, value_rows, context, grad_context, log_totals, segment_row, block_rows):
    row_count = query_rows.shape[0]
    score_scale = 1.0 / math.sqrt(query_rows.shape[1])
    key_cols = key_rows.T
    value_cols = value_rows.T

    def one_block(running, block_start):
        grad_keys, grad_values = running
        query_block = lax.dynamic_slice_in_dim(query_rows, block_start, block_rows, 0)
        segment_block = lax.dynamic_slice_in_dim(segment_row, block_start, block_rows, 0)
        context_block = lax.dynamic_slice_in_dim(context, block_start, block_rows, 0)
        grad_block = lax.dynamic_slice_in_dim(grad_context, block_start, block_rows, 0)
        total_block = lax.dynamic_slice_in_dim(log_totals, block_start, block_rows, 0)
        scores = masked_scores(query_block, key_cols, segment_block, segment_row, block_start, block_rows, score_scale)
        attn_probs = jnp.exp(scores - total_block[:, None])
        grad_probs = jnp.dot(grad_block, value_cols, preferred_element_type=jnp.float32)
        delta_rows = lax.optimization_barrier(jnp.sum(grad_block.astype(jnp.float32) * context_block.astype(jnp.float32), axis=1, keepdims=True))
        grad_scores = (attn_probs * (grad_probs - delta_rows) * score_scale).astype(jnp.bfloat16)
        grad_query = jnp.dot(grad_scores, key_rows, preferred_element_type=jnp.float32)
        grad_keys = grad_keys + jnp.dot(grad_scores.T, query_block, preferred_element_type=jnp.float32)
        grad_values = grad_values + jnp.dot(attn_probs.astype(jnp.bfloat16).T, grad_block, preferred_element_type=jnp.float32)
        return ((grad_keys, grad_values), grad_query)
    block_starts = jnp.arange(row_count // block_rows, dtype=jnp.int32) * block_rows
    zero_rows = jnp.zeros(key_rows.shape, jnp.float32)
    (grad_keys, grad_values), grad_query = lax.scan(one_block, (zero_rows, zero_rows), block_starts)
    return (grad_query.reshape(row_count, -1), grad_keys, grad_values)

def shard_work(rows_in, segment_row, rows_cot, norm_params, qkv_weight, qkv_bias, proj_weight, up_weight, up_bias, down_weight, out_bias):
    row_count = rows_in.shape[0]
    heads_here = qkv_weight.shape[1] // (3 * HD)
    block_rows = min(512, row_count)
    values_in = rows_in.astype(jnp.float32)
    normed, inverse = norm_stats(values_in)
    act_one = (normed * norm_params[0][None, :] + norm_params[1][None, :]).astype(jnp.bfloat16)
    act_two = (normed * norm_params[2][None, :] + norm_params[3][None, :]).astype(jnp.bfloat16)
    cosine, sine = rotary_tables(seq_positions(segment_row), ROT)
    qkv_all = jnp.dot(act_one, qkv_weight, preferred_element_type=jnp.float32) + qkv_bias.astype(jnp.float32)[None, :]
    qkv_all = qkv_all.reshape(row_count, heads_here, 3, HD)
    saved = []
    contexts = []
    for head_num in range(heads_here):
        query_rows = rotate_rows(qkv_all[:, head_num, 0], cosine, sine, ROT, 1.0).astype(jnp.bfloat16)
        key_rows = rotate_rows(qkv_all[:, head_num, 1], cosine, sine, ROT, 1.0).astype(jnp.bfloat16)
        value_rows = qkv_all[:, head_num, 2].astype(jnp.bfloat16)
        context, log_totals = head_forward(query_rows, key_rows, value_rows, segment_row, block_rows)
        saved.append((query_rows, key_rows, value_rows, context, log_totals))
        contexts.append(context)
    context_all = jnp.concatenate(contexts, axis=1)
    pre_up = jnp.dot(act_two, up_weight, preferred_element_type=jnp.float32) + up_bias.astype(jnp.float32)[None, :]
    hidden_act = gelu_exact(pre_up).astype(jnp.bfloat16)
    partial_value = jnp.dot(context_all, proj_weight, preferred_element_type=jnp.float32) + jnp.dot(hidden_act, down_weight, preferred_element_type=jnp.float32)
    rows_out = values_in + partial_value + out_bias.astype(jnp.float32)[None, :]
    cot_values = rows_cot.astype(jnp.float32)
    out_bias_grad = lax.optimization_barrier(jnp.sum(cot_values, axis=0))
    proj_grad = jnp.dot(context_all.T, rows_cot, preferred_element_type=jnp.float32)
    down_grad = jnp.dot(hidden_act.T, rows_cot, preferred_element_type=jnp.float32)
    grad_context = jnp.dot(rows_cot, proj_weight.T, preferred_element_type=jnp.float32).astype(jnp.bfloat16)
    grad_pre = jnp.dot(rows_cot, down_weight.T, preferred_element_type=jnp.float32) * gelu_slope(pre_up)
    up_bias_grad = lax.optimization_barrier(jnp.sum(grad_pre, axis=0))
    grad_pre_low = grad_pre.astype(jnp.bfloat16)
    up_grad = jnp.dot(act_two.T, grad_pre_low, preferred_element_type=jnp.float32)
    grad_act_two = jnp.dot(grad_pre_low, up_weight.T, preferred_element_type=jnp.float32)
    head_grads = []
    for head_num in range(heads_here):
        query_rows, key_rows, value_rows, context, log_totals = saved[head_num]
        grad_slice = grad_context[:, head_num * HD:(head_num + 1) * HD]
        grad_query, grad_keys, grad_values = head_backward(query_rows, key_rows, value_rows, context, grad_slice, log_totals, segment_row, block_rows)
        grad_query = rotate_rows(grad_query, cosine, sine, ROT, -1.0)
        grad_keys = rotate_rows(grad_keys, cosine, sine, ROT, -1.0)
        head_grads.append(jnp.stack([grad_query, grad_keys, grad_values], axis=1))
    grad_qkv = jnp.stack(head_grads, axis=1).reshape(row_count, heads_here * 3 * HD)
    qkv_bias_grad = lax.optimization_barrier(jnp.sum(grad_qkv, axis=0))
    grad_qkv_low = grad_qkv.astype(jnp.bfloat16)
    qkv_grad = jnp.dot(act_one.T, grad_qkv_low, preferred_element_type=jnp.float32)
    grad_act_one = jnp.dot(grad_qkv_low, qkv_weight.T, preferred_element_type=jnp.float32)
    grad_in_one, gain_one, shift_one = norm_backward(grad_act_one, norm_params[0], normed, inverse)
    grad_in_two, gain_two, shift_two = norm_backward(grad_act_two, norm_params[2], normed, inverse)
    rows_grad = cot_values + grad_in_one + grad_in_two
    grads = (qkv_grad, qkv_bias_grad, proj_grad, up_grad, up_bias_grad, down_grad, out_bias_grad, gain_one, shift_one, gain_two, shift_two)
    return (rows_out, rows_grad, grads)

def reference(hidden_in, segment_ids, norm1_gain, norm1_bias, norm2_gain, norm2_bias, qkv_weight, qkv_bias, proj_weight, up_weight, up_bias, down_weight, out_bias, cotangent):
    shard_count = segment_ids.shape[0]
    row_count = segment_ids.shape[1]
    width = hidden_in.shape[1]
    norm_params = jnp.stack([norm1_gain, norm1_bias, norm2_gain, norm2_bias]).astype(jnp.float32)
    inputs = hidden_in.reshape(shard_count, row_count, width)
    cots = cotangent.reshape(shard_count, row_count, width)
    zero_grads = (jnp.zeros(qkv_weight.shape, jnp.float32), jnp.zeros(qkv_bias.shape, jnp.float32), jnp.zeros(proj_weight.shape, jnp.float32), jnp.zeros(up_weight.shape, jnp.float32), jnp.zeros(up_bias.shape, jnp.float32), jnp.zeros(down_weight.shape, jnp.float32), jnp.zeros(out_bias.shape, jnp.float32), jnp.zeros((width,), jnp.float32), jnp.zeros((width,), jnp.float32), jnp.zeros((width,), jnp.float32), jnp.zeros((width,), jnp.float32))

    def one_shard(running, pieces):
        rows_in, segment_row, rows_cot = pieces
        rows_out, rows_grad, grads = shard_work(rows_in, segment_row, rows_cot, norm_params, qkv_weight, qkv_bias, proj_weight, up_weight, up_bias, down_weight, out_bias)
        return (jax.tree.map(lambda left, right: left + right, running, grads), (rows_out, rows_grad))
    grads, (outs_all, grads_all) = lax.scan(one_shard, zero_grads, (inputs, segment_ids, cots))
    qkv_grad, qkv_bias_grad, proj_grad, up_grad, up_bias_grad, down_grad, out_bias_grad, gain_one, shift_one, gain_two, shift_two = grads
    return (outs_all.reshape(shard_count * row_count, width), grads_all.reshape(shard_count * row_count, width), gain_one, shift_one, gain_two, shift_two, qkv_grad, qkv_bias_grad, proj_grad, up_grad, up_bias_grad, down_grad, out_bias_grad)
```

```python
import math

import jax
import jax.numpy as jnp
from jax import lax
from jax.experimental import pallas as pl
from jax.experimental.pallas import tpu as pltpu
from jax.sharding import PartitionSpec as P

HD = 256
ROT = 64


root_half = 0.7071067811865476
inv_root_tau = 0.3989422804014327
F32 = jnp.float32
BF16 = jnp.bfloat16


def norm_stats(values):
    average = jnp.mean(values, axis=1, keepdims=True)
    centred = values - average
    spread_sq = jnp.mean(centred * centred, axis=1, keepdims=True)
    inverse = lax.rsqrt(spread_sq + 1e-05)
    return (centred * inverse, inverse)


def norm_backward(grad_out, gain, normed, inverse):
    scaled = grad_out * gain[None, :]
    first_mean = jnp.mean(scaled, axis=1, keepdims=True)
    second_mean = jnp.mean(scaled * normed, axis=1, keepdims=True)
    grad_in = inverse * (scaled - first_mean - normed * second_mean)
    return (grad_in, jnp.sum(grad_out * normed, axis=0), jnp.sum(grad_out, axis=0))


def seq_positions(segment_row):
    indices = jnp.arange(segment_row.shape[0], dtype=jnp.int32)
    same = segment_row[:, None] == segment_row[None, :]
    earlier = same & (indices[None, :] < indices[:, None])
    return jnp.sum(earlier.astype(F32), axis=1)


def rotary_tables(positions, rot_dims):
    half_dims = rot_dims // 2
    exponent = jnp.arange(half_dims, dtype=F32) * (2.0 / rot_dims)
    inv_freq = jnp.exp(-exponent * math.log(10000.0))
    angles = positions[:, None] * inv_freq[None, :]
    return (jnp.cos(angles), jnp.sin(angles))


def rotate_rows(values, cosine, sine, rot_dims, direction):
    half_dims = rot_dims // 2
    first_half = values[:, :half_dims]
    second_half = values[:, half_dims:rot_dims]
    turned_first = first_half * cosine - direction * second_half * sine
    turned_second = second_half * cosine + direction * first_half * sine
    return jnp.concatenate([turned_first, turned_second, values[:, rot_dims:]], axis=1)


def gelu_exact(values):
    return 0.5 * values * (1.0 + lax.erf(values * root_half))


def gelu_slope(values):
    return (
        0.5 * (1.0 + lax.erf(values * root_half))
        + values * jnp.exp(-0.5 * values * values) * inv_root_tau
    )


def dot(a, b):
    return jnp.dot(a, b, preferred_element_type=F32)


def dot_t(a, b):
    return lax.dot_general(a, b, (((1,), (1,)), ((), ())), preferred_element_type=F32)


def t_dot(a, b):
    return lax.dot_general(a, b, (((0,), (0,)), ((), ())), preferred_element_type=F32)


def head_forward(query_rows, key_rows, value_rows, allowed):
    score_scale = 1.0 / math.sqrt(query_rows.shape[1])
    scores = jnp.where(allowed, dot_t(query_rows, key_rows) * score_scale, -1e30)
    row_max = jnp.max(scores, axis=1, keepdims=True)
    log_total = row_max + jnp.log(jnp.sum(jnp.exp(scores - row_max), axis=1, keepdims=True))
    attn_probs = jnp.exp(scores - log_total)
    probs_low = attn_probs.astype(BF16)
    context = dot(probs_low, value_rows).astype(BF16)
    return (context, attn_probs, probs_low)


def head_backward(query_rows, key_rows, value_rows, context, grad_context, attn_probs, probs_low):
    score_scale = 1.0 / math.sqrt(query_rows.shape[1])
    grad_probs = dot_t(grad_context, value_rows)
    delta_rows = jnp.sum(
        grad_context.astype(F32) * context.astype(F32), axis=1, keepdims=True
    )
    grad_scores = (attn_probs * (grad_probs - delta_rows) * score_scale).astype(BF16)
    grad_query = dot(grad_scores, key_rows)
    grad_keys = t_dot(grad_scores, query_rows)
    grad_values = t_dot(probs_low, grad_context)
    return (grad_query, grad_keys, grad_values)


class Net:
    def __init__(self, mesh):
        self.nd = mesh.shape["dp"]
        self.nt = mesh.shape["tensor"]
        self.bits = self.nd.bit_length() - 1
        assert 1 << self.bits == self.nd

    def swap(self, value, bit):
        pairs = [(i, i ^ (1 << bit)) for i in range(self.nd)]
        return lax.ppermute(value, "dp", pairs)

    def swap_tensor(self, value, k):
        pairs = [(i, i ^ k) for i in range(self.nt)]
        return lax.ppermute(value, "tensor", pairs)

    def shift(self, value):
        pairs = [(i, (i + 1) % self.nt) for i in range(self.nt)]
        return lax.ppermute(value, "tensor", pairs)

    def gather(self, value, splits):
        rows = value.shape[0] // splits
        held = [[value[i * rows : (i + 1) * rows]] for i in range(splits)]
        for _ in range(self.nt - 1):
            for part in held:
                part.append(self.shift(part[-1]))
        me = lax.axis_index("tensor")
        done = []
        for part in held:
            slots = []
            for slot in range(self.nt):
                which = lax.rem(me - slot + self.nt, self.nt)
                chosen = part[0]
                for k in range(1, self.nt):
                    chosen = jnp.where(which == k, part[k], chosen)
                slots.append(chosen)
            done.append(jnp.concatenate(slots, axis=1))
        return jnp.concatenate(done, axis=0)

    def scatter_sum(self, value):
        me = lax.axis_index("tensor")
        width = value.shape[1] // self.nt
        total = lax.dynamic_slice_in_dim(value, me * width, width, 1)
        for k in range(1, self.nt):
            there = jnp.bitwise_xor(me, k)
            block = lax.dynamic_slice_in_dim(value, there * width, width, 1).astype(BF16)
            total = total + self.swap_tensor(block, k).astype(F32)
        return total

    def sum_small(self, value):
        for bit in range(self.bits):
            value = value + self.swap(value, bit)
        return value

    def sum_small_tensor(self, value):
        k = 1
        while k < self.nt:
            value = value + self.swap_tensor(value, k)
            k *= 2
        return value


def flow_orders(bits):
    others = list(range(1, bits))
    return [others, others[::-1]]


def weight_grad(net, left, right):
    me = lax.axis_index("dp")
    bit_of = [jnp.bitwise_and(jnp.right_shift(me, b), 1) for b in range(net.bits)]
    rows = left.shape[1]
    orders = flow_orders(net.bits)

    def product(start, count):
        return t_dot(lax.dynamic_slice_in_dim(left, start, count, 1), right)

    half = rows // 2
    quarter = half // 2
    away = product((1 - bit_of[0]) * half, half).astype(BF16)
    arrived = net.swap(away, 0)
    base = bit_of[0] * half
    owned = []
    for flow, order in enumerate(orders):
        size = quarter // 2
        first = order[0]
        offset = flow * quarter
        send_at = offset + (1 - bit_of[first]) * size
        keep_at = offset + bit_of[first] * size
        send = product(base + send_at, size) + lax.dynamic_slice_in_dim(
            arrived, send_at, size, 0
        ).astype(F32)
        got = net.swap(send.astype(BF16), first)
        keep = product(base + keep_at, size) + lax.dynamic_slice_in_dim(
            arrived, keep_at, size, 0
        ).astype(F32)
        for bit in order[1:]:
            size //= 2
            here, there = bit_of[bit] * size, (1 - bit_of[bit]) * size
            send = lax.dynamic_slice_in_dim(keep, there, size, 0) + lax.dynamic_slice_in_dim(
                got, there, size, 0
            ).astype(F32)
            keep = lax.dynamic_slice_in_dim(keep, here, size, 0) + lax.dynamic_slice_in_dim(
                got, here, size, 0
            ).astype(F32)
            got = net.swap(send.astype(BF16), bit)
        owned.append((keep + got.astype(F32)).astype(BF16))
    pieces = []
    for flow, order in enumerate(orders):
        have = [owned[flow]]
        for bit in order[::-1]:
            have = have + [net.swap(piece, bit) for piece in have]
        have = have + [net.swap(piece, 0) for piece in have]
        pieces.append(have)
    return place_pieces(net, pieces, rows)


def place_pieces(net, pieces, rows):
    orders = flow_orders(net.bits)
    flat = [piece for flow in pieces for piece in flow]
    count = len(flat)
    size, columns = flat[0].shape
    dtype = F32

    def body(*refs):
        ins, out, wide, low, in_sem, out_sem = (
            refs[:count], refs[count], refs[count + 1], refs[count + 2], refs[-2], refs[-1]
        )
        me = lax.axis_index("dp")
        mine = [jnp.bitwise_and(jnp.right_shift(me, b), 1) for b in range(net.bits)]

        def row_of(index):
            flow, k = divmod(index, count // 2)
            order = orders[flow]
            levels = [mine[b] for b in order]
            depth = len(order)
            digits = []
            for level in range(depth):
                flip = (k >> (depth - 1 - level)) & 1
                digits.append(1 - levels[level] if flip else levels[level])
            core = 1 - mine[0] if (k >> depth) & 1 else mine[0]
            block = core * 2 + flow
            for digit in digits:
                block = block * 2 + digit
            return pl.multiple_of(block * size, size)

        def load(i):
            return pltpu.make_async_copy(ins[i], low.at[i % 2], in_sem.at[i % 2])

        def store(i):
            return pltpu.make_async_copy(
                wide.at[i % 2], out.at[pl.ds(row_of(i), size), :], out_sem.at[i % 2]
            )

        load(0).start()
        for i in range(count):
            if i + 1 < count:
                load(i + 1).start()
            load(i).wait()
            if i >= 2:
                store(i - 2).wait()
            wide[i % 2] = low[i % 2].astype(dtype)
            store(i).start()
        for i in range(max(0, count - 2), count):
            store(i).wait()

    return pl.pallas_call(
        body,
        out_shape=jax.ShapeDtypeStruct((rows, columns), dtype),
        in_specs=[pl.BlockSpec(memory_space=pl.ANY)] * count,
        out_specs=pl.BlockSpec(memory_space=pl.ANY),
        scratch_shapes=[
            pltpu.VMEM((2, size, columns), dtype),
            pltpu.VMEM((2, size, columns), BF16),
            pltpu.SemaphoreType.DMA((2,)),
            pltpu.SemaphoreType.DMA((2,)),
        ],
        name="place_pieces",
        cost_estimate=pl.CostEstimate(
            flops=rows * columns, bytes_accessed=rows * columns * 6, transcendentals=0
        ),
    )(*flat)


MESH_ID = pl.DeviceIdType.MESH
TILE = 512
PIECE = 128
DEPTH = 6
VMEM_LIMIT = 66_000_000


class Ring:
    def __init__(self, part, recv0, recv1, recv2, ssem, rsem):
        self.part, self.recv0, self.recv1, self.recv2 = part, recv0, recv1, recv2
        self.ssem, self.rsem = ssem, rsem
        me = lax.axis_index("dp")
        self.me = me
        self.bit = [lax.rem(lax.div(me, 1 << b), 2) for b in range(3)]
        self.dests = []

    def partner(self, bit):
        return {"dp": self.me + (1 - 2 * self.bit[bit]) * (1 << bit)}

    def axes(self, flow):
        return (1, 2) if flow == 0 else (2, 1)

    def barrier(self, extra=()):
        sem = pltpu.get_barrier_semaphore()
        ids = [self.partner(b) for b in range(3)] + list(extra)
        for one in ids:
            pl.semaphore_signal(sem, inc=1, device_id=one, device_id_type=MESH_ID)
        pl.semaphore_wait(sem, len(ids))

    def piece(self, flow, core, a, b):
        first, second = self.axes(flow)

        def digit(bit, flip):
            return 1 - self.bit[bit] if flip else self.bit[bit]

        return digit(0, core) * 8 + flow * 4 + digit(first, a) * 2 + digit(second, b)

    def send(self, src, dst, slot, s, r, bit):
        return pltpu.make_async_remote_copy(
            src_ref=src,
            dst_ref=dst,
            send_sem=self.ssem.at[slot, s],
            recv_sem=self.rsem.at[slot, r],
            device_id=self.partner(bit),
            device_id_type=MESH_ID,
        )

    def rows(self, start, count):
        return pl.ds(pl.multiple_of(start, PIECE), count)

    def add(self, slot, start, source, at, count):
        part = self.part

        @pl.loop(0, count // PIECE)
        def _(k):
            here = self.rows(start + k * PIECE, PIECE)
            there = self.rows(at + k * PIECE, PIECE)
            part[slot, here, :] = (
                part[slot, here, :].astype(F32) + source[there, :].astype(F32)
            ).astype(BF16)

    def copy0(self, i):
        slot = i % DEPTH
        away = (1 - self.bit[0]) * 1024
        return self.send(
            self.part.at[slot, self.rows(away, 1024)], self.recv0.at[slot], slot, 0, 0, 0
        )

    def copy1(self, i, flow):
        slot = i % DEPTH
        a = self.axes(flow)[0]
        start = self.bit[0] * 1024 + flow * 512 + (1 - self.bit[a]) * 256
        return self.send(
            self.part.at[slot, self.rows(start, 256)],
            self.recv1.at[slot, flow],
            slot, 1 + flow, 1 + flow, a,
        )

    def copy2(self, i, flow):
        slot = i % DEPTH
        b = self.axes(flow)[1]
        return self.send(
            self.part.at[slot, self.rows(self.piece(flow, 0, 0, 1) * PIECE, PIECE)],
            self.recv2.at[slot, flow],
            slot, 3 + flow, 3 + flow, b,
        )

    def out(self, i, index):
        return self.dests[i](index)

    def copy3(self, i, flow):
        slot = i % DEPTH
        a, b = self.axes(flow)
        own = self.piece(flow, 0, 0, 0)
        src = self.part.at[slot, self.rows(own * PIECE, PIECE)]
        dst = self.out(i, own)
        s = 5 + flow * 8
        return [
            self.send(src, dst, slot, s, 5 + flow * 7, b),
            self.send(src, dst, slot, s + 1, 6 + flow * 7, a),
            self.send(src, dst, slot, s + 2, 8 + flow * 7, 0),
            pltpu.make_async_copy(src, dst, self.ssem.at[slot, s + 3]),
        ]

    def copy4(self, i, flow):
        slot = i % DEPTH
        a = self.axes(flow)[0]
        ref = self.out(i, self.piece(flow, 0, 0, 1))
        s = 9 + flow * 8
        return [
            self.send(ref, ref, slot, s, 7 + flow * 7, a),
            self.send(ref, ref, slot, s + 1, 9 + flow * 7, 0),
        ]

    def copy5(self, i, flow):
        slot = i % DEPTH
        s = 11 + flow * 8
        refs = [self.out(i, self.piece(flow, 0, 1, k)) for k in range(2)]
        return [self.send(refs[k], refs[k], slot, s + k, 10 + k + flow * 7, 0) for k in range(2)]

    def stage0(self, i):
        self.copy0(i).start()

    def stage1(self, i):
        slot = i % DEPTH
        self.copy0(i).wait()
        half = self.bit[0] * 1024
        for flow in range(2):
            a = self.axes(flow)[0]
            start = flow * 512 + (1 - self.bit[a]) * 256
            self.add(slot, half + start, self.recv0.at[slot], start, 256)
            self.copy1(i, flow).start()
        for flow in range(2):
            a = self.axes(flow)[0]
            start = flow * 512 + self.bit[a] * 256
            self.add(slot, half + start, self.recv0.at[slot], start, 256)

    def stage2(self, i):
        slot = i % DEPTH
        for flow in range(2):
            self.copy1(i, flow).wait()
            b = self.axes(flow)[1]
            source = self.recv1.at[slot, flow]
            there, here = (1 - self.bit[b]) * PIECE, self.bit[b] * PIECE
            self.add(slot, self.piece(flow, 0, 0, 1) * PIECE, source, there, PIECE)
            self.copy2(i, flow).start()
            self.add(slot, self.piece(flow, 0, 0, 0) * PIECE, source, here, PIECE)

    def stage3(self, i):
        slot = i % DEPTH
        for flow in range(2):
            self.copy2(i, flow).wait()
            self.add(
                slot, self.piece(flow, 0, 0, 0) * PIECE, self.recv2.at[slot, flow], 0, PIECE
            )
            for copy in self.copy3(i, flow):
                copy.start()

    def stage4(self, i):
        for flow in range(2):
            copies = self.copy3(i, flow)
            copies[0].wait_recv()
            for copy in self.copy4(i, flow):
                copy.start()
        for flow in range(2):
            copies = self.copy3(i, flow)
            for copy in copies[:3]:
                copy.wait_send()
            copies[3].wait()

    def stage5(self, i):
        for flow in range(2):
            self.copy3(i, flow)[1].wait_recv()
            self.copy4(i, flow)[0].wait()
            for copy in self.copy5(i, flow):
                copy.start()

    def stage6(self, i):
        for flow in range(2):
            self.copy3(i, flow)[2].wait_recv()
            self.copy4(i, flow)[1].wait()
            for copy in self.copy5(i, flow):
                copy.wait()


def ring_scratch():
    return [
        pltpu.VMEM((DEPTH, 2048, TILE), BF16),
        pltpu.VMEM((DEPTH, 1024, TILE), BF16),
        pltpu.VMEM((DEPTH, 2, 256, TILE), BF16),
        pltpu.VMEM((DEPTH, 2, PIECE, TILE), BF16),
        pltpu.SemaphoreType.DMA((DEPTH, 21)),
        pltpu.SemaphoreType.DMA((DEPTH, 19)),
    ]


def wide_dest(ref, column):
    def at(index):
        return ref.at[
            pl.ds(pl.multiple_of(index * PIECE, PIECE), PIECE), pl.ds(column * TILE, TILE)
        ]

    return at


def tall_dest(ref, row):
    def at(index):
        down = row * TILE + lax.rem(index, 4) * PIECE
        across = lax.div(index, 4) * TILE
        return ref.at[
            pl.ds(pl.multiple_of(down, PIECE), PIECE), pl.ds(pl.multiple_of(across, TILE), TILE)
        ]

    return at


def run_kernel(
    hidden_act, act_two, act_one, context, cot, grad_pre, grad_qkv, down, up, qkv, proj, *scratch
):
    ring = Ring(*scratch)
    ring.barrier()
    part = ring.part
    core = ring.bit[0]

    def columns(ref, start, width):
        return ref[:, pl.ds(pl.multiple_of(start, PIECE), width)]

    def product(i, left_of, right_of):
        slot = i % DEPTH

        def half(which):
            @pl.loop(0, 4)
            def _(k):
                tile = which * 4 + k
                part[slot, pl.ds(pl.multiple_of(tile * 256, 256), 256), :] = t_dot(
                    left_of(tile), right_of(tile)
                ).astype(BF16)

        half(1 - core)
        ring.stage0(i)
        half(core)

    jobs = []

    def wide(left, right, out, column):
        ring.dests.append(wide_dest(out, column))
        jobs.append(
            (
                lambda t: columns(left, t * 256, 256),
                lambda t: right[:, column * TILE : (column + 1) * TILE],
            )
        )

    def tall(left, right, out, row):
        ring.dests.append(tall_dest(out, row))
        jobs.append(
            (
                lambda t: columns(left, row * TILE + lax.rem(t, 2) * 256, 256),
                lambda t: columns(right, lax.div(t, 2) * TILE, TILE),
            )
        )

    for j in range(hidden_act.shape[1] // TILE):
        tall(hidden_act, cot, down, j)
        wide(act_two, grad_pre, up, j)
    for j in range(context.shape[1] // TILE):
        tall(context, cot, proj, j)
    for j in range(grad_qkv.shape[1] // TILE):
        wide(act_one, grad_qkv, qkv, j)
    count = len(jobs)
    stages = [ring.stage1, ring.stage2, ring.stage3, ring.stage4, ring.stage5, ring.stage6]
    for step in range(count + DEPTH):
        for depth in range(DEPTH, 0, -1):
            if 0 <= step - depth < count:
                stages[depth - 1](step - depth)
        if step < count:
            product(step, *jobs[step])


def fused_grads(hidden_act, act_two, act_one, context, cot, grad_pre, grad_qkv):
    width = act_one.shape[1]

    def shape(rows, columns):
        return jax.ShapeDtypeStruct((rows, columns), BF16)

    outs = pl.pallas_call(
        run_kernel,
        out_shape=[
            shape(hidden_act.shape[1], width),
            shape(width, grad_pre.shape[1]),
            shape(width, grad_qkv.shape[1]),
            shape(context.shape[1], width),
        ],
        in_specs=[pl.BlockSpec(memory_space=pltpu.VMEM)] * 7,
        out_specs=[pl.BlockSpec(memory_space=pl.ANY)] * 4,
        scratch_shapes=ring_scratch(),
        compiler_params=pltpu.CompilerParams(
            collective_id=0, has_side_effects=True, vmem_limit_bytes=VMEM_LIMIT
        ),
        name="fused_grads",
    )(hidden_act, act_two, act_one, context, cot, grad_pre, grad_qkv)
    return [out.astype(F32) for out in outs]


def per_device(
    net,
    hidden_in,
    segment_ids,
    norm1_gain,
    norm1_bias,
    norm2_gain,
    norm2_bias,
    qkv_weight,
    qkv_bias,
    proj_weight,
    up_weight,
    up_bias,
    down_weight,
    out_bias,
    cotangent,
):
    norm_stack = jnp.stack([norm1_gain, norm1_bias, norm2_gain, norm2_bias])
    full_rows = net.gather(hidden_in, 2)
    norm_full = net.gather(norm_stack, 1)
    cot_full = net.gather(cotangent, 2)
    norm_params = norm_full.astype(F32)
    segment_row = segment_ids[0]
    row_count = full_rows.shape[0]
    heads_here = qkv_weight.shape[1] // (3 * HD)
    normed, inverse = norm_stats(full_rows.astype(F32))
    act_one = (normed * norm_params[0][None, :] + norm_params[1][None, :]).astype(BF16)
    act_two = (normed * norm_params[2][None, :] + norm_params[3][None, :]).astype(BF16)

    pre_up = dot(act_two, up_weight) + up_bias.astype(F32)[None, :]
    hidden_act = gelu_exact(pre_up).astype(BF16)
    grad_pre = dot_t(cot_full, down_weight) * gelu_slope(pre_up)
    up_bias_grad = jnp.sum(grad_pre, axis=0)
    grad_pre_low = grad_pre.astype(BF16)

    cosine, sine = rotary_tables(seq_positions(segment_row), ROT)
    index = jnp.arange(row_count, dtype=jnp.int32)
    allowed = (segment_row[:, None] == segment_row[None, :]) & (index[None, :] <= index[:, None])
    qkv_all = dot(act_one, qkv_weight) + qkv_bias.astype(F32)[None, :]
    saved = []
    contexts = []
    for head_num in range(heads_here):
        part = qkv_all[:, head_num * 3 * HD : (head_num + 1) * 3 * HD]
        query_rows = rotate_rows(part[:, :HD], cosine, sine, ROT, 1.0).astype(BF16)
        key_rows = rotate_rows(part[:, HD : 2 * HD], cosine, sine, ROT, 1.0).astype(BF16)
        value_rows = part[:, 2 * HD :].astype(BF16)
        context, attn_probs, probs_low = head_forward(query_rows, key_rows, value_rows, allowed)
        saved.append((query_rows, key_rows, value_rows, context, attn_probs, probs_low))
        contexts.append(context)
    context_all = jnp.concatenate(contexts, axis=1)
    partial_value = dot(context_all, proj_weight) + dot(hidden_act, down_weight)
    mixed = net.scatter_sum(partial_value)
    hidden_out = hidden_in.astype(F32) + mixed + out_bias.astype(F32)[None, :]
    out_bias_grad = jnp.sum(cotangent.astype(F32), axis=0)
    grad_context = dot_t(cot_full, proj_weight).astype(BF16)
    grad_act_two = dot_t(grad_pre_low, up_weight)
    head_grads = []
    for head_num in range(heads_here):
        grad_slice = grad_context[:, head_num * HD : (head_num + 1) * HD]
        query_rows, key_rows, value_rows, context, attn_probs, probs_low = saved[head_num]
        grad_query, grad_keys, grad_values = head_backward(
            query_rows, key_rows, value_rows, context, grad_slice, attn_probs, probs_low
        )
        head_grads.append(rotate_rows(grad_query, cosine, sine, ROT, -1.0))
        head_grads.append(rotate_rows(grad_keys, cosine, sine, ROT, -1.0))
        head_grads.append(grad_values)
    grad_qkv = jnp.concatenate(head_grads, axis=1)
    qkv_bias_grad = jnp.sum(grad_qkv, axis=0)
    grad_qkv_low = grad_qkv.astype(BF16)
    if net.nd == 8 and context_all.shape[1] == TILE:
        down_grad, up_grad, qkv_grad, proj_grad = fused_grads(
            hidden_act, act_two, act_one, context_all, cot_full, grad_pre_low, grad_qkv_low
        )
    else:
        down_grad = weight_grad(net, hidden_act, cot_full)
        up_grad = weight_grad(net, act_two, grad_pre_low)
        proj_grad = weight_grad(net, context_all, cot_full)
        qkv_grad = weight_grad(net, act_one, grad_qkv_low)
    grad_act_one = dot_t(grad_qkv_low, qkv_weight)
    grad_in_one, gain_one, shift_one = norm_backward(grad_act_one, norm_params[0], normed, inverse)
    grad_in_two, gain_two, shift_two = norm_backward(grad_act_two, norm_params[2], normed, inverse)
    hidden_grad = cotangent.astype(F32) + net.scatter_sum(grad_in_one + grad_in_two)

    width = out_bias.shape[0]
    norm_terms = net.sum_small_tensor(jnp.concatenate([gain_one, shift_one, gain_two, shift_two]))
    norm_share = lax.dynamic_slice_in_dim(
        norm_terms.reshape(4, -1), lax.axis_index("tensor") * width, width, 1
    )
    small = net.sum_small(
        jnp.concatenate([qkv_bias_grad, up_bias_grad, out_bias_grad, norm_share.reshape(-1)])
    )
    sizes = [qkv_bias.shape[0], up_bias.shape[0]] + [width] * 5
    parts, at = [], 0
    for size in sizes:
        parts.append(small[at : at + size])
        at += size
    return (
        hidden_out,
        hidden_grad,
        parts[3],
        parts[4],
        parts[5],
        parts[6],
        qkv_grad,
        parts[0],
        proj_grad,
        up_grad,
        parts[1],
        down_grad,
        parts[2],
    )


def solution(mesh):
    net = Net(mesh)
    placed = (
        P("dp", "tensor"),
        P("dp", None),
        P("tensor"),
        P("tensor"),
        P("tensor"),
        P("tensor"),
        P(None, "tensor"),
        P("tensor"),
        P("tensor", None),
        P(None, "tensor"),
        P("tensor"),
        P("tensor", None),
        P("tensor"),
        P("dp", "tensor"),
    )

    def body(*args):
        return per_device(net, *args)

    return jax.shard_map(
        body,
        mesh=mesh,
        in_specs=placed,
        out_specs=(
            P("dp", "tensor"),
            P("dp", "tensor"),
            P("tensor"),
            P("tensor"),
            P("tensor"),
            P("tensor"),
            P(None, "tensor"),
            P("tensor"),
            P("tensor", None),
            P(None, "tensor"),
            P("tensor"),
            P("tensor", None),
            P("tensor"),
        ),
        check_vma=False,
    )
```

```python
import math

import jax
import jax.numpy as jnp
from jax import lax
from jax.experimental import pallas as pl
from jax.experimental.pallas import tpu as pltpu
from jax.sharding import PartitionSpec as P

HD = 256
ROT = 64


root_half = 0.7071067811865476
inv_root_tau = 0.3989422804014327
F32 = jnp.float32
BF16 = jnp.bfloat16


def norm_stats(values):
    average = jnp.mean(values, axis=1, keepdims=True)
    centred = values - average
    spread_sq = jnp.mean(centred * centred, axis=1, keepdims=True)
    inverse = lax.rsqrt(spread_sq + 1e-05)
    return (centred * inverse, inverse)


def norm_backward(grad_out, gain, normed, inverse):
    scaled = grad_out * gain[None, :]
    first_mean = jnp.mean(scaled, axis=1, keepdims=True)
    second_mean = jnp.mean(scaled * normed, axis=1, keepdims=True)
    grad_in = inverse * (scaled - first_mean - normed * second_mean)
    return (grad_in, jnp.sum(grad_out * normed, axis=0), jnp.sum(grad_out, axis=0))


def seq_positions(segment_row):
    indices = jnp.arange(segment_row.shape[0], dtype=jnp.int32)
    same = segment_row[:, None] == segment_row[None, :]
    earlier = same & (indices[None, :] < indices[:, None])
    return jnp.sum(earlier.astype(F32), axis=1)


def rotary_tables(positions, rot_dims):
    half_dims = rot_dims // 2
    exponent = jnp.arange(half_dims, dtype=F32) * (2.0 / rot_dims)
    inv_freq = jnp.exp(-exponent * math.log(10000.0))
    angles = positions[:, None] * inv_freq[None, :]
    return (jnp.cos(angles), jnp.sin(angles))


def rotate_rows(values, cosine, sine, rot_dims, direction):
    half_dims = rot_dims // 2
    first_half = values[:, :half_dims]
    second_half = values[:, half_dims:rot_dims]
    turned_first = first_half * cosine - direction * second_half * sine
    turned_second = second_half * cosine + direction * first_half * sine
    return jnp.concatenate([turned_first, turned_second, values[:, rot_dims:]], axis=1)


def gelu_exact(values):
    return 0.5 * values * (1.0 + lax.erf(values * root_half))


def gelu_slope(values):
    return (
        0.5 * (1.0 + lax.erf(values * root_half))
        + values * jnp.exp(-0.5 * values * values) * inv_root_tau
    )


def dot(a, b):
    return jnp.dot(a, b, preferred_element_type=F32)


def dot_t(a, b):
    return lax.dot_general(a, b, (((1,), (1,)), ((), ())), preferred_element_type=F32)


def t_dot(a, b):
    return lax.dot_general(a, b, (((0,), (0,)), ((), ())), preferred_element_type=F32)


def head_forward(query_rows, key_rows, value_rows, allowed):
    score_scale = 1.0 / math.sqrt(query_rows.shape[1])
    scores = jnp.where(allowed, dot_t(query_rows, key_rows) * score_scale, -1e30)
    row_max = jnp.max(scores, axis=1, keepdims=True)
    log_total = row_max + jnp.log(jnp.sum(jnp.exp(scores - row_max), axis=1, keepdims=True))
    attn_probs = jnp.exp(scores - log_total)
    probs_low = attn_probs.astype(BF16)
    context = dot(probs_low, value_rows).astype(BF16)
    return (context, attn_probs, probs_low)


def head_backward(query_rows, key_rows, value_rows, context, grad_context, attn_probs, probs_low):
    score_scale = 1.0 / math.sqrt(query_rows.shape[1])
    grad_probs = dot_t(grad_context, value_rows)
    delta_rows = jnp.sum(
        grad_context.astype(F32) * context.astype(F32), axis=1, keepdims=True
    )
    grad_scores = (attn_probs * (grad_probs - delta_rows) * score_scale).astype(BF16)
    grad_query = dot(grad_scores, key_rows)
    grad_keys = t_dot(grad_scores, query_rows)
    grad_values = t_dot(probs_low, grad_context)
    return (grad_query, grad_keys, grad_values)


class Net:
    def __init__(self, mesh):
        self.nd = mesh.shape["dp"]
        self.nt = mesh.shape["tensor"]
        self.bits = self.nd.bit_length() - 1
        assert 1 << self.bits == self.nd

    def swap(self, value, bit):
        pairs = [(i, i ^ (1 << bit)) for i in range(self.nd)]
        return lax.ppermute(value, "dp", pairs)

    def swap_tensor(self, value, k):
        pairs = [(i, i ^ k) for i in range(self.nt)]
        return lax.ppermute(value, "tensor", pairs)

    def shift(self, value):
        pairs = [(i, (i + 1) % self.nt) for i in range(self.nt)]
        return lax.ppermute(value, "tensor", pairs)

    def gather(self, value, splits):
        rows = value.shape[0] // splits
        held = [[value[i * rows : (i + 1) * rows]] for i in range(splits)]
        for _ in range(self.nt - 1):
            for part in held:
                part.append(self.shift(part[-1]))
        me = lax.axis_index("tensor")
        done = []
        for part in held:
            slots = []
            for slot in range(self.nt):
                which = lax.rem(me - slot + self.nt, self.nt)
                chosen = part[0]
                for k in range(1, self.nt):
                    chosen = jnp.where(which == k, part[k], chosen)
                slots.append(chosen)
            done.append(jnp.concatenate(slots, axis=1))
        return jnp.concatenate(done, axis=0)

    def scatter_sum(self, value):
        me = lax.axis_index("tensor")
        width = value.shape[1] // self.nt
        total = lax.dynamic_slice_in_dim(value, me * width, width, 1)
        for k in range(1, self.nt):
            there = jnp.bitwise_xor(me, k)
            block = lax.dynamic_slice_in_dim(value, there * width, width, 1).astype(BF16)
            total = total + self.swap_tensor(block, k).astype(F32)
        return total

    def sum_small(self, value):
        for bit in range(self.bits):
            value = value + self.swap(value, bit)
        return value

    def sum_small_tensor(self, value):
        k = 1
        while k < self.nt:
            value = value + self.swap_tensor(value, k)
            k *= 2
        return value


def flow_orders(bits):
    others = list(range(1, bits))
    return [others, others[::-1]]


def weight_grad(net, left, right):
    me = lax.axis_index("dp")
    bit_of = [jnp.bitwise_and(jnp.right_shift(me, b), 1) for b in range(net.bits)]
    rows = left.shape[1]
    orders = flow_orders(net.bits)

    def product(start, count):
        return t_dot(lax.dynamic_slice_in_dim(left, start, count, 1), right)

    half = rows // 2
    quarter = half // 2
    away = product((1 - bit_of[0]) * half, half).astype(BF16)
    arrived = net.swap(away, 0)
    base = bit_of[0] * half
    owned = []
    for flow, order in enumerate(orders):
        size = quarter // 2
        first = order[0]
        offset = flow * quarter
        send_at = offset + (1 - bit_of[first]) * size
        keep_at = offset + bit_of[first] * size
        send = product(base + send_at, size) + lax.dynamic_slice_in_dim(
            arrived, send_at, size, 0
        ).astype(F32)
        got = net.swap(send.astype(BF16), first)
        keep = product(base + keep_at, size) + lax.dynamic_slice_in_dim(
            arrived, keep_at, size, 0
        ).astype(F32)
        for bit in order[1:]:
            size //= 2
            here, there = bit_of[bit] * size, (1 - bit_of[bit]) * size
            send = lax.dynamic_slice_in_dim(keep, there, size, 0) + lax.dynamic_slice_in_dim(
                got, there, size, 0
            ).astype(F32)
            keep = lax.dynamic_slice_in_dim(keep, here, size, 0) + lax.dynamic_slice_in_dim(
                got, here, size, 0
            ).astype(F32)
            got = net.swap(send.astype(BF16), bit)
        owned.append((keep + got.astype(F32)).astype(BF16))
    pieces = []
    for flow, order in enumerate(orders):
        have = [owned[flow]]
        for bit in order[::-1]:
            have = have + [net.swap(piece, bit) for piece in have]
        have = have + [net.swap(piece, 0) for piece in have]
        pieces.append(have)
    return place_pieces(net, pieces, rows)


def place_pieces(net, pieces, rows):
    orders = flow_orders(net.bits)
    flat = [piece for flow in pieces for piece in flow]
    count = len(flat)
    size, columns = flat[0].shape
    dtype = F32

    def body(*refs):
        ins, out, wide, low, in_sem, out_sem = (
            refs[:count], refs[count], refs[count + 1], refs[count + 2], refs[-2], refs[-1]
        )
        me = lax.axis_index("dp")
        mine = [jnp.bitwise_and(jnp.right_shift(me, b), 1) for b in range(net.bits)]

        def row_of(index):
            flow, k = divmod(index, count // 2)
            order = orders[flow]
            levels = [mine[b] for b in order]
            depth = len(order)
            digits = []
            for level in range(depth):
                flip = (k >> (depth - 1 - level)) & 1
                digits.append(1 - levels[level] if flip else levels[level])
            core = 1 - mine[0] if (k >> depth) & 1 else mine[0]
            block = core * 2 + flow
            for digit in digits:
                block = block * 2 + digit
            return pl.multiple_of(block * size, size)

        def load(i):
            return pltpu.make_async_copy(ins[i], low.at[i % 2], in_sem.at[i % 2])

        def store(i):
            return pltpu.make_async_copy(
                wide.at[i % 2], out.at[pl.ds(row_of(i), size), :], out_sem.at[i % 2]
            )

        load(0).start()
        for i in range(count):
            if i + 1 < count:
                load(i + 1).start()
            load(i).wait()
            if i >= 2:
                store(i - 2).wait()
            wide[i % 2] = low[i % 2].astype(dtype)
            store(i).start()
        for i in range(max(0, count - 2), count):
            store(i).wait()

    return pl.pallas_call(
        body,
        out_shape=jax.ShapeDtypeStruct((rows, columns), dtype),
        in_specs=[pl.BlockSpec(memory_space=pl.ANY)] * count,
        out_specs=pl.BlockSpec(memory_space=pl.ANY),
        scratch_shapes=[
            pltpu.VMEM((2, size, columns), dtype),
            pltpu.VMEM((2, size, columns), BF16),
            pltpu.SemaphoreType.DMA((2,)),
            pltpu.SemaphoreType.DMA((2,)),
        ],
        name="place_pieces",
        cost_estimate=pl.CostEstimate(
            flops=rows * columns, bytes_accessed=rows * columns * 6, transcendentals=0
        ),
    )(*flat)


MESH_ID = pl.DeviceIdType.MESH
TILE = 512
PIECE = 128
DEPTH = 6
SLOTS = 5
VMEM_LIMIT = 67_000_000


def start(index, unit):
    return pl.multiple_of(index * unit, unit)


class Ring:
    def __init__(self, part, recv0, recv1, recv2, ssem, rsem):
        self.part, self.recv0, self.recv1, self.recv2 = part, recv0, recv1, recv2
        self.ssem, self.rsem = ssem, rsem
        me = lax.axis_index("dp")
        self.me = me
        self.bit = [lax.rem(lax.div(me, 1 << b), 2) for b in range(3)]
        self.dests = []

    def partner(self, bit):
        return {"dp": self.me + (1 - 2 * self.bit[bit]) * (1 << bit)}

    def axes(self, flow):
        return (1, 2) if flow == 0 else (2, 1)

    def piece(self, flow, core, a, b):
        first, second = self.axes(flow)

        def digit(bit, flip):
            return 1 - self.bit[bit] if flip else self.bit[bit]

        return digit(0, core) * 8 + flow * 4 + digit(first, a) * 2 + digit(second, b)

    def send(self, src, dst, slot, s, r, bit):
        return pltpu.make_async_remote_copy(
            src_ref=src,
            dst_ref=dst,
            send_sem=self.ssem.at[slot, s],
            recv_sem=self.rsem.at[slot, r],
            device_id=self.partner(bit),
            device_id_type=MESH_ID,
        )

    def rows(self, first, count):
        return pl.ds(pl.multiple_of(first, PIECE), count)

    def add(self, i, first, source, at, count):
        part, slot = self.part, i % SLOTS

        @pl.loop(0, count // PIECE)
        def _(k):
            here = self.rows(first + k * PIECE, PIECE)
            there = self.rows(at + k * PIECE, PIECE)
            part[slot, here, :] = (
                part[slot, here, :].astype(F32) + source[there, :].astype(F32)
            ).astype(BF16)

    def copy0(self, i):
        slot = i % DEPTH
        away = (1 - self.bit[0]) * 1024
        src = self.part.at[i % SLOTS, self.rows(away, 1024)]
        return self.send(src, self.recv0.at[slot], slot, 0, 0, 0)

    def copy1(self, i, flow):
        slot = i % DEPTH
        a = self.axes(flow)[0]
        first = self.bit[0] * 1024 + flow * 512 + (1 - self.bit[a]) * 256
        src = self.part.at[i % SLOTS, self.rows(first, 256)]
        return self.send(src, self.recv1.at[slot, flow], slot, 1 + flow, 1 + flow, a)

    def copy2(self, i, flow):
        slot = i % DEPTH
        b = self.axes(flow)[1]
        src = self.part.at[i % SLOTS, self.rows(self.piece(flow, 0, 0, 1) * PIECE, PIECE)]
        return self.send(src, self.recv2.at[slot, flow], slot, 3 + flow, 3 + flow, b)

    def out(self, i, index):
        return self.dests[i](index)

    def copy3(self, i, flow, which):
        slot = i % DEPTH
        own = self.piece(flow, 0, 0, 0)
        src = self.part.at[i % SLOTS, self.rows(own * PIECE, PIECE)]
        dst = self.out(i, own)
        s, r = 5 + flow * 8, 5 + flow * 7
        if which == 3:
            return pltpu.make_async_copy(src, dst, self.ssem.at[slot, s + 3])
        a, b = self.axes(flow)
        return self.send(src, dst, slot, s + which, r + (0, 1, 3)[which], (b, a, 0)[which])

    def copy4(self, i, flow, which):
        slot = i % DEPTH
        a = self.axes(flow)[0]
        ref = self.out(i, self.piece(flow, 0, 0, 1))
        s, r = 9 + flow * 8, 5 + flow * 7
        return self.send(ref, ref, slot, s + which, r + (2, 4)[which], (a, 0)[which])

    def copy5(self, i, flow, which):
        slot = i % DEPTH
        ref = self.out(i, self.piece(flow, 0, 1, which))
        return self.send(ref, ref, slot, 11 + flow * 8 + which, 10 + flow * 7 + which, 0)

    def stage0(self, i):
        self.copy0(i).start()

    def stage1(self, i):
        slot = i % DEPTH
        self.copy0(i).wait()
        half = self.bit[0] * 1024
        for away in (1, 0):
            for flow in range(2):
                bit = self.bit[self.axes(flow)[0]]
                first = flow * 512 + (1 - bit if away else bit) * 256
                self.add(i, half + first, self.recv0.at[slot], first, 256)
                if away:
                    self.copy1(i, flow).start()

    def stage2(self, i):
        slot = i % DEPTH
        for flow in range(2):
            self.copy1(i, flow).wait()
            bit = self.bit[self.axes(flow)[1]]
            source = self.recv1.at[slot, flow]
            self.add(i, self.piece(flow, 0, 0, 1) * PIECE, source, (1 - bit) * PIECE, PIECE)
            self.copy2(i, flow).start()
            self.add(i, self.piece(flow, 0, 0, 0) * PIECE, source, bit * PIECE, PIECE)

    def stage3(self, i):
        slot = i % DEPTH
        for flow in range(2):
            self.copy2(i, flow).wait()
            self.add(i, self.piece(flow, 0, 0, 0) * PIECE, self.recv2.at[slot, flow], 0, PIECE)
            for which in range(4):
                self.copy3(i, flow, which).start()

    def stage4(self, i):
        for flow in range(2):
            self.copy3(i, flow, 0).wait_recv()
            for which in range(2):
                self.copy4(i, flow, which).start()
        for flow in range(2):
            for which in range(3):
                self.copy3(i, flow, which).wait_send()
            self.copy3(i, flow, 3).wait()

    def stage5(self, i):
        for flow in range(2):
            self.copy3(i, flow, 1).wait_recv()
            self.copy4(i, flow, 0).wait()
            for which in range(2):
                self.copy5(i, flow, which).start()

    def stage6(self, i):
        for flow in range(2):
            self.copy3(i, flow, 2).wait_recv()
            self.copy4(i, flow, 1).wait()
            for which in range(2):
                self.copy5(i, flow, which).wait()


def wide_dest(ref, column):
    def at(index):
        return ref.at[pl.ds(start(index, PIECE), PIECE), pl.ds(start(column, TILE), TILE)]

    return at


def tall_dest(ref, row):
    def at(index):
        down = row * TILE + lax.rem(index, 4) * PIECE
        across = lax.div(index, 4)
        return ref.at[
            pl.ds(pl.multiple_of(down, PIECE), PIECE), pl.ds(start(across, TILE), TILE)
        ]

    return at


INPUTS = (
    "x_in", "cot_in", "seg", "up_w", "down_w", "qkv_w", "proj_w", "up_b", "qkv_b", "out_b",
    "gain1", "bias1", "gain2", "bias2",
)
OUTPUTS = ("down_o", "up_o", "qkv_o", "proj_o", "hid_o", "grad_o", "small_o")
SCRATCH = (
    ("xg", (4, 512, 512), BF16),
    ("info", (4, 8, 512), F32),
    ("cg", (4, 512, 512), BF16),
    ("act1", (4, 512, 512), BF16),
    ("act2", (4, 512, 512), BF16),
    ("hact", (4, 512, 512), BF16),
    ("pre", (4, 512, 512), F32),
    ("gpre", (4, 512, 512), BF16),
    ("gqkv", (3, 512, 512), BF16),
    ("qkvb", (6, 512, 256), BF16),
    ("ctx", (512, 512), BF16),
    ("gctx", (512, 512), BF16),
    ("probs", (512, 512), BF16),
    ("dscore", (512, 512), BF16),
    ("wbuf", (2, 2048, 512), BF16),
    ("pbuf", (4, 512, 512), BF16),
    ("ysend", (3, 512, 512), BF16),
    ("yrecv", (3, 512, 512), BF16),
    ("dsend", (3, 512, 512), BF16),
    ("drecv", (3, 512, 512), BF16),
    ("table", (2, 512, 128), F32),
    ("seg_col", (512, 128), F32),
    ("stat", (4, 512, 128), F32),
    ("hid", (512, 512), F32),
    ("grad", (512, 512), F32),
    ("small", (24, 512), F32),
    ("srecv", (5, 24, 512), F32),
    ("part", (SLOTS, 2048, TILE), BF16),
    ("recv0", (DEPTH, 1024, TILE), BF16),
    ("recv1", (DEPTH, 2, 256, TILE), BF16),
    ("recv2", (DEPTH, 2, PIECE, TILE), BF16),
)
SEMS = (
    ("ssem", (DEPTH, 21)),
    ("rsem", (DEPTH, 19)),
    ("ns", (3,)),
    ("nr", (3,)),
    ("xs", (3, 4)),
    ("xr", (3, 4)),
    ("cs", (3,)),
    ("cr", (3,)),
    ("wsem", (2, 4)),
    ("psem", (4,)),
    ("own", (2,)),
    ("ys", (3,)),
    ("yr", (3,)),
    ("ds", (3,)),
    ("dr", (3,)),
    ("ms", (5,)),
    ("mr", (5,)),
    ("last", (3,)),
)
SCALE = 1.0 / 16.0


class Refs:
    pass


def block_kernel(*refs):
    r = Refs()
    names = INPUTS + OUTPUTS + tuple(s[0] for s in SCRATCH) + tuple(s[0] for s in SEMS)
    for name, ref in zip(names, refs):
        setattr(r, name, ref)
    ring = Ring(r.part, r.recv0, r.recv1, r.recv2, r.ssem, r.rsem)
    core = ring.bit[0]
    me = lax.axis_index("tensor")
    width = 2048.0

    def other(k):
        return lax.rem(me + k, 4)

    barrier = pltpu.get_barrier_semaphore()
    friends = [ring.partner(b) for b in range(3)] + [{"tensor": other(k)} for k in (1, 2, 3)]
    home_x = pltpu.make_async_copy(r.x_in, r.xg.at[me], r.own.at[0])
    home_c = pltpu.make_async_copy(r.cot_in, r.cg.at[me], r.own.at[1])
    home_x.start()
    home_c.start()
    for friend in friends:
        pl.semaphore_signal(barrier, inc=1, device_id=friend, device_id_type=MESH_ID)

    for n, ref in enumerate((r.gain1, r.bias1, r.gain2, r.bias2)):
        r.info[me, n : n + 1, :] = ref[...].astype(F32).reshape(1, 512)
    lane = lax.broadcasted_iota(jnp.int32, (128, 128), 1)
    home_x.wait()

    @pl.loop(0, 4)
    def _(b):
        rows = pl.ds(start(b, 128), 128)
        value = r.xg[me, rows, :].astype(F32)
        mean = jnp.sum(value, axis=1, keepdims=True) / 512.0
        centred = value - mean
        spread = jnp.sum(centred * centred, axis=1, keepdims=True)
        r.stat[2, rows, :] = jnp.where(lane < 64, mean, spread)

    turned = jnp.transpose(r.stat[2])
    r.info[me, 4:5, :] = turned[0:1]
    r.info[me, 5:6, :] = turned[64:65]
    r.info[me, 6:8, :] = jnp.zeros((2, 512), F32)
    pl.semaphore_wait(barrier, len(friends))

    def remote(src, dst, ssem, rsem, where):
        return pltpu.make_async_remote_copy(
            src_ref=src, dst_ref=dst, send_sem=ssem, recv_sem=rsem,
            device_id=where, device_id_type=MESH_ID,
        )

    def block_rows(b):
        return pl.ds(128 * b, 128)

    def info_copy(k):
        ref = r.info.at[other(4 - k)]
        return remote(ref, ref, r.ns.at[k], r.nr.at[k], {"tensor": other(1)})


    def x_copy(k, b):
        slot = other(4 - k)
        rows = block_rows(b)
        ref = r.xg.at[slot, rows]
        return remote(ref, ref, r.xs.at[k, b], r.xr.at[k, b], {"tensor": other(1)})

    def cot_copy(k):
        slot = other(4 - k)
        ref = r.cg.at[slot]
        return remote(ref, ref, r.cs.at[k], r.cr.at[k], {"tensor": other(1)})

    info_copy(0).start()
    x_copy(0, 0).start()
    for k in (1, 2):
        info_copy(k - 1).wait_recv()
        info_copy(k).start()
        x_copy(0, k).start()
    x_copy(0, 3).start()

    def columns_of(ref, block):
        return lambda slot: [
            pltpu.make_async_copy(
                ref.at[:, pl.ds(start(block, 512), 512)], r.wbuf.at[slot], r.wsem.at[slot, 0]
            )
        ]

    def rows_of(ref, block, count):
        return lambda slot: [
            pltpu.make_async_copy(
                ref.at[pl.ds(start(block, 512), 512), pl.ds(k * 512, 512)],
                r.wbuf.at[slot, pl.ds(k * 512, 512)],
                r.wsem.at[slot, k],
            )
            for k in range(count)
        ]

    halves = [2 * (1 - core), 2 * (1 - core) + 1, 2 * core, 2 * core + 1]
    loads = [rows_of(r.up_w, other(4 - k), 4) for k in range(4)]
    loads += [columns_of(r.qkv_w, c) for c in range(3)]
    loads += [rows_of(r.down_w, j, 4) for j in range(4)]
    loads += [columns_of(r.down_w, other(k)) for k in (1, 2, 3, 0)]
    for s in range(4):
        loads += [rows_of(r.up_w, s, 4), rows_of(r.qkv_w, s, 3)]
    used = [0]

    def begin(n):
        for copy in loads[n](n % 2):
            copy.start()

    def weights():
        n = used[0]
        used[0] = n + 1
        for copy in loads[n](n % 2):
            copy.wait()
        if n + 1 < len(loads):
            begin(n + 1)
        return r.wbuf.at[n % 2]

    begin(0)
    proj_loads = [
        pltpu.make_async_copy(r.proj_w.at[:, pl.ds(s * 512, 512)], r.pbuf.at[s], r.psem.at[s])
        for s in range(4)
    ]
    for copy in proj_loads:
        copy.start()

    r.small[...] = jnp.zeros(r.small.shape, F32)
    seg_row = r.seg[...].astype(F32)
    r.seg_col[...] = jnp.transpose(jnp.broadcast_to(seg_row, (128, 512)))

    def visible(rows, first):
        col = lax.broadcasted_iota(jnp.int32, (128, 512), 1)
        row = lax.broadcasted_iota(jnp.int32, (128, 512), 0) + first
        return (r.seg_col[rows, 0:1] == seg_row) & (col <= row)

    @pl.loop(0, 4)
    def _(b):
        rows = pl.ds(start(b, 128), 128)
        seen = jnp.sum(visible(rows, b * 128).astype(F32), axis=1, keepdims=True)
        step = lax.rem(lane, ROT // 2).astype(F32) * (2.0 / ROT)
        angle = (seen - 1.0) * jnp.exp(-step * math.log(10000.0))
        r.table[0, rows, :] = jnp.where(lane < ROT, jnp.cos(angle), 1.0)
        sine = jnp.sin(angle)
        r.table[1, rows, :] = jnp.where(
            lane < ROT // 2, -sine, jnp.where(lane < ROT, sine, 0.0)
        )

    home_c.wait()
    r.small[23:24, :] = jnp.sum(r.cg[me].astype(F32), axis=0, keepdims=True)
    info_copy(2).wait_recv()
    mean = sum(r.info[s, 4:5, :] for s in range(4)) / 4.0
    spread = sum(r.info[s, 5:6, :] for s in range(4))
    for s in range(4):
        off = r.info[s, 4:5, :] - mean
        spread += 512.0 * (off * off)
    inverse = lax.rsqrt(spread / width + 1e-05)
    r.stat[0] = jnp.transpose(jnp.broadcast_to(mean, (128, 512)))
    r.stat[1] = jnp.transpose(jnp.broadcast_to(inverse, (128, 512)))

    def normed_of(s, rows):
        values = r.xg[s, rows, :].astype(F32)
        return (values - r.stat[0, rows, 0:1]) * r.stat[1, rows, 0:1]

    def act_block(s, b):
        @pl.loop(0, 2)
        def _(half):
            rows = pl.ds(start(2 * b + half, 64), 64)
            normed = normed_of(s, rows)
            p = r.info[s]
            r.act1[s, rows, :] = (normed * p[0:1] + p[1:2]).astype(BF16)
            r.act2[s, rows, :] = (normed * p[2:3] + p[3:4]).astype(BF16)

    def up_part(s, w, first):
        @pl.loop(0, 8)
        def _(n):
            j, rows = lax.div(n, 2), pl.ds(start(lax.rem(n, 2), 256), 256)
            value = dot(r.act2[s, rows, :], w[pl.ds(start(j, 512), 512), :])
            if first:
                bias = r.up_b[pl.ds(start(j, 512), 512)].astype(F32).reshape(1, 512)
                r.pre[j, rows, :] = value + bias
            else:
                r.pre[j, rows, :] += value

    for k in range(4):
        shard = other(4 - k)
        for b in range(4):
            if k:
                x_copy(k - 1, b).wait_recv()
                if k < 3:
                    x_copy(k, b).start()
            if k == 3:
                act_block(shard, b)
        if k == 2:
            cot_copy(0).start()
        if k < 3:
            for b in range(4):
                act_block(shard, b)
            up_part(shard, weights(), k == 0)
    last_shard = other(1)
    last_w = weights()

    def up_block(j):
        @pl.loop(0, 2)
        def _(b):
            rows = pl.ds(start(b, 256), 256)
            value = r.pre[j, rows, :] + dot(
                r.act2[last_shard, rows, :], last_w[pl.ds(start(j, 512), 512), :]
            )
            r.pre[j, rows, :] = value
            r.hact[j, rows, :] = gelu_exact(value).astype(BF16)

    def product(i, left_of, right_of, between=None):
        slot = i % SLOTS

        def half(which):
            @pl.loop(0, 4)
            def _(k):
                tile = which * 4 + k
                r.part[slot, pl.ds(start(tile, 256), 256), :] = t_dot(
                    left_of(tile), right_of(tile)
                ).astype(BF16)

        half(1 - core)
        ring.stage0(i)
        if between is not None:
            between()
        half(core)

    def columns(ref, first, count):
        return ref[:, pl.ds(pl.multiple_of(first, 256), count)]

    jobs = []

    def down_job(k):
        shard = other(4 - k)
        ring.dests.append(wide_dest(r.down_o, shard))

        def run(i):
            if k == 0:
                up_block(halves[0])
                up_block(halves[1])

                def between():
                    up_block(halves[2])
                    up_block(halves[3])
            else:
                between = None
            product(
                i,
                lambda t: columns(r.hact.at[lax.div(t, 2)], lax.rem(t, 2) * 256, 256),
                lambda t: r.cg[shard],
                between,
            )

        jobs.append(run)

    def wide_job(left, right, out, column):
        ring.dests.append(wide_dest(out, column))
        jobs.append(
            lambda i: product(
                i,
                lambda t: columns(left.at[lax.div(t, 2)], lax.rem(t, 2) * 256, 256),
                lambda t: right[column],
            )
        )

    def tall_job(left, out):
        ring.dests.append(tall_dest(out, 0))
        jobs.append(
            lambda i: product(
                i,
                lambda t: columns(left, lax.rem(t, 2) * 256, 256),
                lambda t: r.cg[lax.div(t, 2)],
            )
        )

    for k in range(4):
        down_job(k)
    for j in range(4):
        wide_job(r.act2, r.gpre, r.up_o, j)
    tall_job(r.ctx, r.proj_o)
    for c in range(3):
        wide_job(r.act1, r.gqkv, r.qkv_o, c)

    def turn(value, rows, direction):
        count = value.shape[0]
        head = value[:, :128]
        here = lax.broadcasted_iota(jnp.int32, (count, 128), 1)
        mate = jnp.where(
            here < ROT // 2,
            pltpu.roll(head, 128 - ROT // 2, 1),
            pltpu.roll(head, ROT // 2, 1),
        )
        head = head * r.table[0, rows, :] + direction * (mate * r.table[1, rows, :])
        return jnp.concatenate([head, value[:, 128:]], axis=1)

    def qkv_block(c):
        w = weights()

        @pl.loop(0, 2)
        def _(b):
            rows = pl.ds(start(b, 256), 256)
            value = r.qkv_b[c * 512 : (c + 1) * 512].astype(F32).reshape(1, 512)
            for s in range(4):
                value = value + dot(r.act1[s, rows, :], w[s * 512 : (s + 1) * 512, :])
            for k in range(2):
                p = 2 * c + k
                one = value[:, k * 256 : (k + 1) * 256]
                if p % 3 != 2:
                    one = turn(one, rows, 1.0)
                r.qkvb[p, rows, :] = one.astype(BF16)

    def grad_context():
        for copy in proj_loads:
            copy.wait()

        @pl.loop(0, 2)
        def _(b):
            rows = pl.ds(start(b, 256), 256)
            total = sum(dot_t(r.cg[s, rows, :], r.pbuf[s]) for s in range(4))
            r.gctx[rows, :] = total.astype(BF16)

    def keep_qkv(p, rows, value):
        c, across = p // 2, slice((p % 2) * 256, (p % 2) * 256 + 256)
        r.small[20 + c : 21 + c, across] += jnp.sum(value, axis=0, keepdims=True)
        r.gqkv[c, rows, across] = value.astype(BF16)

    def attention(h):
        q, k, v = r.qkvb.at[3 * h], r.qkvb.at[3 * h + 1], r.qkvb.at[3 * h + 2]
        across = slice(h * HD, (h + 1) * HD)

        @pl.loop(0, 4)
        def _(b):
            rows = pl.ds(start(b, 128), 128)
            scores = jnp.where(
                visible(rows, b * 128), dot_t(q[rows, :], k[...]) * SCALE, -1e30
            )
            top = jnp.max(scores, axis=1, keepdims=True)
            total = jnp.sum(jnp.exp(scores - top), axis=1, keepdims=True)
            probs = jnp.exp(scores - (top + jnp.log(total)))
            low = probs.astype(BF16)
            r.probs[rows, :] = low
            context = dot(low, v[...]).astype(BF16)
            r.ctx[rows, across] = context
            grad = r.gctx[rows, across]
            delta = jnp.sum(grad.astype(F32) * context.astype(F32), axis=1, keepdims=True)
            dscore = (probs * (dot_t(grad, v[...]) - delta) * SCALE).astype(BF16)
            r.dscore[rows, :] = dscore
            keep_qkv(3 * h, rows, turn(dot(dscore, k[...]), rows, -1.0))

        @pl.loop(0, 2)
        def _(b):
            rows = pl.ds(start(b, 256), 256)
            keep_qkv(
                3 * h + 1, rows, turn(t_dot(columns(r.dscore, b * 256, 256), q[...]), rows, -1.0)
            )
            keep_qkv(3 * h + 2, rows, t_dot(columns(r.probs, b * 256, 256), r.gctx[:, across]))

    def gpre_block(j):
        w = weights()

        @pl.loop(0, 2)
        def _(b):
            rows = pl.ds(start(b, 256), 256)
            total = sum(
                dot_t(r.cg[s, rows, :], w[s * 512 : (s + 1) * 512, :]) for s in range(4)
            )
            total = total * gelu_slope(r.pre[j, rows, :])
            r.small[16 + j : 17 + j, :] += jnp.sum(total, axis=0, keepdims=True)
            r.gpre[j, rows, :] = total.astype(BF16)

    def z_copy(send, recv, ssem, rsem, k):
        return remote(
            send.at[k - 1], recv.at[k - 1], ssem.at[k - 1], rsem.at[k - 1], {"tensor": other(k)}
        )

    def y_copy(k):
        return z_copy(r.ysend, r.yrecv, r.ys, r.yr, k)

    def d_copy(k):
        return z_copy(r.dsend, r.drecv, r.ds, r.dr, k)

    def y_block(k):
        w = weights()
        shard = other(k)

        @pl.loop(0, 2)
        def _(b):
            rows = pl.ds(start(b, 256), 256)
            total = dot(r.ctx[rows, :], r.pbuf[shard])
            for j in range(4):
                total += dot(r.hact[j, rows, :], w[j * 512 : (j + 1) * 512, :])
            if k:
                r.ysend[k - 1, rows, :] = total.astype(BF16)
            else:
                bias = r.out_b[...].astype(F32).reshape(1, 512)
                r.hid[rows, :] = total + r.xg[me, rows, :].astype(F32) + bias

        if k:
            y_copy(k).start()

    def back_block(s):
        p = r.info[s]
        w_up = weights()

        @pl.loop(0, 2)
        def _(b):
            rows = pl.ds(start(b, 256), 256)
            total = dot_t(r.gpre[0, rows, :], w_up[0:512, :])
            for j in range(1, 4):
                total += dot_t(r.gpre[j, rows, :], w_up[j * 512 : (j + 1) * 512, :])
            normed = normed_of(s, rows)
            r.small[8 + s : 9 + s, :] += jnp.sum(total * normed, axis=0, keepdims=True)
            r.small[12 + s : 13 + s, :] += jnp.sum(total, axis=0, keepdims=True)
            r.pre[s, rows, :] = total * p[2:3]

        w_qkv = weights()

        @pl.loop(0, 2)
        def _(b):
            rows = pl.ds(start(b, 256), 256)
            total = dot_t(r.gqkv[0, rows, :], w_qkv[0:512, :])
            for c in range(1, 3):
                total += dot_t(r.gqkv[c, rows, :], w_qkv[c * 512 : (c + 1) * 512, :])
            normed = normed_of(s, rows)
            r.small[s : 1 + s, :] += jnp.sum(total * normed, axis=0, keepdims=True)
            r.small[4 + s : 5 + s, :] += jnp.sum(total, axis=0, keepdims=True)
            both = r.pre[s, rows, :] + total * p[0:1]
            r.pre[s, rows, :] = both
            one = jnp.sum(both, axis=1, keepdims=True)
            two = jnp.sum(both * normed, axis=1, keepdims=True)
            if s:
                one += r.stat[2, rows, 0:1]
                two += r.stat[3, rows, 0:1]
            r.stat[2, rows, :] = jnp.broadcast_to(one, (256, 128))
            r.stat[3, rows, :] = jnp.broadcast_to(two, (256, 128))

    def finish_rows():
        for k in (1, 2, 3, 0):
            shard = other(k)

            @pl.loop(0, 4)
            def _(b):
                rows = pl.ds(start(b, 128), 128)
                one, two = r.stat[2, rows, 0:1] / width, r.stat[3, rows, 0:1] / width
                normed = normed_of(shard, rows)
                value = r.stat[1, rows, 0:1] * (r.pre[shard, rows, :] - one - normed * two)
                if k:
                    r.dsend[k - 1, rows, :] = value.astype(BF16)
                else:
                    r.grad[rows, :] = value + r.cg[me, rows, :].astype(F32)

            if k:
                d_copy(k).start()

    def collect(out, recv, copy):
        for k in (1, 2, 3):
            copy(k).wait()

        @pl.loop(0, 4)
        def _(b):
            rows = pl.ds(start(b, 128), 128)
            total = out[rows, :]
            for k in range(3):
                total += recv[k, rows, :].astype(F32)
            out[rows, :] = total

    bit0, bit1 = lax.rem(me, 2), lax.div(me, 2)

    def small_copy(n):
        rows = pl.ds(0, 16 if n < 2 else 24)
        if n == 0:
            where = {"tensor": me + 1 - 2 * bit0}
        elif n == 1:
            where = {"tensor": me + 2 - 4 * bit1}
        else:
            where = ring.partner(n - 2)
        return remote(
            r.small.at[rows], r.srecv.at[n, rows], r.ms.at[n], r.mr.at[n], where
        )

    def small_done(n):
        small_copy(n).wait()
        rows = slice(0, 16 if n < 2 else 24)
        r.small[rows, :] += r.srecv[n, rows, :]

    def small_step(n):
        if n:
            small_done(n - 1)
        if n < 5:
            small_copy(n).start()
        else:
            home(2).start()

    def home(n):
        pairs = ((r.hid, r.hid_o), (r.grad, r.grad_o), (r.small, r.small_o))
        return pltpu.make_async_copy(*pairs[n], r.last.at[n])

    def finish_hidden():
        collect(r.hid, r.yrecv, y_copy)
        home(0).start()

    def finish_grad():
        collect(r.grad, r.drecv, d_copy)
        home(1).start()

    def settle():
        for k in range(3):
            for b in range(4):
                x_copy(k, b).wait_send()
            cot_copy(k).wait_send()
            info_copy(k).wait_send()

    extras = {
        3: [lambda: gpre_block(0), lambda: gpre_block(1), grad_context],
        4: [lambda: gpre_block(2), lambda: attention(0)],
        5: [lambda: gpre_block(3), lambda: attention(1)],
        6: [lambda: y_block(1), lambda: y_block(2), lambda: y_block(3), lambda: y_block(0)],
        7: [lambda: back_block(0), lambda: back_block(1)],
        8: [lambda: back_block(2), lambda: back_block(3), finish_rows],
        9: [lambda: small_step(0)],
        10: [lambda: small_step(1)],
        11: [lambda: small_step(2)],
        12: [lambda: small_step(3), settle],
        13: [lambda: small_step(4)],
        14: [lambda: small_step(5), finish_hidden],
        15: [finish_grad],
    }
    count = len(jobs)
    stages = [ring.stage1, ring.stage2, ring.stage3, ring.stage4, ring.stage5, ring.stage6]
    reached = [0] * count

    def advance(i, stage):
        if reached[i] < stage:
            reached[i] = stage
            stages[stage - 1](i)

    def cot_step(k):
        cot_copy(k).wait_recv()
        if k < 2:
            cot_copy(k + 1).start()

    jobs[0](0)
    advance(0, 1)
    for c in range(3):
        qkv_block(c)
    cot_step(0)
    advance(0, 2)
    jobs[1](1)
    advance(1, 1)
    advance(0, 3)
    cot_step(1)
    jobs[2](2)
    advance(1, 2)
    advance(2, 1)
    advance(0, 4)
    advance(1, 3)
    cot_step(2)
    jobs[3](3)
    for step in range(3, count + DEPTH):
        if step > 3:
            for depth in range(1, DEPTH + 1):
                if 0 <= step - depth < count:
                    advance(step - depth, depth)
            if step < count:
                jobs[step](step)
        for extra in extras.get(step, []):
            extra()
    for n in range(3):
        home(n).wait()


def fused_block(
    hidden_in, cotangent, norm_params, segment_ids,
    up_weight, down_weight, qkv_weight, proj_weight, up_bias, qkv_bias, out_bias,
):
    rows, width = hidden_in.shape
    vmem, anywhere = pl.BlockSpec(memory_space=pltpu.VMEM), pl.BlockSpec(memory_space=pl.ANY)
    return pl.pallas_call(
        block_kernel,
        out_shape=[
            jax.ShapeDtypeStruct(down_weight.shape, BF16),
            jax.ShapeDtypeStruct(up_weight.shape, BF16),
            jax.ShapeDtypeStruct(qkv_weight.shape, BF16),
            jax.ShapeDtypeStruct(proj_weight.shape, BF16),
            jax.ShapeDtypeStruct((rows, width), F32),
            jax.ShapeDtypeStruct((rows, width), F32),
            jax.ShapeDtypeStruct((24, width), F32),
        ],
        in_specs=[anywhere] * 2 + [vmem] + [anywhere] * 4 + [vmem] * 7,
        out_specs=[anywhere] * 7,
        scratch_shapes=[pltpu.VMEM(shape, dtype) for _, shape, dtype in SCRATCH]
        + [pltpu.SemaphoreType.DMA(shape) for _, shape in SEMS],
        compiler_params=pltpu.CompilerParams(
            collective_id=0, has_side_effects=True, vmem_limit_bytes=VMEM_LIMIT
        ),
        name="fused_block",
    )(
        hidden_in, cotangent, segment_ids,
        up_weight, down_weight, qkv_weight, proj_weight,
        up_bias, qkv_bias, out_bias, *norm_params,
    )


FINISH_ROWS = 256
IN_SLOTS = 4
OUT_SLOTS = 4


def finish_kernel(
    down, up, qkv, proj, hid, grad, small,
    hid_o, grad_o, gain1_o, bias1_o, gain2_o, bias2_o, qkv_o, qkvb_o, proj_o, up_o, upb_o,
    down_o, outb_o, low, wide, rows_kept, sums, in_sem, out_sem, row_sem,
):
    rows_in = [
        pltpu.make_async_copy(hid, rows_kept.at[0], row_sem.at[0]),
        pltpu.make_async_copy(grad, rows_kept.at[1], row_sem.at[1]),
    ]
    rows_out = [
        pltpu.make_async_copy(rows_kept.at[0], hid_o, row_sem.at[2]),
        pltpu.make_async_copy(rows_kept.at[1], grad_o, row_sem.at[3]),
    ]
    sums_in = pltpu.make_async_copy(small, sums, row_sem.at[4])
    sums_in.start()
    blocks = []
    for src, dst in ((down, down_o), (up, up_o), (qkv, qkv_o), (proj, proj_o)):
        for n in range(src.shape[0] // FINISH_ROWS):
            blocks.append((src, dst, pl.ds(n * FINISH_ROWS, FINISH_ROWS), src.shape[1]))

    def load(n):
        src, _, rows, across = blocks[n]
        slot = n % IN_SLOTS
        return pltpu.make_async_copy(
            src.at[rows], low.at[slot, :, pl.ds(0, across)], in_sem.at[slot]
        )

    def store(n):
        _, dst, rows, across = blocks[n]
        slot = n % OUT_SLOTS
        return pltpu.make_async_copy(
            wide.at[slot, :, pl.ds(0, across)], dst.at[rows], out_sem.at[slot]
        )

    count = len(blocks)
    for n in range(IN_SLOTS - 1):
        load(n).start()
    for copy in rows_in:
        copy.start()
    me = lax.axis_index("tensor")
    sums_in.wait()
    for n, out in enumerate((gain1_o, bias1_o, gain2_o, bias2_o)):
        out[...] = sums[pl.ds(4 * n + me, 1), :].reshape(512)
    for n in range(4):
        upb_o[pl.ds(n * 512, 512)] = sums[16 + n : 17 + n, :].reshape(512)
    for n in range(3):
        qkvb_o[pl.ds(n * 512, 512)] = sums[20 + n : 21 + n, :].reshape(512)
    outb_o[...] = sums[23:24, :].reshape(512)
    for n in range(count):
        if n + IN_SLOTS - 1 < count:
            load(n + IN_SLOTS - 1).start()
        load(n).wait()
        if n >= OUT_SLOTS:
            store(n - OUT_SLOTS).wait()
        across = blocks[n][3]

        @pl.loop(0, FINISH_ROWS // 32)
        def _(b):
            rows = pl.ds(start(b, 32), 32)
            wide[n % OUT_SLOTS, rows, 0:across] = low[n % IN_SLOTS, rows, 0:across].astype(F32)

        store(n).start()
        if n < 2:
            rows_in[n].wait()
            rows_out[n].start()
    for n in range(count - OUT_SLOTS, count):
        store(n).wait()
    for copy in rows_out:
        copy.wait()


def finish(down, up, qkv, proj, hid, grad, small):
    def wide_like(array):
        return jax.ShapeDtypeStruct(array.shape, F32)

    def line(size):
        return jax.ShapeDtypeStruct((size,), F32)

    vmem, anywhere = pl.BlockSpec(memory_space=pltpu.VMEM), pl.BlockSpec(memory_space=pl.ANY)
    big = sum(array.size for array in (down, up, qkv, proj))
    return pl.pallas_call(
        finish_kernel,
        out_shape=[wide_like(hid), wide_like(grad)]
        + [line(512)] * 4
        + [wide_like(qkv), line(1536), wide_like(proj), wide_like(up), line(2048)]
        + [wide_like(down), line(512)],
        in_specs=[anywhere] * 7,
        out_specs=[anywhere] * 2 + [vmem] * 4
        + [anywhere, vmem, anywhere, anywhere, vmem, anywhere, vmem],
        scratch_shapes=[
            pltpu.VMEM((IN_SLOTS, FINISH_ROWS, 2048), BF16),
            pltpu.VMEM((OUT_SLOTS, FINISH_ROWS, 2048), F32),
            pltpu.VMEM((2, 512, 512), F32),
            pltpu.VMEM((24, 512), F32),
            pltpu.SemaphoreType.DMA((IN_SLOTS,)),
            pltpu.SemaphoreType.DMA((OUT_SLOTS,)),
            pltpu.SemaphoreType.DMA((5,)),
        ],
        compiler_params=pltpu.CompilerParams(vmem_limit_bytes=VMEM_LIMIT),
        cost_estimate=pl.CostEstimate(flops=big, bytes_accessed=6 * big, transcendentals=0),
        name="finish",
    )(down, up, qkv, proj, hid, grad, small)


def fits_kernel(net, hidden_in, qkv_weight, up_weight):
    return (
        (net.nd, net.nt) == (8, 4)
        and hidden_in.shape == (512, 512)
        and qkv_weight.shape == (2048, 1536)
        and up_weight.shape == (2048, 2048)
    )


def kernel_path(*args):
    return tuple(finish(*fused_block(*args)))


def per_device(
    net,
    hidden_in,
    segment_ids,
    norm1_gain,
    norm1_bias,
    norm2_gain,
    norm2_bias,
    qkv_weight,
    qkv_bias,
    proj_weight,
    up_weight,
    up_bias,
    down_weight,
    out_bias,
    cotangent,
):
    norm_stack = jnp.stack([norm1_gain, norm1_bias, norm2_gain, norm2_bias])
    if fits_kernel(net, hidden_in, qkv_weight, up_weight):
        return kernel_path(
            hidden_in, cotangent, (norm1_gain, norm1_bias, norm2_gain, norm2_bias), segment_ids,
            up_weight, down_weight, qkv_weight, proj_weight, up_bias, qkv_bias, out_bias,
        )
    full_rows = net.gather(hidden_in, 2)
    norm_full = net.gather(norm_stack, 1)
    cot_full = net.gather(cotangent, 2)
    norm_params = norm_full.astype(F32)
    segment_row = segment_ids[0]
    row_count = full_rows.shape[0]
    heads_here = qkv_weight.shape[1] // (3 * HD)
    normed, inverse = norm_stats(full_rows.astype(F32))
    act_one = (normed * norm_params[0][None, :] + norm_params[1][None, :]).astype(BF16)
    act_two = (normed * norm_params[2][None, :] + norm_params[3][None, :]).astype(BF16)

    pre_up = dot(act_two, up_weight) + up_bias.astype(F32)[None, :]
    hidden_act = gelu_exact(pre_up).astype(BF16)
    down_grad = weight_grad(net, hidden_act, cot_full)
    grad_pre = dot_t(cot_full, down_weight) * gelu_slope(pre_up)
    up_bias_grad = jnp.sum(grad_pre, axis=0)
    grad_pre_low = grad_pre.astype(BF16)
    up_grad = weight_grad(net, act_two, grad_pre_low)

    cosine, sine = rotary_tables(seq_positions(segment_row), ROT)
    index = jnp.arange(row_count, dtype=jnp.int32)
    allowed = (segment_row[:, None] == segment_row[None, :]) & (index[None, :] <= index[:, None])
    qkv_all = dot(act_one, qkv_weight) + qkv_bias.astype(F32)[None, :]
    saved = []
    contexts = []
    for head_num in range(heads_here):
        part = qkv_all[:, head_num * 3 * HD : (head_num + 1) * 3 * HD]
        query_rows = rotate_rows(part[:, :HD], cosine, sine, ROT, 1.0).astype(BF16)
        key_rows = rotate_rows(part[:, HD : 2 * HD], cosine, sine, ROT, 1.0).astype(BF16)
        value_rows = part[:, 2 * HD :].astype(BF16)
        context, attn_probs, probs_low = head_forward(query_rows, key_rows, value_rows, allowed)
        saved.append((query_rows, key_rows, value_rows, context, attn_probs, probs_low))
        contexts.append(context)
    context_all = jnp.concatenate(contexts, axis=1)
    proj_grad = weight_grad(net, context_all, cot_full)
    partial_value = dot(context_all, proj_weight) + dot(hidden_act, down_weight)
    mixed = net.scatter_sum(partial_value)
    hidden_out = hidden_in.astype(F32) + mixed + out_bias.astype(F32)[None, :]
    out_bias_grad = jnp.sum(cotangent.astype(F32), axis=0)
    grad_context = dot_t(cot_full, proj_weight).astype(BF16)
    grad_act_two = dot_t(grad_pre_low, up_weight)
    head_grads = []
    for head_num in range(heads_here):
        grad_slice = grad_context[:, head_num * HD : (head_num + 1) * HD]
        query_rows, key_rows, value_rows, context, attn_probs, probs_low = saved[head_num]
        grad_query, grad_keys, grad_values = head_backward(
            query_rows, key_rows, value_rows, context, grad_slice, attn_probs, probs_low
        )
        head_grads.append(rotate_rows(grad_query, cosine, sine, ROT, -1.0))
        head_grads.append(rotate_rows(grad_keys, cosine, sine, ROT, -1.0))
        head_grads.append(grad_values)
    grad_qkv = jnp.concatenate(head_grads, axis=1)
    qkv_bias_grad = jnp.sum(grad_qkv, axis=0)
    grad_qkv_low = grad_qkv.astype(BF16)
    qkv_grad = weight_grad(net, act_one, grad_qkv_low)
    grad_act_one = dot_t(grad_qkv_low, qkv_weight)
    grad_in_one, gain_one, shift_one = norm_backward(grad_act_one, norm_params[0], normed, inverse)
    grad_in_two, gain_two, shift_two = norm_backward(grad_act_two, norm_params[2], normed, inverse)
    hidden_grad = cotangent.astype(F32) + net.scatter_sum(grad_in_one + grad_in_two)

    width = out_bias.shape[0]
    norm_terms = net.sum_small_tensor(jnp.concatenate([gain_one, shift_one, gain_two, shift_two]))
    norm_share = lax.dynamic_slice_in_dim(
        norm_terms.reshape(4, -1), lax.axis_index("tensor") * width, width, 1
    )
    small = net.sum_small(
        jnp.concatenate([qkv_bias_grad, up_bias_grad, out_bias_grad, norm_share.reshape(-1)])
    )
    sizes = [qkv_bias.shape[0], up_bias.shape[0]] + [width] * 5
    parts, at = [], 0
    for size in sizes:
        parts.append(small[at : at + size])
        at += size
    return (
        hidden_out,
        hidden_grad,
        parts[3],
        parts[4],
        parts[5],
        parts[6],
        qkv_grad,
        parts[0],
        proj_grad,
        up_grad,
        parts[1],
        down_grad,
        parts[2],
    )


def solution(mesh):
    net = Net(mesh)
    placed = (
        P("dp", "tensor"),
        P("dp", None),
        P("tensor"),
        P("tensor"),
        P("tensor"),
        P("tensor"),
        P(None, "tensor"),
        P("tensor"),
        P("tensor", None),
        P(None, "tensor"),
        P("tensor"),
        P("tensor", None),
        P("tensor"),
        P("dp", "tensor"),
    )

    def body(*args):
        return per_device(net, *args)

    return jax.shard_map(
        body,
        mesh=mesh,
        in_specs=placed,
        out_specs=(
            P("dp", "tensor"),
            P("dp", "tensor"),
            P("tensor"),
            P("tensor"),
            P("tensor"),
            P("tensor"),
            P(None, "tensor"),
            P("tensor"),
            P("tensor", None),
            P(None, "tensor"),
            P("tensor"),
            P("tensor", None),
            P("tensor"),
        ),
        check_vma=False,
    )
```

```python
import math

import jax
import jax.numpy as jnp
from jax import lax
from jax.experimental import pallas as pl
from jax.experimental.pallas import tpu as pltpu
from jax.sharding import PartitionSpec as P

HD = 256
ROT = 64


root_half = 0.7071067811865476
inv_root_tau = 0.3989422804014327
F32 = jnp.float32
BF16 = jnp.bfloat16


def norm_stats(values):
    average = jnp.mean(values, axis=1, keepdims=True)
    centred = values - average
    spread_sq = jnp.mean(centred * centred, axis=1, keepdims=True)
    inverse = lax.rsqrt(spread_sq + 1e-05)
    return (centred * inverse, inverse)


def norm_backward(grad_out, gain, normed, inverse):
    scaled = grad_out * gain[None, :]
    first_mean = jnp.mean(scaled, axis=1, keepdims=True)
    second_mean = jnp.mean(scaled * normed, axis=1, keepdims=True)
    grad_in = inverse * (scaled - first_mean - normed * second_mean)
    return (grad_in, jnp.sum(grad_out * normed, axis=0), jnp.sum(grad_out, axis=0))


def seq_positions(segment_row):
    indices = jnp.arange(segment_row.shape[0], dtype=jnp.int32)
    same = segment_row[:, None] == segment_row[None, :]
    earlier = same & (indices[None, :] < indices[:, None])
    return jnp.sum(earlier.astype(F32), axis=1)


def rotary_tables(positions, rot_dims):
    half_dims = rot_dims // 2
    exponent = jnp.arange(half_dims, dtype=F32) * (2.0 / rot_dims)
    inv_freq = jnp.exp(-exponent * math.log(10000.0))
    angles = positions[:, None] * inv_freq[None, :]
    return (jnp.cos(angles), jnp.sin(angles))


def rotate_rows(values, cosine, sine, rot_dims, direction):
    half_dims = rot_dims // 2
    first_half = values[:, :half_dims]
    second_half = values[:, half_dims:rot_dims]
    turned_first = first_half * cosine - direction * second_half * sine
    turned_second = second_half * cosine + direction * first_half * sine
    return jnp.concatenate([turned_first, turned_second, values[:, rot_dims:]], axis=1)


def gelu_exact(values):
    return 0.5 * values * (1.0 + lax.erf(values * root_half))


def gelu_slope(values):
    return (
        0.5 * (1.0 + lax.erf(values * root_half))
        + values * jnp.exp(-0.5 * values * values) * inv_root_tau
    )


def dot(a, b):
    return jnp.dot(a, b, preferred_element_type=F32)


def dot_t(a, b):
    return lax.dot_general(a, b, (((1,), (1,)), ((), ())), preferred_element_type=F32)


def t_dot(a, b):
    return lax.dot_general(a, b, (((0,), (0,)), ((), ())), preferred_element_type=F32)


def head_forward(query_rows, key_rows, value_rows, allowed):
    score_scale = 1.0 / math.sqrt(query_rows.shape[1])
    scores = jnp.where(allowed, dot_t(query_rows, key_rows) * score_scale, -1e30)
    row_max = jnp.max(scores, axis=1, keepdims=True)
    log_total = row_max + jnp.log(jnp.sum(jnp.exp(scores - row_max), axis=1, keepdims=True))
    attn_probs = jnp.exp(scores - log_total)
    probs_low = attn_probs.astype(BF16)
    context = dot(probs_low, value_rows).astype(BF16)
    return (context, attn_probs, probs_low)


def head_backward(query_rows, key_rows, value_rows, context, grad_context, attn_probs, probs_low):
    score_scale = 1.0 / math.sqrt(query_rows.shape[1])
    grad_probs = dot_t(grad_context, value_rows)
    delta_rows = jnp.sum(
        grad_context.astype(F32) * context.astype(F32), axis=1, keepdims=True
    )
    grad_scores = (attn_probs * (grad_probs - delta_rows) * score_scale).astype(BF16)
    grad_query = dot(grad_scores, key_rows)
    grad_keys = t_dot(grad_scores, query_rows)
    grad_values = t_dot(probs_low, grad_context)
    return (grad_query, grad_keys, grad_values)


class Net:
    def __init__(self, mesh):
        self.nd = mesh.shape["dp"]
        self.nt = mesh.shape["tensor"]
        self.bits = self.nd.bit_length() - 1
        assert 1 << self.bits == self.nd

    def swap(self, value, bit):
        pairs = [(i, i ^ (1 << bit)) for i in range(self.nd)]
        return lax.ppermute(value, "dp", pairs)

    def swap_tensor(self, value, k):
        pairs = [(i, i ^ k) for i in range(self.nt)]
        return lax.ppermute(value, "tensor", pairs)

    def shift(self, value):
        pairs = [(i, (i + 1) % self.nt) for i in range(self.nt)]
        return lax.ppermute(value, "tensor", pairs)

    def gather(self, value, splits):
        rows = value.shape[0] // splits
        held = [[value[i * rows : (i + 1) * rows]] for i in range(splits)]
        for _ in range(self.nt - 1):
            for part in held:
                part.append(self.shift(part[-1]))
        me = lax.axis_index("tensor")
        done = []
        for part in held:
            slots = []
            for slot in range(self.nt):
                which = lax.rem(me - slot + self.nt, self.nt)
                chosen = part[0]
                for k in range(1, self.nt):
                    chosen = jnp.where(which == k, part[k], chosen)
                slots.append(chosen)
            done.append(jnp.concatenate(slots, axis=1))
        return jnp.concatenate(done, axis=0)

    def scatter_sum(self, value):
        me = lax.axis_index("tensor")
        width = value.shape[1] // self.nt
        total = lax.dynamic_slice_in_dim(value, me * width, width, 1)
        for k in range(1, self.nt):
            there = jnp.bitwise_xor(me, k)
            block = lax.dynamic_slice_in_dim(value, there * width, width, 1).astype(BF16)
            total = total + self.swap_tensor(block, k).astype(F32)
        return total

    def sum_small(self, value):
        for bit in range(self.bits):
            value = value + self.swap(value, bit)
        return value

    def sum_small_tensor(self, value):
        k = 1
        while k < self.nt:
            value = value + self.swap_tensor(value, k)
            k *= 2
        return value


def flow_orders(bits):
    others = list(range(1, bits))
    return [others, others[::-1]]


def weight_grad(net, left, right):
    me = lax.axis_index("dp")
    bit_of = [jnp.bitwise_and(jnp.right_shift(me, b), 1) for b in range(net.bits)]
    rows = left.shape[1]
    orders = flow_orders(net.bits)

    def product(start, count):
        return t_dot(lax.dynamic_slice_in_dim(left, start, count, 1), right)

    half = rows // 2
    quarter = half // 2
    away = product((1 - bit_of[0]) * half, half).astype(BF16)
    arrived = net.swap(away, 0)
    base = bit_of[0] * half
    owned = []
    for flow, order in enumerate(orders):
        size = quarter // 2
        first = order[0]
        offset = flow * quarter
        send_at = offset + (1 - bit_of[first]) * size
        keep_at = offset + bit_of[first] * size
        send = product(base + send_at, size) + lax.dynamic_slice_in_dim(
            arrived, send_at, size, 0
        ).astype(F32)
        got = net.swap(send.astype(BF16), first)
        keep = product(base + keep_at, size) + lax.dynamic_slice_in_dim(
            arrived, keep_at, size, 0
        ).astype(F32)
        for bit in order[1:]:
            size //= 2
            here, there = bit_of[bit] * size, (1 - bit_of[bit]) * size
            send = lax.dynamic_slice_in_dim(keep, there, size, 0) + lax.dynamic_slice_in_dim(
                got, there, size, 0
            ).astype(F32)
            keep = lax.dynamic_slice_in_dim(keep, here, size, 0) + lax.dynamic_slice_in_dim(
                got, here, size, 0
            ).astype(F32)
            got = net.swap(send.astype(BF16), bit)
        owned.append((keep + got.astype(F32)).astype(BF16))
    pieces = []
    for flow, order in enumerate(orders):
        have = [owned[flow]]
        for bit in order[::-1]:
            have = have + [net.swap(piece, bit) for piece in have]
        have = have + [net.swap(piece, 0) for piece in have]
        pieces.append(have)
    return place_pieces(net, pieces, rows)


def place_pieces(net, pieces, rows):
    orders = flow_orders(net.bits)
    flat = [piece for flow in pieces for piece in flow]
    count = len(flat)
    size, columns = flat[0].shape
    dtype = F32

    def body(*refs):
        ins, out, wide, low, in_sem, out_sem = (
            refs[:count], refs[count], refs[count + 1], refs[count + 2], refs[-2], refs[-1]
        )
        me = lax.axis_index("dp")
        mine = [jnp.bitwise_and(jnp.right_shift(me, b), 1) for b in range(net.bits)]

        def row_of(index):
            flow, k = divmod(index, count // 2)
            order = orders[flow]
            levels = [mine[b] for b in order]
            depth = len(order)
            digits = []
            for level in range(depth):
                flip = (k >> (depth - 1 - level)) & 1
                digits.append(1 - levels[level] if flip else levels[level])
            core = 1 - mine[0] if (k >> depth) & 1 else mine[0]
            block = core * 2 + flow
            for digit in digits:
                block = block * 2 + digit
            return pl.multiple_of(block * size, size)

        def load(i):
            return pltpu.make_async_copy(ins[i], low.at[i % 2], in_sem.at[i % 2])

        def store(i):
            return pltpu.make_async_copy(
                wide.at[i % 2], out.at[pl.ds(row_of(i), size), :], out_sem.at[i % 2]
            )

        load(0).start()
        for i in range(count):
            if i + 1 < count:
                load(i + 1).start()
            load(i).wait()
            if i >= 2:
                store(i - 2).wait()
            wide[i % 2] = low[i % 2].astype(dtype)
            store(i).start()
        for i in range(max(0, count - 2), count):
            store(i).wait()

    return pl.pallas_call(
        body,
        out_shape=jax.ShapeDtypeStruct((rows, columns), dtype),
        in_specs=[pl.BlockSpec(memory_space=pl.ANY)] * count,
        out_specs=pl.BlockSpec(memory_space=pl.ANY),
        scratch_shapes=[
            pltpu.VMEM((2, size, columns), dtype),
            pltpu.VMEM((2, size, columns), BF16),
            pltpu.SemaphoreType.DMA((2,)),
            pltpu.SemaphoreType.DMA((2,)),
        ],
        name="place_pieces",
        cost_estimate=pl.CostEstimate(
            flops=rows * columns, bytes_accessed=rows * columns * 6, transcendentals=0
        ),
    )(*flat)


MESH_ID = pl.DeviceIdType.MESH
TILE = 512
PIECE = 128
DEPTH = 6
SLOTS = 4
SLOTS0 = 2
SLOTS1 = 4
SLOTS2 = 4
VMEM_LIMIT = 56_000_000


def start(index, unit):
    return pl.multiple_of(index * unit, unit)


class Ring:
    def __init__(self, part, recv0, recv1, recv2, ssem, rsem):
        self.part, self.recv0, self.recv1, self.recv2 = part, recv0, recv1, recv2
        self.ssem, self.rsem = ssem, rsem
        me = lax.axis_index("dp")
        self.me = me
        self.bit = [lax.rem(lax.div(me, 1 << b), 2) for b in range(3)]
        self.dests = []

    def partner(self, bit):
        return {"dp": self.me + (1 - 2 * self.bit[bit]) * (1 << bit)}

    def axes(self, flow):
        return (1, 2) if flow == 0 else (2, 1)

    def piece(self, flow, core, a, b):
        first, second = self.axes(flow)

        def digit(bit, flip):
            return 1 - self.bit[bit] if flip else self.bit[bit]

        return digit(0, core) * 8 + flow * 4 + digit(first, a) * 2 + digit(second, b)

    def send(self, src, dst, slot, s, r, bit):
        return pltpu.make_async_remote_copy(
            src_ref=src,
            dst_ref=dst,
            send_sem=self.ssem.at[slot, s],
            recv_sem=self.rsem.at[slot, r],
            device_id=self.partner(bit),
            device_id_type=MESH_ID,
        )

    def rows(self, first, count):
        return pl.ds(pl.multiple_of(first, PIECE), count)

    def add(self, i, first, source, at, count):
        part, slot = self.part, i % SLOTS

        @pl.loop(0, count // PIECE)
        def _(k):
            here = self.rows(first + k * PIECE, PIECE)
            there = self.rows(at + k * PIECE, PIECE)
            part[slot, here, :] = (
                part[slot, here, :].astype(F32) + source[there, :].astype(F32)
            ).astype(BF16)

    def copy0(self, i, flow):
        slot = i % DEPTH
        away = (1 - self.bit[0]) * 1024 + flow * 512
        src = self.part.at[i % SLOTS, self.rows(away, 512)]
        dst = self.recv0.at[i % SLOTS0, pl.ds(flow * 512, 512)]
        return self.send(src, dst, slot, (0, 21)[flow], (0, 19)[flow], 0)

    def copy1(self, i, flow):
        slot = i % DEPTH
        a = self.axes(flow)[0]
        first = self.bit[0] * 1024 + flow * 512 + (1 - self.bit[a]) * 256
        src = self.part.at[i % SLOTS, self.rows(first, 256)]
        return self.send(src, self.recv1.at[i % SLOTS1, flow], slot, 1 + flow, 1 + flow, a)

    def copy2(self, i, flow):
        slot = i % DEPTH
        b = self.axes(flow)[1]
        src = self.part.at[i % SLOTS, self.rows(self.piece(flow, 0, 0, 1) * PIECE, PIECE)]
        return self.send(src, self.recv2.at[i % SLOTS2, flow], slot, 3 + flow, 3 + flow, b)

    def out(self, i, index):
        return self.dests[i](index)

    def copy3(self, i, flow, which):
        slot = i % DEPTH
        own = self.piece(flow, 0, 0, 0)
        src = self.part.at[i % SLOTS, self.rows(own * PIECE, PIECE)]
        dst = self.out(i, own)
        s, r = 5 + flow * 8, 5 + flow * 7
        if which == 3:
            return pltpu.make_async_copy(src, dst, self.ssem.at[slot, s + 3])
        a, b = self.axes(flow)
        return self.send(src, dst, slot, s + which, r + (0, 1, 3)[which], (b, a, 0)[which])

    def copy4(self, i, flow, which):
        slot = i % DEPTH
        a = self.axes(flow)[0]
        ref = self.out(i, self.piece(flow, 0, 0, 1))
        s, r = 9 + flow * 8, 5 + flow * 7
        return self.send(ref, ref, slot, s + which, r + (2, 4)[which], (a, 0)[which])

    def copy5(self, i, flow, which):
        slot = i % DEPTH
        ref = self.out(i, self.piece(flow, 0, 1, which))
        return self.send(ref, ref, slot, 11 + flow * 8 + which, 10 + flow * 7 + which, 0)

    def stage1(self, i):
        half = self.bit[0] * 1024
        for away in (1, 0):
            for flow in range(2):
                if away:
                    self.copy0(i, flow).wait()
                bit = self.bit[self.axes(flow)[0]]
                first = flow * 512 + (1 - bit if away else bit) * 256
                self.add(i, half + first, self.recv0.at[i % SLOTS0], first, 256)
                if away:
                    self.copy1(i, flow).start()

    def stage2(self, i):
        for flow in range(2):
            self.copy1(i, flow).wait()
            bit = self.bit[self.axes(flow)[1]]
            source = self.recv1.at[i % SLOTS1, flow]
            self.add(i, self.piece(flow, 0, 0, 1) * PIECE, source, (1 - bit) * PIECE, PIECE)
            self.copy2(i, flow).start()
            self.add(i, self.piece(flow, 0, 0, 0) * PIECE, source, bit * PIECE, PIECE)

    def stage3(self, i):
        for flow in range(2):
            self.copy2(i, flow).wait()
            self.add(
                i, self.piece(flow, 0, 0, 0) * PIECE, self.recv2.at[i % SLOTS2, flow], 0, PIECE
            )
            for which in range(4):
                self.copy3(i, flow, which).start()

    def stage4(self, i):
        for flow in range(2):
            self.copy3(i, flow, 0).wait_recv()
            for which in range(2):
                self.copy4(i, flow, which).start()
        for flow in range(2):
            for which in range(3):
                self.copy3(i, flow, which).wait_send()
            self.copy3(i, flow, 3).wait()

    def stage5(self, i):
        for flow in range(2):
            self.copy3(i, flow, 1).wait_recv()
            self.copy4(i, flow, 0).wait()
            for which in range(2):
                self.copy5(i, flow, which).start()

    def stage6(self, i):
        for flow in range(2):
            self.copy3(i, flow, 2).wait_recv()
            self.copy4(i, flow, 1).wait()
            for which in range(2):
                self.copy5(i, flow, which).wait()


def wide_dest(ref, column):
    def at(index):
        return ref.at[pl.ds(start(index, PIECE), PIECE), pl.ds(start(column, TILE), TILE)]

    return at


def tall_dest(ref, row):
    def at(index):
        down = row * TILE + lax.rem(index, 4) * PIECE
        across = lax.div(index, 4)
        return ref.at[
            pl.ds(pl.multiple_of(down, PIECE), PIECE), pl.ds(start(across, TILE), TILE)
        ]

    return at


INPUTS = (
    "x_in", "cot_in", "seg", "up_w", "down_w", "qkv_w", "proj_w", "up_b", "qkv_b", "out_b",
    "gain1", "bias1", "gain2", "bias2",
)
OUTPUTS = ("down_o", "up_o", "qkv_o", "proj_o", "hid", "grad", "small")
SCRATCH = (
    ("xg", (4, 512, 512), BF16),
    ("info", (4, 8, 512), F32),
    ("cg", (4, 512, 512), BF16),
    ("act1", (4, 512, 512), BF16),
    ("act2", (4, 512, 512), BF16),
    ("hact", (4, 512, 512), BF16),
    ("pre", (4, 512, 512), F32),
    ("gpre", (4, 512, 512), BF16),
    ("gqkv", (3, 512, 512), BF16),
    ("qkvb", (6, 512, 256), BF16),
    ("ctx", (512, 512), BF16),
    ("gctx", (512, 512), BF16),
    ("probs", (512, 512), BF16),
    ("dscore", (512, 512), BF16),
    ("wbuf", (2, 2048, 512), BF16),
    ("pbuf", (4, 512, 512), BF16),
    ("ysend", (3, 512, 512), BF16),
    ("yrecv", (3, 512, 512), BF16),
    ("dsend", (3, 512, 512), BF16),
    ("drecv", (3, 512, 512), BF16),
    ("table", (2, 512, 128), F32),
    ("seg_col", (512, 128), F32),
    ("stat", (4, 512, 128), F32),
    ("srecv", (5, 24, 512), F32),
    ("part", (SLOTS, 2048, TILE), BF16),
    ("recv0", (SLOTS0, 1024, TILE), BF16),
    ("recv1", (SLOTS1, 2, 256, TILE), BF16),
    ("recv2", (SLOTS2, 2, PIECE, TILE), BF16),
)
SEMS = (
    ("ssem", (DEPTH, 22)),
    ("rsem", (DEPTH, 20)),
    ("ns", (3,)),
    ("nr", (3,)),
    ("xs", (3, 4)),
    ("xr", (3, 4)),
    ("cs", (3,)),
    ("cr", (3,)),
    ("wsem", (2, 4)),
    ("psem", (4,)),
    ("own", (2,)),
    ("ys", (3,)),
    ("yr", (3,)),
    ("ds", (3,)),
    ("dr", (3,)),
    ("ms", (5,)),
    ("mr", (5,)),
)
SCALE = 1.0 / 16.0


class Refs:
    pass


def block_kernel(*refs):
    r = Refs()
    names = INPUTS + OUTPUTS + tuple(s[0] for s in SCRATCH) + tuple(s[0] for s in SEMS)
    for name, ref in zip(names, refs):
        setattr(r, name, ref)
    ring = Ring(r.part, r.recv0, r.recv1, r.recv2, r.ssem, r.rsem)
    core = ring.bit[0]
    me = lax.axis_index("tensor")
    width = 2048.0

    def other(k):
        return lax.rem(me + k, 4)

    barrier = pltpu.get_barrier_semaphore()
    friends = [ring.partner(b) for b in range(3)] + [{"tensor": other(k)} for k in (1, 2, 3)]
    home_x = pltpu.make_async_copy(r.x_in, r.xg.at[me], r.own.at[0])
    home_c = pltpu.make_async_copy(r.cot_in, r.cg.at[me], r.own.at[1])
    home_x.start()
    home_c.start()
    for friend in friends:
        pl.semaphore_signal(barrier, inc=1, device_id=friend, device_id_type=MESH_ID)

    for n, ref in enumerate((r.gain1, r.bias1, r.gain2, r.bias2)):
        r.info[me, n : n + 1, :] = ref[...].astype(F32).reshape(1, 512)
    lane = lax.broadcasted_iota(jnp.int32, (128, 128), 1)
    home_x.wait()

    @pl.loop(0, 4)
    def _(b):
        rows = pl.ds(start(b, 128), 128)
        value = r.xg[me, rows, :].astype(F32)
        mean = jnp.sum(value, axis=1, keepdims=True) / 512.0
        centred = value - mean
        spread = jnp.sum(centred * centred, axis=1, keepdims=True)
        r.stat[2, rows, :] = jnp.where(lane < 64, mean, spread)

    turned = jnp.transpose(r.stat[2])
    r.info[me, 4:5, :] = turned[0:1]
    r.info[me, 5:6, :] = turned[64:65]
    r.info[me, 6:8, :] = jnp.zeros((2, 512), F32)
    pl.semaphore_wait(barrier, len(friends))

    def remote(src, dst, ssem, rsem, where):
        return pltpu.make_async_remote_copy(
            src_ref=src, dst_ref=dst, send_sem=ssem, recv_sem=rsem,
            device_id=where, device_id_type=MESH_ID,
        )

    def block_rows(b):
        return pl.ds(128 * b, 128)

    def info_copy(k):
        ref = r.info.at[other(4 - k)]
        return remote(ref, ref, r.ns.at[k], r.nr.at[k], {"tensor": other(1)})


    def x_copy(k, b):
        slot = other(4 - k)
        rows = block_rows(b)
        ref = r.xg.at[slot, rows]
        return remote(ref, ref, r.xs.at[k, b], r.xr.at[k, b], {"tensor": other(1)})

    def cot_copy(k):
        slot = other(4 - k)
        ref = r.cg.at[slot]
        return remote(ref, ref, r.cs.at[k], r.cr.at[k], {"tensor": other(1)})

    x_copy(0, 0).start()
    info_copy(0).start()
    x_copy(0, 1).start()
    x_copy(0, 2).start()
    info_copy(0).wait_recv()
    info_copy(1).start()
    x_copy(0, 3).start()

    def columns_of(ref, block):
        return lambda slot: [
            pltpu.make_async_copy(
                ref.at[:, pl.ds(start(block, 512), 512)], r.wbuf.at[slot], r.wsem.at[slot, 0]
            )
        ]

    def rows_of(ref, block, count):
        return lambda slot: [
            pltpu.make_async_copy(
                ref.at[pl.ds(start(block, 512), 512), pl.ds(k * 512, 512)],
                r.wbuf.at[slot, pl.ds(k * 512, 512)],
                r.wsem.at[slot, k],
            )
            for k in range(count)
        ]

    loads = [rows_of(r.up_w, other(4 - k), 4) for k in range(4)]
    loads += [columns_of(r.qkv_w, c) for c in range(3)]
    loads += [rows_of(r.down_w, j, 4) for j in range(4)]
    loads += [columns_of(r.down_w, other(k)) for k in (1, 2, 3, 0)]
    for s in range(4):
        loads += [rows_of(r.up_w, s, 4), rows_of(r.qkv_w, s, 3)]
    used = [0]

    def begin(n):
        for copy in loads[n](n % 2):
            copy.start()

    def weights():
        n = used[0]
        used[0] = n + 1
        for copy in loads[n](n % 2):
            copy.wait()
        if n + 1 < len(loads):
            begin(n + 1)
        return r.wbuf.at[n % 2]

    begin(0)
    proj_loads = [
        pltpu.make_async_copy(r.proj_w.at[:, pl.ds(s * 512, 512)], r.pbuf.at[s], r.psem.at[s])
        for s in range(4)
    ]
    for copy in proj_loads:
        copy.start()

    info_copy(1).wait_recv()
    info_copy(2).start()
    for b in range(4):
        x_copy(0, b).wait_recv()
        x_copy(1, b).start()

    r.small[...] = jnp.zeros(r.small.shape, F32)
    seg_row = r.seg[...].astype(F32)
    r.seg_col[...] = jnp.transpose(jnp.broadcast_to(seg_row, (128, 512)))

    def visible(rows, first):
        col = lax.broadcasted_iota(jnp.int32, (128, 512), 1)
        row = lax.broadcasted_iota(jnp.int32, (128, 512), 0) + first
        return (r.seg_col[rows, 0:1] == seg_row) & (col <= row)

    @pl.loop(0, 4)
    def _(b):
        rows = pl.ds(start(b, 128), 128)
        seen = jnp.sum(visible(rows, b * 128).astype(F32), axis=1, keepdims=True)
        step = lax.rem(lane, ROT // 2).astype(F32) * (2.0 / ROT)
        angle = (seen - 1.0) * jnp.exp(-step * math.log(10000.0))
        r.table[0, rows, :] = jnp.where(lane < ROT, jnp.cos(angle), 1.0)
        sine = jnp.sin(angle)
        r.table[1, rows, :] = jnp.where(
            lane < ROT // 2, -sine, jnp.where(lane < ROT, sine, 0.0)
        )

    home_c.wait()
    r.small[23:24, :] = jnp.sum(r.cg[me].astype(F32), axis=0, keepdims=True)
    info_copy(2).wait_recv()
    mean = sum(r.info[s, 4:5, :] for s in range(4)) / 4.0
    spread = sum(r.info[s, 5:6, :] for s in range(4))
    for s in range(4):
        off = r.info[s, 4:5, :] - mean
        spread += 512.0 * (off * off)
    inverse = lax.rsqrt(spread / width + 1e-05)
    r.stat[0] = jnp.transpose(jnp.broadcast_to(mean, (128, 512)))
    r.stat[1] = jnp.transpose(jnp.broadcast_to(inverse, (128, 512)))

    def normed_of(s, rows):
        values = r.xg[s, rows, :].astype(F32)
        return (values - r.stat[0, rows, 0:1]) * r.stat[1, rows, 0:1]

    def act_block(s, b):
        @pl.loop(0, 2)
        def _(half):
            rows = pl.ds(start(2 * b + half, 64), 64)
            normed = normed_of(s, rows)
            p = r.info[s]
            r.act1[s, rows, :] = (normed * p[0:1] + p[1:2]).astype(BF16)
            r.act2[s, rows, :] = (normed * p[2:3] + p[3:4]).astype(BF16)

    def up_part(s, w, first):
        @pl.loop(0, 8)
        def _(n):
            j, rows = lax.div(n, 2), pl.ds(start(lax.rem(n, 2), 256), 256)
            value = dot(r.act2[s, rows, :], w[pl.ds(start(j, 512), 512), :])
            if first:
                bias = r.up_b[pl.ds(start(j, 512), 512)].astype(F32).reshape(1, 512)
                r.pre[j, rows, :] = value + bias
            else:
                r.pre[j, rows, :] += value

    for k in range(3):
        shard = other(4 - k)
        if k == 1:
            for b in range(4):
                x_copy(1, b).wait_recv()
                x_copy(2, b).start()
            cot_copy(0).start()
        for b in range(4):
            act_block(shard, b)
        up_part(shard, weights(), k == 0)
    last_shard = other(1)
    last_w = weights()
    for b in range(4):
        x_copy(2, b).wait_recv()
        act_block(last_shard, b)

        @pl.loop(0, 4)
        def _(j):
            rows = pl.ds(b * 128, 128)
            value = r.pre[j, rows, :] + dot(
                r.act2[last_shard, rows, :], last_w[pl.ds(start(j, 512), 512), :]
            )
            r.pre[j, rows, :] = value
            r.hact[j, rows, :] = gelu_exact(value).astype(BF16)

    def product(i, left_of, right_of):
        slot = i % SLOTS

        def quarter(which, flow):
            @pl.loop(0, 2)
            def _(k):
                tile = which * 4 + flow * 2 + k
                r.part[slot, pl.ds(start(tile, 256), 256), :] = t_dot(
                    left_of(tile), right_of(tile)
                ).astype(BF16)

        for flow in range(2):
            quarter(1 - core, flow)
            ring.copy0(i, flow).start()
        for flow in range(2):
            quarter(core, flow)

    def columns(ref, first, count):
        return ref[:, pl.ds(pl.multiple_of(first, 256), count)]

    jobs = []

    def down_job(k):
        shard = other(4 - k)
        ring.dests.append(wide_dest(r.down_o, shard))

        jobs.append(
            lambda i: product(
                i,
                lambda t: columns(r.hact.at[lax.div(t, 2)], lax.rem(t, 2) * 256, 256),
                lambda t: r.cg[shard],
            )
        )

    def wide_job(left, right, out, column):
        ring.dests.append(wide_dest(out, column))
        jobs.append(
            lambda i: product(
                i,
                lambda t: columns(left.at[lax.div(t, 2)], lax.rem(t, 2) * 256, 256),
                lambda t: right[column],
            )
        )

    def tall_job(left, out):
        ring.dests.append(tall_dest(out, 0))
        jobs.append(
            lambda i: product(
                i,
                lambda t: columns(left, lax.rem(t, 2) * 256, 256),
                lambda t: r.cg[lax.div(t, 2)],
            )
        )

    for k in range(4):
        down_job(k)
    for j in range(4):
        wide_job(r.act2, r.gpre, r.up_o, j)
    tall_job(r.ctx, r.proj_o)
    for c in range(3):
        wide_job(r.act1, r.gqkv, r.qkv_o, c)

    def turn(value, rows, direction):
        count = value.shape[0]
        head = value[:, :128]
        here = lax.broadcasted_iota(jnp.int32, (count, 128), 1)
        mate = jnp.where(
            here < ROT // 2,
            pltpu.roll(head, 128 - ROT // 2, 1),
            pltpu.roll(head, ROT // 2, 1),
        )
        head = head * r.table[0, rows, :] + direction * (mate * r.table[1, rows, :])
        return jnp.concatenate([head, value[:, 128:]], axis=1)

    def qkv_block(c):
        w = weights()

        @pl.loop(0, 2)
        def _(b):
            rows = pl.ds(start(b, 256), 256)
            value = r.qkv_b[c * 512 : (c + 1) * 512].astype(F32).reshape(1, 512)
            for s in range(4):
                value = value + dot(r.act1[s, rows, :], w[s * 512 : (s + 1) * 512, :])
            for k in range(2):
                p = 2 * c + k
                one = value[:, k * 256 : (k + 1) * 256]
                if p % 3 != 2:
                    one = turn(one, rows, 1.0)
                r.qkvb[p, rows, :] = one.astype(BF16)

    def grad_context():
        for copy in proj_loads:
            copy.wait()

        @pl.loop(0, 2)
        def _(b):
            rows = pl.ds(start(b, 256), 256)
            total = sum(dot_t(r.cg[s, rows, :], r.pbuf[s]) for s in range(4))
            r.gctx[rows, :] = total.astype(BF16)

    def keep_qkv(p, rows, value):
        c, across = p // 2, slice((p % 2) * 256, (p % 2) * 256 + 256)
        r.small[20 + c : 21 + c, across] += jnp.sum(value, axis=0, keepdims=True)
        r.gqkv[c, rows, across] = value.astype(BF16)

    def attention(h):
        q, k, v = r.qkvb.at[3 * h], r.qkvb.at[3 * h + 1], r.qkvb.at[3 * h + 2]
        across = slice(h * HD, (h + 1) * HD)

        @pl.loop(0, 4)
        def _(b):
            rows = pl.ds(start(b, 128), 128)
            scores = jnp.where(
                visible(rows, b * 128), dot_t(q[rows, :], k[...]) * SCALE, -1e30
            )
            top = jnp.max(scores, axis=1, keepdims=True)
            total = jnp.sum(jnp.exp(scores - top), axis=1, keepdims=True)
            probs = jnp.exp(scores - (top + jnp.log(total)))
            low = probs.astype(BF16)
            r.probs[rows, :] = low
            context = dot(low, v[...]).astype(BF16)
            r.ctx[rows, across] = context
            grad = r.gctx[rows, across]
            delta = jnp.sum(grad.astype(F32) * context.astype(F32), axis=1, keepdims=True)
            dscore = (probs * (dot_t(grad, v[...]) - delta) * SCALE).astype(BF16)
            r.dscore[rows, :] = dscore
            keep_qkv(3 * h, rows, turn(dot(dscore, k[...]), rows, -1.0))

        @pl.loop(0, 2)
        def _(b):
            rows = pl.ds(start(b, 256), 256)
            keep_qkv(
                3 * h + 1, rows, turn(t_dot(columns(r.dscore, b * 256, 256), q[...]), rows, -1.0)
            )
            keep_qkv(3 * h + 2, rows, t_dot(columns(r.probs, b * 256, 256), r.gctx[:, across]))

    def gpre_block(j):
        w = weights()

        @pl.loop(0, 2)
        def _(b):
            rows = pl.ds(start(b, 256), 256)
            total = sum(
                dot_t(r.cg[s, rows, :], w[s * 512 : (s + 1) * 512, :]) for s in range(4)
            )
            total = total * gelu_slope(r.pre[j, rows, :])
            r.small[16 + j : 17 + j, :] += jnp.sum(total, axis=0, keepdims=True)
            r.gpre[j, rows, :] = total.astype(BF16)

    def z_copy(send, recv, ssem, rsem, k):
        return remote(
            send.at[k - 1], recv.at[k - 1], ssem.at[k - 1], rsem.at[k - 1], {"tensor": other(k)}
        )

    def y_copy(k):
        return z_copy(r.ysend, r.yrecv, r.ys, r.yr, k)

    def d_copy(k):
        return z_copy(r.dsend, r.drecv, r.ds, r.dr, k)

    def y_block(k):
        w = weights()
        shard = other(k)

        @pl.loop(0, 2)
        def _(b):
            rows = pl.ds(start(b, 256), 256)
            total = dot(r.ctx[rows, :], r.pbuf[shard])
            for j in range(4):
                total += dot(r.hact[j, rows, :], w[j * 512 : (j + 1) * 512, :])
            if k:
                r.ysend[k - 1, rows, :] = total.astype(BF16)
            else:
                bias = r.out_b[...].astype(F32).reshape(1, 512)
                r.hid[rows, :] = total + r.xg[me, rows, :].astype(F32) + bias

        if k:
            y_copy(k).start()

    def back_block(s):
        p = r.info[s]
        w_up = weights()

        @pl.loop(0, 2)
        def _(b):
            rows = pl.ds(start(b, 256), 256)
            total = dot_t(r.gpre[0, rows, :], w_up[0:512, :])
            for j in range(1, 4):
                total += dot_t(r.gpre[j, rows, :], w_up[j * 512 : (j + 1) * 512, :])
            normed = normed_of(s, rows)
            r.small[8 + s : 9 + s, :] += jnp.sum(total * normed, axis=0, keepdims=True)
            r.small[12 + s : 13 + s, :] += jnp.sum(total, axis=0, keepdims=True)
            r.pre[s, rows, :] = total * p[2:3]

        w_qkv = weights()

        @pl.loop(0, 2)
        def _(b):
            rows = pl.ds(start(b, 256), 256)
            total = dot_t(r.gqkv[0, rows, :], w_qkv[0:512, :])
            for c in range(1, 3):
                total += dot_t(r.gqkv[c, rows, :], w_qkv[c * 512 : (c + 1) * 512, :])
            normed = normed_of(s, rows)
            r.small[s : 1 + s, :] += jnp.sum(total * normed, axis=0, keepdims=True)
            r.small[4 + s : 5 + s, :] += jnp.sum(total, axis=0, keepdims=True)
            both = r.pre[s, rows, :] + total * p[0:1]
            r.pre[s, rows, :] = both
            one = jnp.sum(both, axis=1, keepdims=True)
            two = jnp.sum(both * normed, axis=1, keepdims=True)
            if s:
                one += r.stat[2, rows, 0:1]
                two += r.stat[3, rows, 0:1]
            r.stat[2, rows, :] = jnp.broadcast_to(one, (256, 128))
            r.stat[3, rows, :] = jnp.broadcast_to(two, (256, 128))

    def finish_rows():
        for k in (1, 2, 3, 0):
            shard = other(k)

            @pl.loop(0, 4)
            def _(b):
                rows = pl.ds(start(b, 128), 128)
                one, two = r.stat[2, rows, 0:1] / width, r.stat[3, rows, 0:1] / width
                normed = normed_of(shard, rows)
                value = r.stat[1, rows, 0:1] * (r.pre[shard, rows, :] - one - normed * two)
                if k:
                    r.dsend[k - 1, rows, :] = value.astype(BF16)
                else:
                    r.grad[rows, :] = value + r.cg[me, rows, :].astype(F32)

            if k:
                d_copy(k).start()

    def collect(out, recv, copy):
        for k in (1, 2, 3):
            copy(k).wait()

        @pl.loop(0, 4)
        def _(b):
            rows = pl.ds(start(b, 128), 128)
            total = out[rows, :]
            for k in range(3):
                total += recv[k, rows, :].astype(F32)
            out[rows, :] = total

    bit0, bit1 = lax.rem(me, 2), lax.div(me, 2)

    def small_copy(n):
        rows = pl.ds(0, 16 if n < 2 else 24)
        if n == 0:
            where = {"tensor": me + 1 - 2 * bit0}
        elif n == 1:
            where = {"tensor": me + 2 - 4 * bit1}
        else:
            where = ring.partner(n - 2)
        return remote(
            r.small.at[rows], r.srecv.at[n, rows], r.ms.at[n], r.mr.at[n], where
        )

    def small_done(n):
        small_copy(n).wait()
        rows = slice(0, 16 if n < 2 else 24)
        r.small[rows, :] += r.srecv[n, rows, :]

    def small_step(n):
        if n:
            small_done(n - 1)
        if n < 5:
            small_copy(n).start()

    def finish_hidden():
        collect(r.hid, r.yrecv, y_copy)

    def finish_grad():
        collect(r.grad, r.drecv, d_copy)

    def settle():
        for k in range(3):
            for b in range(4):
                x_copy(k, b).wait_send()
            cot_copy(k).wait_send()
            info_copy(k).wait_send()

    extras = {
        3: [lambda: gpre_block(0), lambda: gpre_block(1), grad_context],
        4: [lambda: gpre_block(2), lambda: attention(0)],
        5: [lambda: gpre_block(3), lambda: attention(1)],
        6: [lambda: y_block(1), lambda: y_block(2), lambda: y_block(3), lambda: y_block(0)],
        7: [lambda: back_block(0), lambda: back_block(1)],
        8: [lambda: back_block(2), lambda: back_block(3), finish_rows],
        9: [lambda: small_step(0)],
        10: [lambda: small_step(1)],
        11: [lambda: small_step(2)],
        12: [lambda: small_step(3), settle],
        13: [lambda: small_step(4)],
        14: [lambda: small_step(5), finish_hidden],
        15: [finish_grad],
    }
    count = len(jobs)
    stages = [ring.stage1, ring.stage2, ring.stage3, ring.stage4, ring.stage5, ring.stage6]
    reached = [0] * count

    def advance(i, stage):
        if reached[i] < stage:
            reached[i] = stage
            stages[stage - 1](i)

    def cot_step(k):
        cot_copy(k).wait_recv()
        if k < 2:
            cot_copy(k + 1).start()

    jobs[0](0)
    advance(0, 1)
    for c in range(3):
        qkv_block(c)
    cot_step(0)
    advance(0, 2)
    jobs[1](1)
    advance(1, 1)
    advance(0, 3)
    cot_step(1)
    advance(1, 2)
    jobs[2](2)
    advance(0, 4)
    advance(2, 1)
    advance(1, 3)
    cot_step(2)
    jobs[3](3)
    for step in range(3, count + DEPTH):
        if step > 3:
            for depth in range(1, DEPTH + 1):
                if 0 <= step - depth < count:
                    advance(step - depth, depth)
            if step < count:
                jobs[step](step)
        for extra in extras.get(step, []):
            extra()


def fused_block(
    hidden_in, cotangent, norm_params, segment_ids,
    up_weight, down_weight, qkv_weight, proj_weight, up_bias, qkv_bias, out_bias,
):
    rows, width = hidden_in.shape
    vmem, anywhere = pl.BlockSpec(memory_space=pltpu.VMEM), pl.BlockSpec(memory_space=pl.ANY)
    return pl.pallas_call(
        block_kernel,
        out_shape=[
            jax.ShapeDtypeStruct(down_weight.shape, BF16),
            jax.ShapeDtypeStruct(up_weight.shape, BF16),
            pltpu.VMEM(qkv_weight.shape, BF16),
            pltpu.VMEM(proj_weight.shape, BF16),
            pltpu.VMEM((rows, width), F32),
            pltpu.VMEM((rows, width), F32),
            pltpu.VMEM((24, width), F32),
        ],
        in_specs=[anywhere] * 2 + [vmem] + [anywhere] * 4 + [vmem] * 7,
        out_specs=[anywhere] * 2 + [vmem] * 5,
        scratch_shapes=[pltpu.VMEM(shape, dtype) for _, shape, dtype in SCRATCH]
        + [pltpu.SemaphoreType.DMA(shape) for _, shape in SEMS],
        compiler_params=pltpu.CompilerParams(
            collective_id=0, has_side_effects=True, vmem_limit_bytes=VMEM_LIMIT
        ),
        name="fused_block",
    )(
        hidden_in, cotangent, segment_ids,
        up_weight, down_weight, qkv_weight, proj_weight,
        up_bias, qkv_bias, out_bias, *norm_params,
    )


FINISH_ROWS = 256
IN_SLOTS = 4
OUT_SLOTS = 4


def finish_kernel(
    down, up, qkv, proj, hid, grad, small,
    hid_o, grad_o, gain1_o, bias1_o, gain2_o, bias2_o, qkv_o, qkvb_o, proj_o, up_o, upb_o,
    down_o, outb_o, low, wide, in_sem, out_sem, row_sem,
):
    rows_out = [
        pltpu.make_async_copy(hid, hid_o, row_sem.at[0]),
        pltpu.make_async_copy(grad, grad_o, row_sem.at[1]),
    ]
    blocks, loaded = [], []
    for src, dst, near in ((qkv, qkv_o, 1), (proj, proj_o, 1), (down, down_o, 0), (up, up_o, 0)):
        for n in range(src.shape[0] // FINISH_ROWS):
            if not near:
                loaded.append(len(blocks))
            blocks.append((src, dst, n * FINISH_ROWS, src.shape[1], near))

    def load(m):
        src, _, first, across, _ = blocks[loaded[m]]
        slot = m % IN_SLOTS
        return pltpu.make_async_copy(
            src.at[pl.ds(first, FINISH_ROWS)], low.at[slot, :, pl.ds(0, across)], in_sem.at[slot]
        )

    def store(n):
        _, dst, first, across, _ = blocks[n]
        slot = n % OUT_SLOTS
        return pltpu.make_async_copy(
            wide.at[slot, :, pl.ds(0, across)], dst.at[pl.ds(first, FINISH_ROWS)], out_sem.at[slot]
        )

    for copy in rows_out:
        copy.start()
    for m in range(IN_SLOTS - 1):
        load(m).start()
    me = lax.axis_index("tensor")
    for n, out in enumerate((gain1_o, bias1_o, gain2_o, bias2_o)):
        out[...] = small[pl.ds(4 * n + me, 1), :].reshape(512)
    for n in range(4):
        upb_o[pl.ds(n * 512, 512)] = small[16 + n : 17 + n, :].reshape(512)
    for n in range(3):
        qkvb_o[pl.ds(n * 512, 512)] = small[20 + n : 21 + n, :].reshape(512)
    outb_o[...] = small[23:24, :].reshape(512)
    taken = 0
    for n, (src, _, first, across, near) in enumerate(blocks):
        if near:
            source, offset = src, first
        else:
            if taken + IN_SLOTS - 1 < len(loaded):
                load(taken + IN_SLOTS - 1).start()
            load(taken).wait()
            source, offset = low.at[taken % IN_SLOTS], 0
            taken += 1
        if n >= OUT_SLOTS:
            store(n - OUT_SLOTS).wait()

        @pl.loop(0, FINISH_ROWS // 32)
        def _(b):
            rows = pl.ds(start(b, 32), 32)
            here = pl.ds(pl.multiple_of(offset + b * 32, 32), 32)
            wide[n % OUT_SLOTS, rows, 0:across] = source[here, 0:across].astype(F32)

        store(n).start()
    for n in range(len(blocks) - OUT_SLOTS, len(blocks)):
        store(n).wait()
    for copy in rows_out:
        copy.wait()


def finish(down, up, qkv, proj, hid, grad, small):
    def wide_like(array):
        return jax.ShapeDtypeStruct(array.shape, F32)

    def line(size):
        return jax.ShapeDtypeStruct((size,), F32)

    vmem, anywhere = pl.BlockSpec(memory_space=pltpu.VMEM), pl.BlockSpec(memory_space=pl.ANY)
    big = sum(array.size for array in (down, up, qkv, proj))
    return pl.pallas_call(
        finish_kernel,
        out_shape=[wide_like(hid), wide_like(grad)]
        + [line(512)] * 4
        + [wide_like(qkv), line(1536), wide_like(proj), wide_like(up), line(2048)]
        + [wide_like(down), line(512)],
        in_specs=[anywhere] * 2 + [vmem] * 5,
        out_specs=[anywhere] * 2 + [vmem] * 4
        + [anywhere, vmem, anywhere, anywhere, vmem, anywhere, vmem],
        scratch_shapes=[
            pltpu.VMEM((IN_SLOTS, FINISH_ROWS, 2048), BF16),
            pltpu.VMEM((OUT_SLOTS, FINISH_ROWS, 2048), F32),
            pltpu.SemaphoreType.DMA((IN_SLOTS,)),
            pltpu.SemaphoreType.DMA((OUT_SLOTS,)),
            pltpu.SemaphoreType.DMA((2,)),
        ],
        compiler_params=pltpu.CompilerParams(vmem_limit_bytes=40_000_000),
        cost_estimate=pl.CostEstimate(flops=big, bytes_accessed=6 * big, transcendentals=0),
        name="finish",
    )(down, up, qkv, proj, hid, grad, small)


def fits_kernel(net, hidden_in, qkv_weight, up_weight):
    return (
        (net.nd, net.nt) == (8, 4)
        and hidden_in.shape == (512, 512)
        and qkv_weight.shape == (2048, 1536)
        and up_weight.shape == (2048, 2048)
    )


def kernel_path(*args):
    return tuple(finish(*fused_block(*args)))


def per_device(
    net,
    hidden_in,
    segment_ids,
    norm1_gain,
    norm1_bias,
    norm2_gain,
    norm2_bias,
    qkv_weight,
    qkv_bias,
    proj_weight,
    up_weight,
    up_bias,
    down_weight,
    out_bias,
    cotangent,
):
    norm_stack = jnp.stack([norm1_gain, norm1_bias, norm2_gain, norm2_bias])
    if fits_kernel(net, hidden_in, qkv_weight, up_weight):
        return kernel_path(
            hidden_in, cotangent, (norm1_gain, norm1_bias, norm2_gain, norm2_bias), segment_ids,
            up_weight, down_weight, qkv_weight, proj_weight, up_bias, qkv_bias, out_bias,
        )
    full_rows = net.gather(hidden_in, 2)
    norm_full = net.gather(norm_stack, 1)
    cot_full = net.gather(cotangent, 2)
    norm_params = norm_full.astype(F32)
    segment_row = segment_ids[0]
    row_count = full_rows.shape[0]
    heads_here = qkv_weight.shape[1] // (3 * HD)
    normed, inverse = norm_stats(full_rows.astype(F32))
    act_one = (normed * norm_params[0][None, :] + norm_params[1][None, :]).astype(BF16)
    act_two = (normed * norm_params[2][None, :] + norm_params[3][None, :]).astype(BF16)

    pre_up = dot(act_two, up_weight) + up_bias.astype(F32)[None, :]
    hidden_act = gelu_exact(pre_up).astype(BF16)
    down_grad = weight_grad(net, hidden_act, cot_full)
    grad_pre = dot_t(cot_full, down_weight) * gelu_slope(pre_up)
    up_bias_grad = jnp.sum(grad_pre, axis=0)
    grad_pre_low = grad_pre.astype(BF16)
    up_grad = weight_grad(net, act_two, grad_pre_low)

    cosine, sine = rotary_tables(seq_positions(segment_row), ROT)
    index = jnp.arange(row_count, dtype=jnp.int32)
    allowed = (segment_row[:, None] == segment_row[None, :]) & (index[None, :] <= index[:, None])
    qkv_all = dot(act_one, qkv_weight) + qkv_bias.astype(F32)[None, :]
    saved = []
    contexts = []
    for head_num in range(heads_here):
        part = qkv_all[:, head_num * 3 * HD : (head_num + 1) * 3 * HD]
        query_rows = rotate_rows(part[:, :HD], cosine, sine, ROT, 1.0).astype(BF16)
        key_rows = rotate_rows(part[:, HD : 2 * HD], cosine, sine, ROT, 1.0).astype(BF16)
        value_rows = part[:, 2 * HD :].astype(BF16)
        context, attn_probs, probs_low = head_forward(query_rows, key_rows, value_rows, allowed)
        saved.append((query_rows, key_rows, value_rows, context, attn_probs, probs_low))
        contexts.append(context)
    context_all = jnp.concatenate(contexts, axis=1)
    proj_grad = weight_grad(net, context_all, cot_full)
    partial_value = dot(context_all, proj_weight) + dot(hidden_act, down_weight)
    mixed = net.scatter_sum(partial_value)
    hidden_out = hidden_in.astype(F32) + mixed + out_bias.astype(F32)[None, :]
    out_bias_grad = jnp.sum(cotangent.astype(F32), axis=0)
    grad_context = dot_t(cot_full, proj_weight).astype(BF16)
    grad_act_two = dot_t(grad_pre_low, up_weight)
    head_grads = []
    for head_num in range(heads_here):
        grad_slice = grad_context[:, head_num * HD : (head_num + 1) * HD]
        query_rows, key_rows, value_rows, context, attn_probs, probs_low = saved[head_num]
        grad_query, grad_keys, grad_values = head_backward(
            query_rows, key_rows, value_rows, context, grad_slice, attn_probs, probs_low
        )
        head_grads.append(rotate_rows(grad_query, cosine, sine, ROT, -1.0))
        head_grads.append(rotate_rows(grad_keys, cosine, sine, ROT, -1.0))
        head_grads.append(grad_values)
    grad_qkv = jnp.concatenate(head_grads, axis=1)
    qkv_bias_grad = jnp.sum(grad_qkv, axis=0)
    grad_qkv_low = grad_qkv.astype(BF16)
    qkv_grad = weight_grad(net, act_one, grad_qkv_low)
    grad_act_one = dot_t(grad_qkv_low, qkv_weight)
    grad_in_one, gain_one, shift_one = norm_backward(grad_act_one, norm_params[0], normed, inverse)
    grad_in_two, gain_two, shift_two = norm_backward(grad_act_two, norm_params[2], normed, inverse)
    hidden_grad = cotangent.astype(F32) + net.scatter_sum(grad_in_one + grad_in_two)

    width = out_bias.shape[0]
    norm_terms = net.sum_small_tensor(jnp.concatenate([gain_one, shift_one, gain_two, shift_two]))
    norm_share = lax.dynamic_slice_in_dim(
        norm_terms.reshape(4, -1), lax.axis_index("tensor") * width, width, 1
    )
    small = net.sum_small(
        jnp.concatenate([qkv_bias_grad, up_bias_grad, out_bias_grad, norm_share.reshape(-1)])
    )
    sizes = [qkv_bias.shape[0], up_bias.shape[0]] + [width] * 5
    parts, at = [], 0
    for size in sizes:
        parts.append(small[at : at + size])
        at += size
    return (
        hidden_out,
        hidden_grad,
        parts[3],
        parts[4],
        parts[5],
        parts[6],
        qkv_grad,
        parts[0],
        proj_grad,
        up_grad,
        parts[1],
        down_grad,
        parts[2],
    )


def solution(mesh):
    net = Net(mesh)
    placed = (
        P("dp", "tensor"),
        P("dp", None),
        P("tensor"),
        P("tensor"),
        P("tensor"),
        P("tensor"),
        P(None, "tensor"),
        P("tensor"),
        P("tensor", None),
        P(None, "tensor"),
        P("tensor"),
        P("tensor", None),
        P("tensor"),
        P("dp", "tensor"),
    )

    def body(*args):
        return per_device(net, *args)

    return jax.shard_map(
        body,
        mesh=mesh,
        in_specs=placed,
        out_specs=(
            P("dp", "tensor"),
            P("dp", "tensor"),
            P("tensor"),
            P("tensor"),
            P("tensor"),
            P("tensor"),
            P(None, "tensor"),
            P("tensor"),
            P("tensor", None),
            P(None, "tensor"),
            P("tensor"),
            P("tensor", None),
            P("tensor"),
        ),
        check_vma=False,
    )
```

```python
import math

import jax
import jax.numpy as jnp
from jax import lax
from jax.experimental import pallas as pl
from jax.experimental.pallas import tpu as pltpu
from jax.sharding import PartitionSpec as P

HD = 256
ROT = 64


root_half = 0.7071067811865476
inv_root_tau = 0.3989422804014327
F32 = jnp.float32
BF16 = jnp.bfloat16


def norm_stats(values):
    average = jnp.mean(values, axis=1, keepdims=True)
    centred = values - average
    spread_sq = jnp.mean(centred * centred, axis=1, keepdims=True)
    inverse = lax.rsqrt(spread_sq + 1e-05)
    return (centred * inverse, inverse)


def norm_backward(grad_out, gain, normed, inverse):
    scaled = grad_out * gain[None, :]
    first_mean = jnp.mean(scaled, axis=1, keepdims=True)
    second_mean = jnp.mean(scaled * normed, axis=1, keepdims=True)
    grad_in = inverse * (scaled - first_mean - normed * second_mean)
    return (grad_in, jnp.sum(grad_out * normed, axis=0), jnp.sum(grad_out, axis=0))


def seq_positions(segment_row):
    indices = jnp.arange(segment_row.shape[0], dtype=jnp.int32)
    same = segment_row[:, None] == segment_row[None, :]
    earlier = same & (indices[None, :] < indices[:, None])
    return jnp.sum(earlier.astype(F32), axis=1)


def rotary_tables(positions, rot_dims):
    half_dims = rot_dims // 2
    exponent = jnp.arange(half_dims, dtype=F32) * (2.0 / rot_dims)
    inv_freq = jnp.exp(-exponent * math.log(10000.0))
    angles = positions[:, None] * inv_freq[None, :]
    return (jnp.cos(angles), jnp.sin(angles))


def rotate_rows(values, cosine, sine, rot_dims, direction):
    half_dims = rot_dims // 2
    first_half = values[:, :half_dims]
    second_half = values[:, half_dims:rot_dims]
    turned_first = first_half * cosine - direction * second_half * sine
    turned_second = second_half * cosine + direction * first_half * sine
    return jnp.concatenate([turned_first, turned_second, values[:, rot_dims:]], axis=1)


def gelu_exact(values):
    return 0.5 * values * (1.0 + lax.erf(values * root_half))


def gelu_slope(values):
    return (
        0.5 * (1.0 + lax.erf(values * root_half))
        + values * jnp.exp(-0.5 * values * values) * inv_root_tau
    )


def dot(a, b):
    return jnp.dot(a, b, preferred_element_type=F32)


def dot_t(a, b):
    return lax.dot_general(a, b, (((1,), (1,)), ((), ())), preferred_element_type=F32)


def t_dot(a, b):
    return lax.dot_general(a, b, (((0,), (0,)), ((), ())), preferred_element_type=F32)


def head_forward(query_rows, key_rows, value_rows, allowed):
    score_scale = 1.0 / math.sqrt(query_rows.shape[1])
    scores = jnp.where(allowed, dot_t(query_rows, key_rows) * score_scale, -1e30)
    row_max = jnp.max(scores, axis=1, keepdims=True)
    log_total = row_max + jnp.log(jnp.sum(jnp.exp(scores - row_max), axis=1, keepdims=True))
    attn_probs = jnp.exp(scores - log_total)
    probs_low = attn_probs.astype(BF16)
    context = dot(probs_low, value_rows).astype(BF16)
    return (context, attn_probs, probs_low)


def head_backward(query_rows, key_rows, value_rows, context, grad_context, attn_probs, probs_low):
    score_scale = 1.0 / math.sqrt(query_rows.shape[1])
    grad_probs = dot_t(grad_context, value_rows)
    delta_rows = jnp.sum(
        grad_context.astype(F32) * context.astype(F32), axis=1, keepdims=True
    )
    grad_scores = (attn_probs * (grad_probs - delta_rows) * score_scale).astype(BF16)
    grad_query = dot(grad_scores, key_rows)
    grad_keys = t_dot(grad_scores, query_rows)
    grad_values = t_dot(probs_low, grad_context)
    return (grad_query, grad_keys, grad_values)


class Net:
    def __init__(self, mesh):
        self.nd = mesh.shape["dp"]
        self.nt = mesh.shape["tensor"]
        self.bits = self.nd.bit_length() - 1
        assert 1 << self.bits == self.nd

    def swap(self, value, bit):
        pairs = [(i, i ^ (1 << bit)) for i in range(self.nd)]
        return lax.ppermute(value, "dp", pairs)

    def swap_tensor(self, value, k):
        pairs = [(i, i ^ k) for i in range(self.nt)]
        return lax.ppermute(value, "tensor", pairs)

    def shift(self, value):
        pairs = [(i, (i + 1) % self.nt) for i in range(self.nt)]
        return lax.ppermute(value, "tensor", pairs)

    def gather(self, value, splits):
        rows = value.shape[0] // splits
        held = [[value[i * rows : (i + 1) * rows]] for i in range(splits)]
        for _ in range(self.nt - 1):
            for part in held:
                part.append(self.shift(part[-1]))
        me = lax.axis_index("tensor")
        done = []
        for part in held:
            slots = []
            for slot in range(self.nt):
                which = lax.rem(me - slot + self.nt, self.nt)
                chosen = part[0]
                for k in range(1, self.nt):
                    chosen = jnp.where(which == k, part[k], chosen)
                slots.append(chosen)
            done.append(jnp.concatenate(slots, axis=1))
        return jnp.concatenate(done, axis=0)

    def scatter_sum(self, value):
        me = lax.axis_index("tensor")
        width = value.shape[1] // self.nt
        total = lax.dynamic_slice_in_dim(value, me * width, width, 1)
        for k in range(1, self.nt):
            there = jnp.bitwise_xor(me, k)
            block = lax.dynamic_slice_in_dim(value, there * width, width, 1).astype(BF16)
            total = total + self.swap_tensor(block, k).astype(F32)
        return total

    def sum_small(self, value):
        for bit in range(self.bits):
            value = value + self.swap(value, bit)
        return value

    def sum_small_tensor(self, value):
        k = 1
        while k < self.nt:
            value = value + self.swap_tensor(value, k)
            k *= 2
        return value


def flow_orders(bits):
    others = list(range(1, bits))
    return [others, others[::-1]]


def weight_grad(net, left, right):
    me = lax.axis_index("dp")
    bit_of = [jnp.bitwise_and(jnp.right_shift(me, b), 1) for b in range(net.bits)]
    rows = left.shape[1]
    orders = flow_orders(net.bits)

    def product(start, count):
        return t_dot(lax.dynamic_slice_in_dim(left, start, count, 1), right)

    half = rows // 2
    quarter = half // 2
    away = product((1 - bit_of[0]) * half, half).astype(BF16)
    arrived = net.swap(away, 0)
    base = bit_of[0] * half
    owned = []
    for flow, order in enumerate(orders):
        size = quarter // 2
        first = order[0]
        offset = flow * quarter
        send_at = offset + (1 - bit_of[first]) * size
        keep_at = offset + bit_of[first] * size
        send = product(base + send_at, size) + lax.dynamic_slice_in_dim(
            arrived, send_at, size, 0
        ).astype(F32)
        got = net.swap(send.astype(BF16), first)
        keep = product(base + keep_at, size) + lax.dynamic_slice_in_dim(
            arrived, keep_at, size, 0
        ).astype(F32)
        for bit in order[1:]:
            size //= 2
            here, there = bit_of[bit] * size, (1 - bit_of[bit]) * size
            send = lax.dynamic_slice_in_dim(keep, there, size, 0) + lax.dynamic_slice_in_dim(
                got, there, size, 0
            ).astype(F32)
            keep = lax.dynamic_slice_in_dim(keep, here, size, 0) + lax.dynamic_slice_in_dim(
                got, here, size, 0
            ).astype(F32)
            got = net.swap(send.astype(BF16), bit)
        owned.append((keep + got.astype(F32)).astype(BF16))
    pieces = []
    for flow, order in enumerate(orders):
        have = [owned[flow]]
        for bit in order[::-1]:
            have = have + [net.swap(piece, bit) for piece in have]
        have = have + [net.swap(piece, 0) for piece in have]
        pieces.append(have)
    return place_pieces(net, pieces, rows)


def place_pieces(net, pieces, rows):
    orders = flow_orders(net.bits)
    flat = [piece for flow in pieces for piece in flow]
    count = len(flat)
    size, columns = flat[0].shape
    dtype = F32

    def body(*refs):
        ins, out, wide, low, in_sem, out_sem = (
            refs[:count], refs[count], refs[count + 1], refs[count + 2], refs[-2], refs[-1]
        )
        me = lax.axis_index("dp")
        mine = [jnp.bitwise_and(jnp.right_shift(me, b), 1) for b in range(net.bits)]

        def row_of(index):
            flow, k = divmod(index, count // 2)
            order = orders[flow]
            levels = [mine[b] for b in order]
            depth = len(order)
            digits = []
            for level in range(depth):
                flip = (k >> (depth - 1 - level)) & 1
                digits.append(1 - levels[level] if flip else levels[level])
            core = 1 - mine[0] if (k >> depth) & 1 else mine[0]
            block = core * 2 + flow
            for digit in digits:
                block = block * 2 + digit
            return pl.multiple_of(block * size, size)

        def load(i):
            return pltpu.make_async_copy(ins[i], low.at[i % 2], in_sem.at[i % 2])

        def store(i):
            return pltpu.make_async_copy(
                wide.at[i % 2], out.at[pl.ds(row_of(i), size), :], out_sem.at[i % 2]
            )

        load(0).start()
        for i in range(count):
            if i + 1 < count:
                load(i + 1).start()
            load(i).wait()
            if i >= 2:
                store(i - 2).wait()
            wide[i % 2] = low[i % 2].astype(dtype)
            store(i).start()
        for i in range(max(0, count - 2), count):
            store(i).wait()

    return pl.pallas_call(
        body,
        out_shape=jax.ShapeDtypeStruct((rows, columns), dtype),
        in_specs=[pl.BlockSpec(memory_space=pl.ANY)] * count,
        out_specs=pl.BlockSpec(memory_space=pl.ANY),
        scratch_shapes=[
            pltpu.VMEM((2, size, columns), dtype),
            pltpu.VMEM((2, size, columns), BF16),
            pltpu.SemaphoreType.DMA((2,)),
            pltpu.SemaphoreType.DMA((2,)),
        ],
        name="place_pieces",
        cost_estimate=pl.CostEstimate(
            flops=rows * columns, bytes_accessed=rows * columns * 6, transcendentals=0
        ),
    )(*flat)


MESH_ID = pl.DeviceIdType.MESH
TILE = 512
PIECE = 128
DEPTH = 6
SLOTS = 4
SLOTS0 = 2
SLOTS1 = 4
SLOTS2 = 4
VMEM_LIMIT = 39_400_000


def start(index, unit):
    return pl.multiple_of(index * unit, unit)


class Ring:
    def __init__(self, part, recv0, recv1, recv2, ssem, rsem):
        self.part, self.recv0, self.recv1, self.recv2 = part, recv0, recv1, recv2
        self.ssem, self.rsem = ssem, rsem
        me = lax.axis_index("dp")
        self.me = me
        self.bit = [lax.rem(lax.div(me, 1 << b), 2) for b in range(3)]
        self.dests = []

    def partner(self, bit):
        return {"dp": self.me + (1 - 2 * self.bit[bit]) * (1 << bit)}

    def axes(self, flow):
        return (1, 2) if flow == 0 else (2, 1)

    def piece(self, flow, core, a, b):
        first, second = self.axes(flow)

        def digit(bit, flip):
            return 1 - self.bit[bit] if flip else self.bit[bit]

        return digit(0, core) * 8 + flow * 4 + digit(first, a) * 2 + digit(second, b)

    def send(self, src, dst, slot, s, r, bit):
        return pltpu.make_async_remote_copy(
            src_ref=src,
            dst_ref=dst,
            send_sem=self.ssem.at[slot, s],
            recv_sem=self.rsem.at[slot, r],
            device_id=self.partner(bit),
            device_id_type=MESH_ID,
        )

    def rows(self, first, count):
        return pl.ds(pl.multiple_of(first, PIECE), count)

    def add(self, i, first, source, at, count):
        part, slot = self.part, i % SLOTS

        @pl.loop(0, count // PIECE)
        def _(k):
            here = self.rows(first + k * PIECE, PIECE)
            there = self.rows(at + k * PIECE, PIECE)
            part[slot, here, :] = (
                part[slot, here, :].astype(F32) + source[there, :].astype(F32)
            ).astype(BF16)

    def copy0(self, i, flow):
        slot = i % DEPTH
        away = (1 - self.bit[0]) * 1024 + flow * 512
        src = self.part.at[i % SLOTS, self.rows(away, 512)]
        dst = self.recv0.at[i % SLOTS0, pl.ds(flow * 512, 512)]
        return self.send(src, dst, slot, (0, 21)[flow], (0, 19)[flow], 0)

    def copy1(self, i, flow):
        slot = i % DEPTH
        a = self.axes(flow)[0]
        first = self.bit[0] * 1024 + flow * 512 + (1 - self.bit[a]) * 256
        src = self.part.at[i % SLOTS, self.rows(first, 256)]
        return self.send(src, self.recv1.at[i % SLOTS1, flow], slot, 1 + flow, 1 + flow, a)

    def copy2(self, i, flow):
        slot = i % DEPTH
        b = self.axes(flow)[1]
        src = self.part.at[i % SLOTS, self.rows(self.piece(flow, 0, 0, 1) * PIECE, PIECE)]
        return self.send(src, self.recv2.at[i % SLOTS2, flow], slot, 3 + flow, 3 + flow, b)

    def out(self, i, index):
        return self.dests[i](index)

    def copy3(self, i, flow, which):
        slot = i % DEPTH
        own = self.piece(flow, 0, 0, 0)
        src = self.part.at[i % SLOTS, self.rows(own * PIECE, PIECE)]
        dst = self.out(i, own)
        s, r = 5 + flow * 8, 5 + flow * 7
        if which == 3:
            return pltpu.make_async_copy(src, dst, self.ssem.at[slot, s + 3])
        a, b = self.axes(flow)
        return self.send(src, dst, slot, s + which, r + (0, 1, 3)[which], (b, a, 0)[which])

    def copy4(self, i, flow, which):
        slot = i % DEPTH
        a = self.axes(flow)[0]
        ref = self.out(i, self.piece(flow, 0, 0, 1))
        s, r = 9 + flow * 8, 5 + flow * 7
        return self.send(ref, ref, slot, s + which, r + (2, 4)[which], (a, 0)[which])

    def copy5(self, i, flow, which):
        slot = i % DEPTH
        ref = self.out(i, self.piece(flow, 0, 1, which))
        return self.send(ref, ref, slot, 11 + flow * 8 + which, 10 + flow * 7 + which, 0)

    def stage1(self, i):
        half = self.bit[0] * 1024
        for away in (1, 0):
            for flow in range(2):
                if away:
                    self.copy0(i, flow).wait()
                bit = self.bit[self.axes(flow)[0]]
                first = flow * 512 + (1 - bit if away else bit) * 256
                self.add(i, half + first, self.recv0.at[i % SLOTS0], first, 256)
                if away:
                    self.copy1(i, flow).start()

    def stage2(self, i):
        for flow in range(2):
            self.copy1(i, flow).wait()
            bit = self.bit[self.axes(flow)[1]]
            source = self.recv1.at[i % SLOTS1, flow]
            self.add(i, self.piece(flow, 0, 0, 1) * PIECE, source, (1 - bit) * PIECE, PIECE)
            self.copy2(i, flow).start()
            self.add(i, self.piece(flow, 0, 0, 0) * PIECE, source, bit * PIECE, PIECE)

    def stage3(self, i):
        for flow in range(2):
            self.copy2(i, flow).wait()
            self.add(
                i, self.piece(flow, 0, 0, 0) * PIECE, self.recv2.at[i % SLOTS2, flow], 0, PIECE
            )
            for which in range(4):
                self.copy3(i, flow, which).start()

    def stage4(self, i):
        for flow in range(2):
            self.copy3(i, flow, 0).wait_recv()
            for which in range(2):
                self.copy4(i, flow, which).start()
        for flow in range(2):
            for which in range(3):
                self.copy3(i, flow, which).wait_send()
            self.copy3(i, flow, 3).wait()

    def stage5(self, i):
        for flow in range(2):
            self.copy3(i, flow, 1).wait_recv()
            self.copy4(i, flow, 0).wait()
            for which in range(2):
                self.copy5(i, flow, which).start()

    def stage6(self, i):
        for flow in range(2):
            self.copy3(i, flow, 2).wait_recv()
            self.copy4(i, flow, 1).wait()
            for which in range(2):
                self.copy5(i, flow, which).wait()


def wide_dest(ref, column):
    def at(index):
        return ref.at[pl.ds(start(index, PIECE), PIECE), pl.ds(start(column, TILE), TILE)]

    return at


def tall_dest(ref, row):
    def at(index):
        down = row * TILE + lax.rem(index, 4) * PIECE
        across = lax.div(index, 4)
        return ref.at[
            pl.ds(pl.multiple_of(down, PIECE), PIECE), pl.ds(start(across, TILE), TILE)
        ]

    return at


INPUTS = (
    "x_in", "cot_in", "seg", "up_w", "down_w", "qkv_w", "proj_w", "up_b", "qkv_b", "out_b",
    "gain1", "bias1", "gain2", "bias2",
)
OUTPUTS = ("down_o", "up_o", "qkv_o", "proj_o", "hid", "grad", "small")
SCRATCH = (
    ("xg", (4, 512, 512), BF16),
    ("info", (4, 8, 512), F32),
    ("cg", (4, 512, 512), BF16),
    ("act1", (4, 512, 512), BF16),
    ("pre", (4, 512, 512), F32),
    ("gpre", (4, 512, 512), BF16),
    ("gqkv", (3, 512, 512), BF16),
    ("ctx", (512, 512), BF16),
    ("probs", (512, 512), BF16),
    ("dscore", (512, 512), BF16),
    ("ysend", (3, 512, 512), BF16),
    ("yrecv", (3, 512, 512), BF16),
    ("dsend", (3, 512, 512), BF16),
    ("drecv", (3, 512, 512), BF16),
    ("table", (2, 512, 128), F32),
    ("seg_col", (512, 128), F32),
    ("stat", (4, 512, 128), F32),
    ("srecv", (5, 24, 512), F32),
    ("part", (SLOTS, 2048, TILE), BF16),
    ("recv0", (SLOTS0, 1024, TILE), BF16),
    ("recv1", (SLOTS1, 2, 256, TILE), BF16),
    ("recv2", (SLOTS2, 2, PIECE, TILE), BF16),
)
SEMS = (
    ("ssem", (DEPTH, 22)),
    ("rsem", (DEPTH, 20)),
    ("ns", (3,)),
    ("nr", (3,)),
    ("xs", (3, 4)),
    ("xr", (3, 4)),
    ("cs", (3,)),
    ("cr", (3,)),
    ("wsem", (2, 4)),
    ("psem", (4,)),
    ("own", (2,)),
    ("ys", (3,)),
    ("yr", (3,)),
    ("ds", (3,)),
    ("dr", (3,)),
    ("ms", (5,)),
    ("mr", (5,)),
)
SCALE = 1.0 / 16.0


class Refs:
    pass


def block_kernel(*refs):
    r = Refs()
    names = INPUTS + OUTPUTS + tuple(s[0] for s in SCRATCH) + tuple(s[0] for s in SEMS)
    for name, ref in zip(names, refs):
        setattr(r, name, ref)
    ring = Ring(r.part, r.recv0, r.recv1, r.recv2, r.ssem, r.rsem)
    core = ring.bit[0]
    me = lax.axis_index("tensor")
    width = 2048.0

    def other(k):
        return lax.rem(me + k, 4)

    def wbuf(slot):
        return r.qkv_o.at[:, pl.ds(slot * 512, 512)]

    def pbuf(s):
        return r.qkv_o.at[pl.ds(start(s, 512), 512), pl.ds(1024, 512)]

    def act1(s):
        return r.act1.at[s]

    def act2(s):
        return r.proj_o.at[:, pl.ds(start(s, 512), 512)]

    def hact(j):
        return r.up_o.at[pl.ds(start(j, 512), 512), pl.ds(1536, 512)]

    def qkvb(p):
        return r.up_o.at[pl.ds((p // 2) * 512, 512), pl.ds(1024 + (p % 2) * 256, 256)]

    gctx = r.up_o.at[pl.ds(1536, 512), pl.ds(1024, 512)]

    barrier = pltpu.get_barrier_semaphore()
    friends = [ring.partner(b) for b in range(3)] + [{"tensor": other(k)} for k in (1, 2, 3)]
    home_x = pltpu.make_async_copy(r.x_in, r.xg.at[me], r.own.at[0])
    home_c = pltpu.make_async_copy(r.cot_in, r.cg.at[me], r.own.at[1])
    home_x.start()
    home_c.start()
    for friend in friends:
        pl.semaphore_signal(barrier, inc=1, device_id=friend, device_id_type=MESH_ID)

    for n, ref in enumerate((r.gain1, r.bias1, r.gain2, r.bias2)):
        r.info[me, n : n + 1, :] = ref[...].astype(F32).reshape(1, 512)
    lane = lax.broadcasted_iota(jnp.int32, (128, 128), 1)
    home_x.wait()

    @pl.loop(0, 4)
    def _(b):
        rows = pl.ds(start(b, 128), 128)
        value = r.xg[me, rows, :].astype(F32)
        mean = jnp.sum(value, axis=1, keepdims=True) / 512.0
        centred = value - mean
        spread = jnp.sum(centred * centred, axis=1, keepdims=True)
        r.stat[2, rows, :] = jnp.where(lane < 64, mean, spread)

    turned = jnp.transpose(r.stat[2])
    r.info[me, 4:5, :] = turned[0:1]
    r.info[me, 5:6, :] = turned[64:65]
    r.info[me, 6:8, :] = jnp.zeros((2, 512), F32)
    pl.semaphore_wait(barrier, len(friends))

    def remote(src, dst, ssem, rsem, where):
        return pltpu.make_async_remote_copy(
            src_ref=src, dst_ref=dst, send_sem=ssem, recv_sem=rsem,
            device_id=where, device_id_type=MESH_ID,
        )

    def block_rows(b):
        return pl.ds(128 * b, 128)

    def info_copy(k):
        ref = r.info.at[other(4 - k)]
        return remote(ref, ref, r.ns.at[k], r.nr.at[k], {"tensor": other(1)})


    def x_copy(k, b):
        slot = other(4 - k)
        rows = block_rows(b)
        ref = r.xg.at[slot, rows]
        return remote(ref, ref, r.xs.at[k, b], r.xr.at[k, b], {"tensor": other(1)})

    def cot_copy(k):
        slot = other(4 - k)
        ref = r.cg.at[slot]
        return remote(ref, ref, r.cs.at[k], r.cr.at[k], {"tensor": other(1)})

    x_copy(0, 0).start()
    info_copy(0).start()
    x_copy(0, 1).start()
    x_copy(0, 2).start()
    info_copy(0).wait_recv()
    info_copy(1).start()
    x_copy(0, 3).start()

    def columns_of(ref, block):
        return lambda slot: [
            pltpu.make_async_copy(
                ref.at[:, pl.ds(start(block, 512), 512)], wbuf(slot), r.wsem.at[slot, 0]
            )
        ]

    def rows_of(ref, block, count):
        return lambda slot: [
            pltpu.make_async_copy(
                ref.at[pl.ds(start(block, 512), 512), pl.ds(k * 512, 512)],
                wbuf(slot).at[pl.ds(k * 512, 512)],
                r.wsem.at[slot, k],
            )
            for k in range(count)
        ]

    loads = [rows_of(r.up_w, other(4 - k), 4) for k in range(4)]
    loads += [columns_of(r.qkv_w, c) for c in range(3)]
    loads += [rows_of(r.down_w, j, 4) for j in range(4)]
    loads += [columns_of(r.down_w, other(k)) for k in (1, 2, 3, 0)]
    for s in range(4):
        loads += [rows_of(r.up_w, s, 4), rows_of(r.qkv_w, s, 3)]
    used = [0]

    def begin(n):
        for copy in loads[n](n % 2):
            copy.start()

    def weights():
        n = used[0]
        used[0] = n + 1
        for copy in loads[n](n % 2):
            copy.wait()
        if n + 1 < len(loads):
            begin(n + 1)
        return wbuf(n % 2)

    begin(0)
    proj_loads = [
        pltpu.make_async_copy(r.proj_w.at[:, pl.ds(s * 512, 512)], pbuf(s), r.psem.at[s])
        for s in range(4)
    ]
    for copy in proj_loads:
        copy.start()

    info_copy(1).wait_recv()
    info_copy(2).start()
    for b in range(4):
        x_copy(0, b).wait_recv()
        x_copy(1, b).start()

    r.small[...] = jnp.zeros(r.small.shape, F32)
    seg_row = r.seg[...].astype(F32)
    r.seg_col[...] = jnp.transpose(jnp.broadcast_to(seg_row, (128, 512)))

    def visible(rows, first):
        col = lax.broadcasted_iota(jnp.int32, (128, 512), 1)
        row = lax.broadcasted_iota(jnp.int32, (128, 512), 0) + first
        return (r.seg_col[rows, 0:1] == seg_row) & (col <= row)

    @pl.loop(0, 4)
    def _(b):
        rows = pl.ds(start(b, 128), 128)
        seen = jnp.sum(visible(rows, b * 128).astype(F32), axis=1, keepdims=True)
        step = lax.rem(lane, ROT // 2).astype(F32) * (2.0 / ROT)
        angle = (seen - 1.0) * jnp.exp(-step * math.log(10000.0))
        r.table[0, rows, :] = jnp.where(lane < ROT, jnp.cos(angle), 1.0)
        sine = jnp.sin(angle)
        r.table[1, rows, :] = jnp.where(
            lane < ROT // 2, -sine, jnp.where(lane < ROT, sine, 0.0)
        )

    home_c.wait()
    r.small[23:24, :] = jnp.sum(r.cg[me].astype(F32), axis=0, keepdims=True)
    info_copy(2).wait_recv()
    mean = sum(r.info[s, 4:5, :] for s in range(4)) / 4.0
    spread = sum(r.info[s, 5:6, :] for s in range(4))
    for s in range(4):
        off = r.info[s, 4:5, :] - mean
        spread += 512.0 * (off * off)
    inverse = lax.rsqrt(spread / width + 1e-05)
    r.stat[0] = jnp.transpose(jnp.broadcast_to(mean, (128, 512)))
    r.stat[1] = jnp.transpose(jnp.broadcast_to(inverse, (128, 512)))

    def normed_of(s, rows):
        values = r.xg[s, rows, :].astype(F32)
        return (values - r.stat[0, rows, 0:1]) * r.stat[1, rows, 0:1]

    def act_block(s, b):
        @pl.loop(0, 2)
        def _(half):
            rows = pl.ds(start(2 * b + half, 64), 64)
            normed = normed_of(s, rows)
            p = r.info[s]
            r.act1[s, rows, :] = (normed * p[0:1] + p[1:2]).astype(BF16)
            act2(s)[rows, :] = (normed * p[2:3] + p[3:4]).astype(BF16)

    def up_part(s, w, first):
        @pl.loop(0, 8)
        def _(n):
            j, rows = lax.div(n, 2), pl.ds(start(lax.rem(n, 2), 256), 256)
            value = dot(act2(s)[rows, :], w[pl.ds(start(j, 512), 512), :])
            if first:
                bias = r.up_b[pl.ds(start(j, 512), 512)].astype(F32).reshape(1, 512)
                r.pre[j, rows, :] = value + bias
            else:
                r.pre[j, rows, :] += value

    for k in range(3):
        shard = other(4 - k)
        if k == 1:
            for b in range(4):
                x_copy(1, b).wait_recv()
                x_copy(2, b).start()
            cot_copy(0).start()
        for b in range(4):
            act_block(shard, b)
        up_part(shard, weights(), k == 0)
    last_shard = other(1)
    last_w = weights()
    for b in range(4):
        x_copy(2, b).wait_recv()
        act_block(last_shard, b)

        @pl.loop(0, 4)
        def _(j):
            rows = pl.ds(b * 128, 128)
            value = r.pre[j, rows, :] + dot(
                act2(last_shard)[rows, :], last_w[pl.ds(start(j, 512), 512), :]
            )
            r.pre[j, rows, :] = value
            hact(j)[rows, :] = gelu_exact(value).astype(BF16)

    def product(i, left_of, right_of):
        slot = i % SLOTS

        def quarter(which, flow):
            @pl.loop(0, 2)
            def _(k):
                tile = which * 4 + flow * 2 + k
                r.part[slot, pl.ds(start(tile, 256), 256), :] = t_dot(
                    left_of(tile), right_of(tile)
                ).astype(BF16)

        for flow in range(2):
            quarter(1 - core, flow)
            ring.copy0(i, flow).start()
        for flow in range(2):
            quarter(core, flow)

    def columns(ref, first, count):
        return ref[:, pl.ds(pl.multiple_of(first, 256), count)]

    jobs = []

    def down_job(k):
        shard = other(4 - k)
        ring.dests.append(wide_dest(r.down_o, shard))

        jobs.append(
            lambda i: product(
                i,
                lambda t: columns(hact(lax.div(t, 2)), lax.rem(t, 2) * 256, 256),
                lambda t: r.cg[shard],
            )
        )

    def wide_job(left, right, out, column):
        ring.dests.append(wide_dest(out, column))
        jobs.append(
            lambda i: product(
                i,
                lambda t: columns(left(lax.div(t, 2)), lax.rem(t, 2) * 256, 256),
                lambda t: right[column],
            )
        )

    def tall_job(left, out):
        ring.dests.append(tall_dest(out, 0))
        jobs.append(
            lambda i: product(
                i,
                lambda t: columns(left, lax.rem(t, 2) * 256, 256),
                lambda t: r.cg[lax.div(t, 2)],
            )
        )

    for k in range(4):
        down_job(k)
    for j in range(4):
        wide_job(act2, r.gpre, r.up_o, j)
    tall_job(r.ctx, r.proj_o)
    for c in range(3):
        wide_job(act1, r.gqkv, r.qkv_o, c)

    def turn(value, rows, direction):
        count = value.shape[0]
        head = value[:, :128]
        here = lax.broadcasted_iota(jnp.int32, (count, 128), 1)
        mate = jnp.where(
            here < ROT // 2,
            pltpu.roll(head, 128 - ROT // 2, 1),
            pltpu.roll(head, ROT // 2, 1),
        )
        head = head * r.table[0, rows, :] + direction * (mate * r.table[1, rows, :])
        return jnp.concatenate([head, value[:, 128:]], axis=1)

    def qkv_block(c):
        w = weights()

        @pl.loop(0, 2)
        def _(b):
            rows = pl.ds(start(b, 256), 256)
            value = r.qkv_b[c * 512 : (c + 1) * 512].astype(F32).reshape(1, 512)
            for s in range(4):
                value = value + dot(r.act1[s, rows, :], w[s * 512 : (s + 1) * 512, :])
            for k in range(2):
                p = 2 * c + k
                one = value[:, k * 256 : (k + 1) * 256]
                if p % 3 != 2:
                    one = turn(one, rows, 1.0)
                qkvb(p)[rows, :] = one.astype(BF16)

    def grad_context():
        for copy in proj_loads:
            copy.wait()

        @pl.loop(0, 2)
        def _(b):
            rows = pl.ds(start(b, 256), 256)
            total = sum(dot_t(r.cg[s, rows, :], pbuf(s)[...]) for s in range(4))
            gctx[rows, :] = total.astype(BF16)

    def keep_qkv(p, rows, value):
        c, across = p // 2, slice((p % 2) * 256, (p % 2) * 256 + 256)
        r.small[20 + c : 21 + c, across] += jnp.sum(value, axis=0, keepdims=True)
        r.gqkv[c, rows, across] = value.astype(BF16)

    def attention(h):
        q, k, v = qkvb(3 * h), qkvb(3 * h + 1), qkvb(3 * h + 2)
        across = slice(h * HD, (h + 1) * HD)

        @pl.loop(0, 4)
        def _(b):
            rows = pl.ds(start(b, 128), 128)
            scores = jnp.where(
                visible(rows, b * 128), dot_t(q[rows, :], k[...]) * SCALE, -1e30
            )
            top = jnp.max(scores, axis=1, keepdims=True)
            total = jnp.sum(jnp.exp(scores - top), axis=1, keepdims=True)
            probs = jnp.exp(scores - (top + jnp.log(total)))
            low = probs.astype(BF16)
            r.probs[rows, :] = low
            context = dot(low, v[...]).astype(BF16)
            r.ctx[rows, across] = context
            grad = gctx[rows, across]
            delta = jnp.sum(grad.astype(F32) * context.astype(F32), axis=1, keepdims=True)
            dscore = (probs * (dot_t(grad, v[...]) - delta) * SCALE).astype(BF16)
            r.dscore[rows, :] = dscore
            keep_qkv(3 * h, rows, turn(dot(dscore, k[...]), rows, -1.0))

        @pl.loop(0, 2)
        def _(b):
            rows = pl.ds(start(b, 256), 256)
            keep_qkv(
                3 * h + 1, rows, turn(t_dot(columns(r.dscore, b * 256, 256), q[...]), rows, -1.0)
            )
            keep_qkv(3 * h + 2, rows, t_dot(columns(r.probs, b * 256, 256), gctx[:, across]))

    def gpre_block(j):
        w = weights()

        @pl.loop(0, 2)
        def _(b):
            rows = pl.ds(start(b, 256), 256)
            total = sum(
                dot_t(r.cg[s, rows, :], w[s * 512 : (s + 1) * 512, :]) for s in range(4)
            )
            total = total * gelu_slope(r.pre[j, rows, :])
            r.small[16 + j : 17 + j, :] += jnp.sum(total, axis=0, keepdims=True)
            r.gpre[j, rows, :] = total.astype(BF16)

    def z_copy(send, recv, ssem, rsem, k):
        return remote(
            send.at[k - 1], recv.at[k - 1], ssem.at[k - 1], rsem.at[k - 1], {"tensor": other(k)}
        )

    def y_copy(k):
        return z_copy(r.ysend, r.yrecv, r.ys, r.yr, k)

    def d_copy(k):
        return z_copy(r.dsend, r.drecv, r.ds, r.dr, k)

    def y_block(k):
        w = weights()
        shard = other(k)

        @pl.loop(0, 2)
        def _(b):
            rows = pl.ds(start(b, 256), 256)
            total = dot(r.ctx[rows, :], pbuf(shard)[...])
            for j in range(4):
                total += dot(hact(j)[rows, :], w[j * 512 : (j + 1) * 512, :])
            if k:
                r.ysend[k - 1, rows, :] = total.astype(BF16)
            else:
                bias = r.out_b[...].astype(F32).reshape(1, 512)
                r.hid[rows, :] = total + r.xg[me, rows, :].astype(F32) + bias

        if k:
            y_copy(k).start()

    def back_block(s):
        p = r.info[s]
        w_up = weights()

        @pl.loop(0, 2)
        def _(b):
            rows = pl.ds(start(b, 256), 256)
            total = dot_t(r.gpre[0, rows, :], w_up[0:512, :])
            for j in range(1, 4):
                total += dot_t(r.gpre[j, rows, :], w_up[j * 512 : (j + 1) * 512, :])
            normed = normed_of(s, rows)
            r.small[8 + s : 9 + s, :] += jnp.sum(total * normed, axis=0, keepdims=True)
            r.small[12 + s : 13 + s, :] += jnp.sum(total, axis=0, keepdims=True)
            r.pre[s, rows, :] = total * p[2:3]

        w_qkv = weights()

        @pl.loop(0, 2)
        def _(b):
            rows = pl.ds(start(b, 256), 256)
            total = dot_t(r.gqkv[0, rows, :], w_qkv[0:512, :])
            for c in range(1, 3):
                total += dot_t(r.gqkv[c, rows, :], w_qkv[c * 512 : (c + 1) * 512, :])
            normed = normed_of(s, rows)
            r.small[s : 1 + s, :] += jnp.sum(total * normed, axis=0, keepdims=True)
            r.small[4 + s : 5 + s, :] += jnp.sum(total, axis=0, keepdims=True)
            both = r.pre[s, rows, :] + total * p[0:1]
            r.pre[s, rows, :] = both
            one = jnp.sum(both, axis=1, keepdims=True)
            two = jnp.sum(both * normed, axis=1, keepdims=True)
            if s:
                one += r.stat[2, rows, 0:1]
                two += r.stat[3, rows, 0:1]
            r.stat[2, rows, :] = jnp.broadcast_to(one, (256, 128))
            r.stat[3, rows, :] = jnp.broadcast_to(two, (256, 128))

    def finish_rows():
        for k in (1, 2, 3, 0):
            shard = other(k)

            @pl.loop(0, 4)
            def _(b):
                rows = pl.ds(start(b, 128), 128)
                one, two = r.stat[2, rows, 0:1] / width, r.stat[3, rows, 0:1] / width
                normed = normed_of(shard, rows)
                value = r.stat[1, rows, 0:1] * (r.pre[shard, rows, :] - one - normed * two)
                if k:
                    r.dsend[k - 1, rows, :] = value.astype(BF16)
                else:
                    r.grad[rows, :] = value + r.cg[me, rows, :].astype(F32)

            if k:
                d_copy(k).start()

    def collect(out, recv, copy):
        for k in (1, 2, 3):
            copy(k).wait()

        @pl.loop(0, 4)
        def _(b):
            rows = pl.ds(start(b, 128), 128)
            total = out[rows, :]
            for k in range(3):
                total += recv[k, rows, :].astype(F32)
            out[rows, :] = total

    bit0, bit1 = lax.rem(me, 2), lax.div(me, 2)

    def small_copy(n):
        rows = pl.ds(0, 16 if n < 2 else 24)
        if n == 0:
            where = {"tensor": me + 1 - 2 * bit0}
        elif n == 1:
            where = {"tensor": me + 2 - 4 * bit1}
        else:
            where = ring.partner(n - 2)
        return remote(
            r.small.at[rows], r.srecv.at[n, rows], r.ms.at[n], r.mr.at[n], where
        )

    def small_done(n):
        small_copy(n).wait()
        rows = slice(0, 16 if n < 2 else 24)
        r.small[rows, :] += r.srecv[n, rows, :]

    def small_step(n):
        if n:
            small_done(n - 1)
        if n < 5:
            small_copy(n).start()

    def finish_hidden():
        collect(r.hid, r.yrecv, y_copy)

    def finish_grad():
        collect(r.grad, r.drecv, d_copy)

    def settle():
        for k in range(3):
            for b in range(4):
                x_copy(k, b).wait_send()
            cot_copy(k).wait_send()
            info_copy(k).wait_send()

    extras = {
        3: [lambda: gpre_block(0), lambda: gpre_block(1), grad_context],
        4: [lambda: gpre_block(2), lambda: attention(0)],
        5: [lambda: gpre_block(3), lambda: attention(1)],
        6: [lambda: y_block(1), lambda: y_block(2), lambda: y_block(3), lambda: y_block(0)],
        7: [lambda: back_block(0), lambda: back_block(1)],
        8: [lambda: back_block(2), lambda: back_block(3), finish_rows],
        9: [lambda: small_step(0)],
        10: [lambda: small_step(1)],
        11: [lambda: small_step(2)],
        12: [lambda: small_step(3), settle],
        13: [lambda: small_step(4)],
        14: [lambda: small_step(5), finish_hidden],
        15: [finish_grad],
    }
    count = len(jobs)
    stages = [ring.stage1, ring.stage2, ring.stage3, ring.stage4, ring.stage5, ring.stage6]
    reached = [0] * count

    def advance(i, stage):
        if reached[i] < stage:
            reached[i] = stage
            stages[stage - 1](i)

    def cot_step(k):
        cot_copy(k).wait_recv()
        if k < 2:
            cot_copy(k + 1).start()

    jobs[0](0)
    advance(0, 1)
    for c in range(3):
        qkv_block(c)
    cot_step(0)
    advance(0, 2)
    jobs[1](1)
    advance(1, 1)
    advance(0, 3)
    cot_step(1)
    advance(1, 2)
    jobs[2](2)
    advance(0, 4)
    advance(2, 1)
    advance(1, 3)
    cot_step(2)
    jobs[3](3)
    for step in range(3, count + DEPTH):
        if step > 3:
            for depth in range(1, DEPTH + 1):
                if 0 <= step - depth < count:
                    advance(step - depth, depth)
            if step < count:
                jobs[step](step)
        for extra in extras.get(step, []):
            extra()


def fused_block(
    hidden_in, cotangent, norm_params, segment_ids,
    up_weight, down_weight, qkv_weight, proj_weight, up_bias, qkv_bias, out_bias,
):
    rows, width = hidden_in.shape
    vmem, anywhere = pl.BlockSpec(memory_space=pltpu.VMEM), pl.BlockSpec(memory_space=pl.ANY)
    return pl.pallas_call(
        block_kernel,
        out_shape=[
            pltpu.VMEM(down_weight.shape, BF16),
            pltpu.VMEM(up_weight.shape, BF16),
            pltpu.VMEM(qkv_weight.shape, BF16),
            pltpu.VMEM(proj_weight.shape, BF16),
            pltpu.VMEM((rows, width), F32),
            pltpu.VMEM((rows, width), F32),
            pltpu.VMEM((24, width), F32),
        ],
        in_specs=[anywhere] * 2 + [vmem] + [anywhere] * 4 + [vmem] * 7,
        out_specs=[vmem] * 7,
        scratch_shapes=[pltpu.VMEM(shape, dtype) for _, shape, dtype in SCRATCH]
        + [pltpu.SemaphoreType.DMA(shape) for _, shape in SEMS],
        compiler_params=pltpu.CompilerParams(
            collective_id=0, has_side_effects=True, vmem_limit_bytes=VMEM_LIMIT
        ),
        name="fused_block",
    )(
        hidden_in, cotangent, segment_ids,
        up_weight, down_weight, qkv_weight, proj_weight,
        up_bias, qkv_bias, out_bias, *norm_params,
    )


FINISH_ROWS = 256
OUT_SLOTS = 4


def finish_kernel(
    down, up, qkv, proj, hid, grad, small,
    hid_o, grad_o, gain1_o, bias1_o, gain2_o, bias2_o, qkv_o, qkvb_o, proj_o, up_o, upb_o,
    down_o, outb_o, wide, out_sem, row_sem,
):
    rows_out = [
        pltpu.make_async_copy(hid, hid_o, row_sem.at[0]),
        pltpu.make_async_copy(grad, grad_o, row_sem.at[1]),
    ]
    blocks = []
    for src, dst in ((down, down_o), (up, up_o), (qkv, qkv_o), (proj, proj_o)):
        for n in range(src.shape[0] // FINISH_ROWS):
            blocks.append((src, dst, n * FINISH_ROWS, src.shape[1]))

    def store(n):
        _, dst, first, across = blocks[n]
        slot = n % OUT_SLOTS
        return pltpu.make_async_copy(
            wide.at[slot, :, pl.ds(0, across)], dst.at[pl.ds(first, FINISH_ROWS)], out_sem.at[slot]
        )

    for copy in rows_out:
        copy.start()
    me = lax.axis_index("tensor")
    for n, out in enumerate((gain1_o, bias1_o, gain2_o, bias2_o)):
        out[...] = small[pl.ds(4 * n + me, 1), :].reshape(512)
    for n in range(4):
        upb_o[pl.ds(n * 512, 512)] = small[16 + n : 17 + n, :].reshape(512)
    for n in range(3):
        qkvb_o[pl.ds(n * 512, 512)] = small[20 + n : 21 + n, :].reshape(512)
    outb_o[...] = small[23:24, :].reshape(512)
    for n, (src, _, first, across) in enumerate(blocks):
        if n >= OUT_SLOTS:
            store(n - OUT_SLOTS).wait()

        @pl.loop(0, FINISH_ROWS // 32)
        def _(b):
            rows = pl.ds(start(b, 32), 32)
            here = pl.ds(pl.multiple_of(first + b * 32, 32), 32)
            wide[n % OUT_SLOTS, rows, 0:across] = src[here, :].astype(F32)

        store(n).start()
    for n in range(len(blocks) - OUT_SLOTS, len(blocks)):
        store(n).wait()
    for copy in rows_out:
        copy.wait()


def finish(down, up, qkv, proj, hid, grad, small):
    def wide_like(array):
        return jax.ShapeDtypeStruct(array.shape, F32)

    def line(size):
        return jax.ShapeDtypeStruct((size,), F32)

    vmem, anywhere = pl.BlockSpec(memory_space=pltpu.VMEM), pl.BlockSpec(memory_space=pl.ANY)
    big = sum(array.size for array in (down, up, qkv, proj))
    return pl.pallas_call(
        finish_kernel,
        out_shape=[wide_like(hid), wide_like(grad)]
        + [line(512)] * 4
        + [wide_like(qkv), line(1536), wide_like(proj), wide_like(up), line(2048)]
        + [wide_like(down), line(512)],
        in_specs=[vmem] * 7,
        out_specs=[anywhere] * 2 + [vmem] * 4
        + [anywhere, vmem, anywhere, anywhere, vmem, anywhere, vmem],
        scratch_shapes=[
            pltpu.VMEM((OUT_SLOTS, FINISH_ROWS, 2048), F32),
            pltpu.SemaphoreType.DMA((OUT_SLOTS,)),
            pltpu.SemaphoreType.DMA((2,)),
        ],
        compiler_params=pltpu.CompilerParams(vmem_limit_bytes=9_000_000),
        cost_estimate=pl.CostEstimate(flops=big, bytes_accessed=4 * big, transcendentals=0),
        name="finish",
    )(down, up, qkv, proj, hid, grad, small)


def fits_kernel(net, hidden_in, qkv_weight, up_weight):
    return (
        (net.nd, net.nt) == (8, 4)
        and hidden_in.shape == (512, 512)
        and qkv_weight.shape == (2048, 1536)
        and up_weight.shape == (2048, 2048)
    )


def kernel_path(*args):
    return tuple(finish(*fused_block(*args)))


def per_device(
    net,
    hidden_in,
    segment_ids,
    norm1_gain,
    norm1_bias,
    norm2_gain,
    norm2_bias,
    qkv_weight,
    qkv_bias,
    proj_weight,
    up_weight,
    up_bias,
    down_weight,
    out_bias,
    cotangent,
):
    norm_stack = jnp.stack([norm1_gain, norm1_bias, norm2_gain, norm2_bias])
    if fits_kernel(net, hidden_in, qkv_weight, up_weight):
        return kernel_path(
            hidden_in, cotangent, (norm1_gain, norm1_bias, norm2_gain, norm2_bias), segment_ids,
            up_weight, down_weight, qkv_weight, proj_weight, up_bias, qkv_bias, out_bias,
        )
    full_rows = net.gather(hidden_in, 2)
    norm_full = net.gather(norm_stack, 1)
    cot_full = net.gather(cotangent, 2)
    norm_params = norm_full.astype(F32)
    segment_row = segment_ids[0]
    row_count = full_rows.shape[0]
    heads_here = qkv_weight.shape[1] // (3 * HD)
    normed, inverse = norm_stats(full_rows.astype(F32))
    act_one = (normed * norm_params[0][None, :] + norm_params[1][None, :]).astype(BF16)
    act_two = (normed * norm_params[2][None, :] + norm_params[3][None, :]).astype(BF16)

    pre_up = dot(act_two, up_weight) + up_bias.astype(F32)[None, :]
    hidden_act = gelu_exact(pre_up).astype(BF16)
    down_grad = weight_grad(net, hidden_act, cot_full)
    grad_pre = dot_t(cot_full, down_weight) * gelu_slope(pre_up)
    up_bias_grad = jnp.sum(grad_pre, axis=0)
    grad_pre_low = grad_pre.astype(BF16)
    up_grad = weight_grad(net, act_two, grad_pre_low)

    cosine, sine = rotary_tables(seq_positions(segment_row), ROT)
    index = jnp.arange(row_count, dtype=jnp.int32)
    allowed = (segment_row[:, None] == segment_row[None, :]) & (index[None, :] <= index[:, None])
    qkv_all = dot(act_one, qkv_weight) + qkv_bias.astype(F32)[None, :]
    saved = []
    contexts = []
    for head_num in range(heads_here):
        part = qkv_all[:, head_num * 3 * HD : (head_num + 1) * 3 * HD]
        query_rows = rotate_rows(part[:, :HD], cosine, sine, ROT, 1.0).astype(BF16)
        key_rows = rotate_rows(part[:, HD : 2 * HD], cosine, sine, ROT, 1.0).astype(BF16)
        value_rows = part[:, 2 * HD :].astype(BF16)
        context, attn_probs, probs_low = head_forward(query_rows, key_rows, value_rows, allowed)
        saved.append((query_rows, key_rows, value_rows, context, attn_probs, probs_low))
        contexts.append(context)
    context_all = jnp.concatenate(contexts, axis=1)
    proj_grad = weight_grad(net, context_all, cot_full)
    partial_value = dot(context_all, proj_weight) + dot(hidden_act, down_weight)
    mixed = net.scatter_sum(partial_value)
    hidden_out = hidden_in.astype(F32) + mixed + out_bias.astype(F32)[None, :]
    out_bias_grad = jnp.sum(cotangent.astype(F32), axis=0)
    grad_context = dot_t(cot_full, proj_weight).astype(BF16)
    grad_act_two = dot_t(grad_pre_low, up_weight)
    head_grads = []
    for head_num in range(heads_here):
        grad_slice = grad_context[:, head_num * HD : (head_num + 1) * HD]
        query_rows, key_rows, value_rows, context, attn_probs, probs_low = saved[head_num]
        grad_query, grad_keys, grad_values = head_backward(
            query_rows, key_rows, value_rows, context, grad_slice, attn_probs, probs_low
        )
        head_grads.append(rotate_rows(grad_query, cosine, sine, ROT, -1.0))
        head_grads.append(rotate_rows(grad_keys, cosine, sine, ROT, -1.0))
        head_grads.append(grad_values)
    grad_qkv = jnp.concatenate(head_grads, axis=1)
    qkv_bias_grad = jnp.sum(grad_qkv, axis=0)
    grad_qkv_low = grad_qkv.astype(BF16)
    qkv_grad = weight_grad(net, act_one, grad_qkv_low)
    grad_act_one = dot_t(grad_qkv_low, qkv_weight)
    grad_in_one, gain_one, shift_one = norm_backward(grad_act_one, norm_params[0], normed, inverse)
    grad_in_two, gain_two, shift_two = norm_backward(grad_act_two, norm_params[2], normed, inverse)
    hidden_grad = cotangent.astype(F32) + net.scatter_sum(grad_in_one + grad_in_two)

    width = out_bias.shape[0]
    norm_terms = net.sum_small_tensor(jnp.concatenate([gain_one, shift_one, gain_two, shift_two]))
    norm_share = lax.dynamic_slice_in_dim(
        norm_terms.reshape(4, -1), lax.axis_index("tensor") * width, width, 1
    )
    small = net.sum_small(
        jnp.concatenate([qkv_bias_grad, up_bias_grad, out_bias_grad, norm_share.reshape(-1)])
    )
    sizes = [qkv_bias.shape[0], up_bias.shape[0]] + [width] * 5
    parts, at = [], 0
    for size in sizes:
        parts.append(small[at : at + size])
        at += size
    return (
        hidden_out,
        hidden_grad,
        parts[3],
        parts[4],
        parts[5],
        parts[6],
        qkv_grad,
        parts[0],
        proj_grad,
        up_grad,
        parts[1],
        down_grad,
        parts[2],
    )


def solution(mesh):
    net = Net(mesh)
    placed = (
        P("dp", "tensor"),
        P("dp", None),
        P("tensor"),
        P("tensor"),
        P("tensor"),
        P("tensor"),
        P(None, "tensor"),
        P("tensor"),
        P("tensor", None),
        P(None, "tensor"),
        P("tensor"),
        P("tensor", None),
        P("tensor"),
        P("dp", "tensor"),
    )

    def body(*args):
        return per_device(net, *args)

    return jax.shard_map(
        body,
        mesh=mesh,
        in_specs=placed,
        out_specs=(
            P("dp", "tensor"),
            P("dp", "tensor"),
            P("tensor"),
            P("tensor"),
            P("tensor"),
            P("tensor"),
            P(None, "tensor"),
            P("tensor"),
            P("tensor", None),
            P(None, "tensor"),
            P("tensor"),
            P("tensor", None),
            P("tensor"),
        ),
        check_vma=False,
    )
```
